128 devices in a mesh: fsdp: 32 (over z, y, core), seq: 4 (over x).
Axes of the slice: x: 4, y: 4, z: 4, core: 2. Of those that a mesh axis runs over, the one named last changes fastest.
Arguments:
- tokens: bfloat16 [32, 512, 4096], P('fsdp'), may hold values from -7 to 7
- norm_gain: float32 [4096], replicated, may hold values from 0.1 to 1.9
- curvature: bfloat16 [32, 512, 4096], P('fsdp'), may hold values from 0.19921875 to 2
- weight_slots: bfloat16 [4, 384, 128, 128], P('seq', 'fsdp'), may hold values from -1 to 1
- probe_slots: bfloat16 [4, 384, 128, 128], P('seq', 'fsdp'), may hold values from -0.09375 to 0.09375
- block_counts: int32 [4, 32], P('seq'), may hold values from 1 to 12, 320 in all within a row
Outputs:
- hvp_slots: float32 [4, 384, 128, 128], P('seq', 'fsdp')
The draws below stay inside these ranges and needn't reach their ends.
Inputs may be any that keep to these rules, and one draw needn't show every extreme that they name: `block_counts`: in each row, device d along fsdp owns the n_d blocks that follow the earlier devices' blocks, in its first n_d slots; a row sums to 320, and 12 is reached in every row.
All inputs are finite; a program needn't handle non-finite values.
Results may differ from the reference program's by a relative error of at most 0.018.
Values may be sent and summed in bfloat16 or wider, within the bound.
A program may use at most 128 MiB of HBM per device.

```python
import math
import jax
import jax.numpy as jnp
import numpy as np
from jax import lax

D = 4096
HQ = 16
HK = 4
HD = 128
BLK = 128
LEN = 512
NB = 320
SLOTS = 12
N_FSDP = 32
N_SEQ = 4


def draw_tokens(key, part):
    own_key = jax.random.fold_in(key, 11)
    noise = jax.random.normal(own_key, (N_FSDP, LEN, D), jnp.float32)
    result = jnp.clip(noise, -6.0, 6.0)
    return result.astype(jnp.bfloat16)


def draw_weight_slots(key, part):
    own_key = jax.random.fold_in(key, 12)
    result = jnp.clip(jax.random.normal(own_key, (N_SEQ, N_FSDP * SLOTS, BLK, BLK), jnp.float32), -6.0, 6.0) * D ** (-0.5)
    return result.astype(jnp.bfloat16)


def block_scale(key, extent, shards, least, largest):
    def one(axis_at, blocks):
        heights = jax.random.uniform(jax.random.fold_in(jax.random.fold_in(key, 6), axis_at), (blocks,), jnp.float32, least / len(shards), largest / len(shards))
        return jnp.repeat(jnp.exp(heights), extent[axis_at] // blocks).reshape((-1,) + (1,) * (len(extent) - axis_at - 1))

    gain = one(*shards[0])
    for cut in shards[1:]:
        gain = gain * one(*cut)
    return gain


def length_profile(number_of, total, reach, skew):
    weights = [(1 << 20) // math.isqrt(grade ** skew) + 1 for grade in range(2, number_of + 1)]
    surplus, holding = total - reach - (number_of - 1), [1] * (number_of - 1)
    while surplus > 0:
        candidates = [i for i in range(number_of - 1) if holding[i] < reach]
        whole, left = sum([weights[i] for i in candidates]), surplus
        for i in candidates:
            more = min(reach - holding[i], max(1, left * weights[i] // whole), surplus)
            holding[i] = holding[i] + more
            surplus = surplus - more
    return np.array([reach] + holding)


def ragged_sizes(key, count, total, bound, slope):
    if count == 2:
        one = jax.random.randint(key, (), max(1, total - bound), min(bound, total - 1) + 1)
        return jnp.stack([one, total - one])
    lengths = jnp.asarray(length_profile(count, total, bound, slope), jnp.int32)
    couples = (count - 1) // 2
    giver, receiver = lengths[1:1 + 2 * couples:2], lengths[2:2 + 2 * couples:2]
    margin = jnp.minimum(giver - 1, bound - receiver)
    moved = jax.random.randint(jax.random.fold_in(key, 1), (couples,), 0, 1 << 20) % (margin + 1)
    lengths = lengths.at[1:1 + 2 * couples:2].set(giver - moved).at[2:2 + 2 * couples:2].set(receiver + moved)
    return lengths[jax.random.permutation(jax.random.fold_in(key, 2), count)]


def centred(rng, dims, deviation, bound, cuts=(), kind=jnp.bfloat16):
    loudness = block_scale(rng, dims, cuts, -0.22, 0.18) if cuts else 1.0
    values = jax.random.normal(rng, dims, jnp.float32) * deviation * loudness
    return jnp.minimum(jnp.maximum(values, -bound), bound).astype(kind)


def setup_inputs(seed: int = 0) -> dict:
    streams_of = jax.random.split(jax.random.key(seed), 7)
    tokens = draw_tokens(jax.random.fold_in(streams_of[6], 71), 0)
    norm_gain = jnp.clip(1.0 + 0.18 * jax.random.normal(streams_of[1], (D,), jnp.float32), 0.1, 1.9)
    curvature = jnp.clip(jnp.exp(math.log(2.0) - 2.306499 * jax.random.uniform(streams_of[2], (N_FSDP, LEN, D), jnp.float32) ** block_scale(streams_of[2], (N_FSDP, LEN, D), ((0, 32),), -0.2, 0.2)), 0.19921875, 2.0).astype(jnp.bfloat16)
    weight_slots = draw_weight_slots(jax.random.fold_in(streams_of[6], 71), 0)
    probe_slots = centred(streams_of[4], (N_SEQ, N_FSDP * SLOTS, BLK, BLK), D ** -0.5, 0.09375, ((0, 4), (1, 32)))
    block_counts = jax.vmap(lambda own: ragged_sizes(own, N_FSDP, NB, SLOTS, 2))(jax.random.split(streams_of[5], N_SEQ)).reshape((N_SEQ, N_FSDP)).astype(jnp.int32)
    return dict(tokens=tokens, norm_gain=norm_gain, curvature=curvature, weight_slots=weight_slots, probe_slots=probe_slots, block_counts=block_counts)


THETA = 500000.0
EPS = 1e-05
NEGATIVE = -1e+30

def rotary(length, head_dim):
    half_dim = head_dim // 2
    frequency = jnp.exp(-jnp.log(THETA) * 2.0 * jnp.arange(half_dim, dtype=jnp.float32) / head_dim)
    angles = jnp.arange(length, dtype=jnp.float32)[:, None] * frequency[None, :]
    return (jnp.cos(angles)[:, None, :], jnp.sin(angles)[:, None, :])

def rotate(field_in, cosine, sine):
    half_dim = field_in.shape[-1] // 2
    first_half = field_in[..., :half_dim]
    second = field_in[..., half_dim:]
    return jnp.concatenate([first_half * cosine - second * sine, second * cosine + first_half * sine], axis=-1)

def normalize(tokens, norm_gain):
    values = tokens.astype(jnp.float32)
    factor = lax.rsqrt(lax.optimization_barrier(jnp.mean(values * values, axis=-1, keepdims=True)) + EPS)
    return (values * factor * norm_gain).astype(jnp.bfloat16)

def attention_branch(w_qkv, w_out, normed, cosine, sine, q_heads, kv_heads):
    length = normed.shape[0]
    head_dim = w_out.shape[0] // q_heads
    projected = jnp.dot(normed, w_qkv, preferred_element_type=jnp.float32)
    q_end = q_heads * head_dim
    k_end = q_end + kv_heads * head_dim
    queries = rotate(projected[:, :q_end].reshape(length, q_heads, head_dim), cosine, sine).astype(jnp.bfloat16)
    key_rows = rotate(projected[:, q_end:k_end].reshape(length, kv_heads, head_dim), cosine, sine).astype(jnp.bfloat16)
    values = projected[:, k_end:].reshape(length, kv_heads, head_dim).astype(jnp.bfloat16)
    queries, key_rows, values = lax.optimization_barrier((queries, key_rows, values))
    queries = queries.reshape(length, kv_heads, q_heads // kv_heads, head_dim)
    scores = jnp.einsum('qkgd,skd->kgqs', queries.astype(jnp.float32), key_rows.astype(jnp.float32)) * head_dim ** (-0.5)
    causal = jnp.arange(length)[:, None] >= jnp.arange(length)[None, :]
    scores = jnp.where(causal, scores, NEGATIVE)
    attn_probs = jax.nn.softmax(scores, axis=-1).astype(jnp.bfloat16)
    attn_probs = lax.optimization_barrier(attn_probs)
    mixed_heads = jnp.einsum('kgqs,skd->qkgd', attn_probs.astype(jnp.float32), values.astype(jnp.float32))
    mixed_heads = mixed_heads.reshape(length, q_heads * head_dim).astype(jnp.bfloat16)
    return jnp.dot(mixed_heads, w_out, preferred_element_type=jnp.float32)

def owner_slots(counts, blocks, slots):
    range_ends = jnp.cumsum(counts).astype(jnp.int32)
    starts = (range_ends - counts).astype(jnp.int32)
    block_ids = jnp.arange(blocks, dtype=jnp.int32)
    owners = lax.optimization_barrier(jnp.sum((range_ends[None, :] <= block_ids[:, None]).astype(jnp.int32), axis=1)).astype(jnp.int32)
    owner_hot = owners[:, None] == jnp.arange(counts.shape[0], dtype=jnp.int32)[None, :]
    first_block = lax.optimization_barrier(jnp.sum(jnp.where(owner_hot, starts[None, :], 0), axis=1)).astype(jnp.int32)
    return (owners * slots + block_ids - first_block).astype(jnp.int32)

def to_matrix(blocks, row_blocks, col_blocks):
    blk_edge = blocks.shape[-1]
    return blocks.reshape(row_blocks, col_blocks, blk_edge, blk_edge).transpose(0, 2, 1, 3).reshape(row_blocks * blk_edge, col_blocks * blk_edge)

def to_blocks(matrix, blk_edge):
    row_blocks = matrix.shape[0] // blk_edge
    col_blocks = matrix.shape[1] // blk_edge
    return matrix.reshape(row_blocks, blk_edge, col_blocks, blk_edge).transpose(0, 2, 1, 3).reshape(row_blocks * col_blocks, blk_edge, blk_edge)

def reference(tokens, norm_gain, curvature, weight_slots, probe_slots, block_counts):
    n_columns = weight_slots.shape[0]
    q_heads = HQ // n_columns
    kv_heads = HK // n_columns
    row_blocks = D // BLK
    qkv_cols = (q_heads + 2 * kv_heads) * HD // BLK
    out_rows = q_heads * HD // BLK
    qkv_split = row_blocks * qkv_cols
    cosine, sine = rotary(LEN, HD)
    normed = jax.vmap(normalize, in_axes=(0, None))(tokens, norm_gain)
    tangent_sum = jnp.zeros((N_FSDP, LEN, D), jnp.float32)
    unpacked = []
    for column in range(n_columns):
        slot_of = owner_slots(block_counts[column], NB, SLOTS)
        w_blocks = weight_slots[column][slot_of]
        p_blocks = probe_slots[column][slot_of]
        w_qkv = to_matrix(w_blocks[:qkv_split], row_blocks, qkv_cols)
        w_out = to_matrix(w_blocks[qkv_split:], out_rows, row_blocks)
        p_qkv = to_matrix(p_blocks[:qkv_split], row_blocks, qkv_cols)
        p_out = to_matrix(p_blocks[qkv_split:], out_rows, row_blocks)

        def tangent_one(seq_normed, w_qkv=w_qkv, w_out=w_out, p_qkv=p_qkv, p_out=p_out):

            def inner(first_w, second_w):
                return attention_branch(first_w, second_w, seq_normed, cosine, sine, q_heads, kv_heads)
            return jax.jvp(inner, (w_qkv, w_out), (p_qkv, p_out))[1]
        tangent_sum = tangent_sum + lax.map(tangent_one, normed)
        unpacked.append((slot_of, w_qkv, w_out))
    weighted = (curvature.astype(jnp.float32) * tangent_sum).astype(jnp.bfloat16)
    factor = 1.0 / jnp.sqrt(jnp.float32(LEN * N_FSDP))
    results = []
    for column in range(n_columns):
        slot_of, w_qkv, w_out = unpacked[column]

        def accumulate(grad_total, seq_pair, w_qkv=w_qkv, w_out=w_out):
            seq_normed, seq_weighted = seq_pair

            def inner(first_w, second_w):
                return attention_branch(first_w, second_w, seq_normed, cosine, sine, q_heads, kv_heads)
            _, pullback = jax.vjp(inner, w_qkv, w_out)
            g_qkv, g_out = pullback(seq_weighted.astype(jnp.float32))
            grad_blocks = jnp.concatenate([to_blocks(g_qkv, BLK), to_blocks(g_out, BLK)], axis=0)
            return (grad_total + grad_blocks.astype(jnp.float32), None)
        grad_total, _ = lax.scan(accumulate, jnp.zeros((NB, BLK, BLK), jnp.float32), (normed, weighted))
        packed = jnp.zeros((N_FSDP * SLOTS, BLK, BLK), jnp.float32).at[slot_of].set(grad_total * factor)
        results.append(packed)
    return jnp.stack(results)
```

```python
import functools

import jax
import jax.numpy as jnp
import numpy as np
from jax import lax
from jax.experimental import pallas as pl
from jax.experimental.pallas import tpu as pltpu
from jax.sharding import PartitionSpec as P

D = 4096
HD = 128
BLK = 128
LEN = 512
QH = 4
QKV = 768
OUT = 512
NQKV = 192
NB = 320
SLOTS = 12
HALF = 6
THETA = 500000.0
EPS = 1e-05
NEGATIVE = -1e30
VMEM_LIMIT = 66_000_000
MESH = pl.DeviceIdType.MESH
F32 = jnp.float32
BF16 = jnp.bfloat16


def tables():
    half = HD // 2
    frequency = np.exp(-np.log(THETA) * 2.0 * np.arange(half) / HD)
    angles = np.arange(LEN)[:, None] * frequency[None, :]
    c, s = np.cos(angles), np.sin(angles)
    return (
        np.concatenate([c, c], axis=1).astype(np.float32),
        np.concatenate([-s, s], axis=1).astype(np.float32),
    )


def place():
    me = lax.axis_index("fsdp")
    core = lax.rem(me, 2)
    y = lax.rem(me // 2, 4)
    z = me // 8
    return me, core, y, z


def index_of(z, y, core):
    return (z * 4 + y) * 2 + core


def wrap(a):
    return lax.rem(a + 4, 4)


def greet(targets):
    barrier = pltpu.get_barrier_semaphore()
    for t in targets:
        pl.semaphore_signal(barrier, inc=1, device_id=t, device_id_type=MESH)
    pl.semaphore_wait(barrier, len(targets))


def gather_kernel(w_ref, p_ref, out_ref, send_sem, recv_sem, local_sem):
    me, core, y, z = place()
    sib = index_of(z, y, 1 - core)

    def at(axis, step):
        if axis == "y":
            return {"fsdp": index_of(z, wrap(y + step), core)}
        return {"fsdp": index_of(wrap(z + step), y, core)}

    greet([at("y", 1), at("y", -1), at("z", 1), at("z", -1), {"fsdp": sib}])

    own = [
        pltpu.make_async_copy(w_ref, out_ref.at[me, 0], local_sem.at[0]),
        pltpu.make_async_copy(p_ref, out_ref.at[me, 1], local_sem.at[1]),
    ]
    for c in own:
        c.start()

    counter = [0]
    sends = []

    def sem():
        counter[0] += 1
        return counter[0] - 1

    def send(src, dst, number, target):
        copy = pltpu.make_async_remote_copy(
            src_ref=src,
            dst_ref=dst,
            send_sem=send_sem.at[number],
            recv_sem=recv_sem.at[number],
            device_id=target,
            device_id_type=MESH,
        )
        copy.start()
        sends.append(copy)
        return copy

    def piece(tensor, origin, part=None):
        if part is None:
            return out_ref.at[origin, tensor]
        return out_ref.at[origin, tensor, pl.ds(part * HALF, HALF)]

    first = ("y", "z")
    second = ("z", "y")

    def origin_of(tensor, f, s):
        if tensor == 0:
            return index_of(wrap(z + s), wrap(y + f), core)
        return index_of(wrap(z + f), wrap(y + s), core)

    number = {}
    for tensor in (0, 1):
        for role in ("f+", "f-", "fa", "fb"):
            number[tensor, role] = sem()
        for f in (0, 1, -1, 2):
            for role in ("s+", "s-", "sa", "sb"):
                number[tensor, role, f] = sem()
        for f in (0, 1, -1, 2):
            for s in (0, 1, -1, 2):
                number[tensor, "sib", f, s] = sem()

    arrivals = {}

    def go(tensor, role, src_origin, axis, step, part=None, src=None):
        ref = piece(tensor, src_origin, part)
        copy = send(ref if src is None else src, ref, number[(tensor,) + role], at(axis, step))
        arrivals[(tensor,) + role] = copy

    def to_sib(tensor, f, s, src=None):
        origin = origin_of(tensor, f, s)
        ref = piece(tensor, origin)
        copy = send(ref if src is None else src, ref, number[tensor, "sib", f, s], {"fsdp": sib})
        arrivals[tensor, "sib", f, s] = copy

    mine = (w_ref, p_ref)
    for tensor in (0, 1):
        go(tensor, ("f+",), me, first[tensor], 1, src=mine[tensor])
        go(tensor, ("f-",), me, first[tensor], -1, src=mine[tensor])
    for tensor in (0, 1):
        go(tensor, ("s+", 0), me, second[tensor], 1, src=mine[tensor])
        go(tensor, ("s-", 0), me, second[tensor], -1, src=mine[tensor])
    for tensor in (0, 1):
        to_sib(tensor, 0, 0, src=mine[tensor])

    for tensor in (0, 1):
        arrivals[tensor, "f+"].wait_recv()
        lower = origin_of(tensor, -1, 0)
        go(tensor, ("fa",), lower, first[tensor], 1, part=0)
        go(tensor, ("s+", -1), lower, second[tensor], 1)
        go(tensor, ("s-", -1), lower, second[tensor], -1)
        arrivals[tensor, "f-"].wait_recv()
        upper = origin_of(tensor, 1, 0)
        go(tensor, ("fb",), upper, first[tensor], -1, part=1)
        go(tensor, ("s+", 1), upper, second[tensor], 1)
        go(tensor, ("s-", 1), upper, second[tensor], -1)
        to_sib(tensor, -1, 0)
        to_sib(tensor, 1, 0)

    def pass_on(tensor, f):
        arrivals[tensor, "s+", f].wait_recv()
        go(tensor, ("sa", f), origin_of(tensor, f, -1), second[tensor], 1, part=0)
        to_sib(tensor, f, -1)
        arrivals[tensor, "s-", f].wait_recv()
        go(tensor, ("sb", f), origin_of(tensor, f, 1), second[tensor], -1, part=1)
        to_sib(tensor, f, 1)

    for tensor in (0, 1):
        pass_on(tensor, 0)
    for tensor in (0, 1):
        arrivals[tensor, "fa"].wait_recv()
        arrivals[tensor, "fb"].wait_recv()
        far = origin_of(tensor, 2, 0)
        go(tensor, ("s+", 2), far, second[tensor], 1)
        go(tensor, ("s-", 2), far, second[tensor], -1)
        to_sib(tensor, 2, 0)
    for f in (-1, 1, 2):
        for tensor in (0, 1):
            pass_on(tensor, f)
            if f == -1:
                g = 0
            elif f == 1:
                g = -1
            else:
                g = 1
            arrivals[tensor, "sa", g].wait_recv()
            arrivals[tensor, "sb", g].wait_recv()
            to_sib(tensor, g, 2)
    for tensor in (0, 1):
        arrivals[tensor, "sa", 2].wait_recv()
        arrivals[tensor, "sb", 2].wait_recv()
        to_sib(tensor, 2, 2)
    for key, copy in arrivals.items():
        if key[1] == "sib":
            copy.wait_recv()
    for c in own:
        c.wait()
    for copy in sends:
        copy.wait_send()


def gather(w, p):
    vmem = pl.BlockSpec(memory_space=pltpu.VMEM)
    return pl.pallas_call(
        gather_kernel,
        out_shape=jax.ShapeDtypeStruct((32, 2, SLOTS, BLK, BLK), BF16),
        in_specs=[vmem, vmem],
        out_specs=pl.BlockSpec(memory_space=pl.ANY),
        scratch_shapes=[
            pltpu.SemaphoreType.DMA((72,)),
            pltpu.SemaphoreType.DMA((72,)),
            pltpu.SemaphoreType.DMA((2,)),
        ],
        compiler_params=pltpu.CompilerParams(collective_id=0, has_side_effects=True),
        name="gather",
    )(w, p)


def nt(a, b):
    return lax.dot_general(a, b, (((1,), (1,)), ((), ())), preferred_element_type=F32)


def nn(a, b):
    return jnp.dot(a, b, preferred_element_type=F32)


def causal_mask():
    row = lax.broadcasted_iota(jnp.int32, (LEN, LEN), 0)
    col = lax.broadcasted_iota(jnp.int32, (LEN, LEN), 1)
    return row >= col


def forward_kernel(
    counts,
    tokens,
    gain,
    cos,
    sin,
    slots,
    tan_out,
    normed_out,
    qkv_out,
    mixed_out,
    probs_out,
    wo_out,
    normed,
    wqkv,
    wout,
    proj,
    sides,
    probs,
    qkv,
    sem,
):
    def device(d, start):
        n = counts[d]

        def one(t, carry):
            b = start + t

            @pl.when(b < NQKV)
            def _():
                r = pl.multiple_of((b // 6) * BLK, BLK)
                c = pl.multiple_of((b % 6) * BLK, BLK)
                pltpu.make_async_copy(
                    slots.at[d, :, t], wqkv.at[:, pl.ds(r, BLK), pl.ds(c, BLK)], sem.at[0]
                ).start()

            @pl.when(b >= NQKV)
            def _():
                e = b - NQKV
                r = pl.multiple_of((e // 32) * BLK, BLK)
                c = pl.multiple_of((e % 32) * BLK, BLK)
                pltpu.make_async_copy(
                    slots.at[d, :, t], wout.at[:, pl.ds(r, BLK), pl.ds(c, BLK)], sem.at[1]
                ).start()

            return carry

        lax.fori_loop(0, n, one, 0)
        return start + n

    lax.fori_loop(0, 32, device, 0)

    def norm(i, carry):
        rows = pl.ds(pl.multiple_of(i * 32, 32), 32)
        x = tokens[rows, :].astype(F32)
        factor = lax.rsqrt(jnp.mean(x * x, axis=-1, keepdims=True) + EPS)
        normed[rows, :] = (x * factor * gain[...]).astype(BF16)
        return carry

    lax.fori_loop(0, LEN // 32, norm, 0)
    save_normed = pltpu.make_async_copy(normed, normed_out, sem.at[2])
    save_normed.start()
    pltpu.make_async_copy(wqkv, wqkv, sem.at[0]).wait()

    for tensor in (0, 1):
        for n in range(3):
            cols = slice(n * 256, (n + 1) * 256)
            proj[tensor, :, cols] = nn(normed[...], wqkv[tensor, :, cols])

    c2, s2 = cos[...], sin[...]

    def rot(x):
        return x * c2 + pltpu.roll(x, 64, 1) * s2

    def head(tensor, h):
        x = proj[tensor, :, h * HD : (h + 1) * HD]
        if h < QH + 1:
            x = rot(x)
        return x.astype(BF16)

    for h in range(QH + 2):
        qkv[:, h * HD : (h + 1) * HD] = head(0, h)
    save_qkv = pltpu.make_async_copy(qkv, qkv_out, sem.at[3])
    save_qkv.start()
    k = qkv[:, QH * HD : (QH + 1) * HD]
    v = qkv[:, (QH + 1) * HD :]
    keys = jnp.concatenate([k, head(1, QH)], axis=1)
    values = jnp.concatenate([v, head(1, QH + 1)], axis=1)
    causal = causal_mask()
    scale = HD**-0.5
    for h in range(QH):
        q = qkv[:, h * HD : (h + 1) * HD]
        tq = head(1, h)
        s = jnp.where(causal, nt(q, k) * scale, NEGATIVE)
        m = jnp.max(s, axis=-1, keepdims=True)
        e = jnp.exp(s - m)
        p = e * (1.0 / jnp.sum(e, axis=-1, keepdims=True))
        ts = nt(jnp.concatenate([tq, q], axis=1), keys) * scale
        pt = p * ts
        tp = pt - p * jnp.sum(pt, axis=-1, keepdims=True)
        pb = p.astype(BF16)
        probs[h] = pb
        both = nn(pb, values)
        mixed_t = nn(tp.astype(BF16), v) + both[:, HD:]
        sides[0, :, h * HD : (h + 1) * HD] = mixed_t.astype(BF16)
        sides[1, :, h * HD : (h + 1) * HD] = both[:, :HD].astype(BF16)
    save_probs = pltpu.make_async_copy(probs, probs_out, sem.at[4])
    save_probs.start()
    save_mixed = pltpu.make_async_copy(sides.at[1], mixed_out, sem.at[5])
    save_mixed.start()
    pltpu.make_async_copy(wout, wout, sem.at[1]).wait()
    save_wo = pltpu.make_async_copy(wout.at[0], wo_out, sem.at[6])
    save_wo.start()
    for n in range(8):
        cols = slice(n * 512, (n + 1) * 512)
        tan_out[:, cols] = (
            nn(sides[0], wout[0, :, cols]) + nn(sides[1], wout[1, :, cols])
        ).astype(BF16)
    for c in (save_normed, save_qkv, save_probs, save_mixed, save_wo):
        c.wait()


def forward(counts, tokens, gain, cos, sin, slots):
    vmem = pl.BlockSpec(memory_space=pltpu.VMEM)
    hbm = pl.BlockSpec(memory_space=pl.ANY)
    smem = pl.BlockSpec(memory_space=pltpu.SMEM)
    shape = jax.ShapeDtypeStruct
    return pl.pallas_call(
        forward_kernel,
        out_shape=[
            shape((LEN, D), BF16),
            shape((LEN, D), BF16),
            shape((LEN, QKV), BF16),
            shape((LEN, OUT), BF16),
            shape((QH, LEN, LEN), BF16),
            shape((OUT, D), BF16),
        ],
        in_specs=[smem, vmem, vmem, vmem, vmem, hbm],
        out_specs=[vmem, hbm, hbm, hbm, hbm, hbm],
        scratch_shapes=[
            pltpu.VMEM((LEN, D), BF16),
            pltpu.VMEM((2, D, QKV), BF16),
            pltpu.VMEM((2, OUT, D), BF16),
            pltpu.VMEM((2, LEN, QKV), F32),
            pltpu.VMEM((2, LEN, OUT), BF16),
            pltpu.VMEM((QH, LEN, LEN), BF16),
            pltpu.VMEM((LEN, QKV), BF16),
            pltpu.SemaphoreType.DMA((7,)),
        ],
        compiler_params=pltpu.CompilerParams(vmem_limit_bytes=VMEM_LIMIT),
        name="forward",
    )(counts, tokens, gain, cos, sin, slots)


def exchange_kernel(tan, curv, out, cbuf, opp_a, opp_b, low, high, send_sem, recv_sem, sem):
    me = lax.axis_index("seq")
    rows = LEN // 4
    half = rows // 2
    up, down = {"seq": wrap(me + 1)}, {"seq": wrap(me - 1)}
    greet([up, down])
    get = pltpu.make_async_copy(
        curv.at[pl.ds(pl.multiple_of(me * rows, rows), rows)], cbuf, sem.at[0]
    )
    get.start()

    def span(chunk, part=None):
        if part is None:
            return pl.ds(pl.multiple_of(chunk * rows, rows), rows)
        return pl.ds(pl.multiple_of(chunk * rows + part * half, half), half)

    sends = []

    def send(src, dst, number, target):
        copy = pltpu.make_async_remote_copy(
            src_ref=src,
            dst_ref=dst,
            send_sem=send_sem.at[number],
            recv_sem=recv_sem.at[number],
            device_id=target,
            device_id_type=MESH,
        )
        copy.start()
        sends.append(copy)
        return copy

    far = wrap(me + 2)
    nxt, prv = wrap(me + 1), wrap(me - 1)
    a0 = send(tan.at[span(far, 0)], opp_a, 0, up)
    b0 = send(tan.at[span(far, 1)], opp_b, 1, down)
    a1 = send(tan.at[span(nxt, 1)], low.at[1], 2, up)
    b1 = send(tan.at[span(prv, 0)], high.at[0], 3, down)
    a0.wait_recv()
    opp_a[...] = (opp_a[...].astype(F32) + tan[span(nxt, 0), :].astype(F32)).astype(BF16)
    a2 = send(opp_a, low.at[0], 4, up)
    b0.wait_recv()
    opp_b[...] = (opp_b[...].astype(F32) + tan[span(prv, 1), :].astype(F32)).astype(BF16)
    b2 = send(opp_b, high.at[1], 5, down)
    get.wait()

    def finish(part):
        total = (
            tan[span(me, part), :].astype(F32)
            + low[part].astype(F32)
            + high[part].astype(F32)
        )
        c = cbuf[pl.ds(part * half, half), :].astype(F32)
        out[span(me, part), :] = (total * c).astype(BF16)

    a1.wait_recv()
    b2.wait_recv()
    finish(1)
    c1 = send(out.at[span(me, 1)], out.at[span(me, 1)], 6, up)
    d1 = send(out.at[span(me, 1)], out.at[span(me, 1)], 7, down)
    a2.wait_recv()
    b1.wait_recv()
    finish(0)
    c0 = send(out.at[span(me, 0)], out.at[span(me, 0)], 8, up)
    d0 = send(out.at[span(me, 0)], out.at[span(me, 0)], 9, down)
    c1.wait_recv()
    e1 = send(out.at[span(prv, 1)], out.at[span(prv, 1)], 10, up)
    d1.wait_recv()
    d0.wait_recv()
    e0 = send(out.at[span(nxt, 0)], out.at[span(nxt, 0)], 11, down)
    c0.wait_recv()
    e1.wait_recv()
    e0.wait_recv()
    for copy in sends:
        copy.wait_send()


def exchange(tan, curv):
    vmem = pl.BlockSpec(memory_space=pltpu.VMEM)
    hbm = pl.BlockSpec(memory_space=pl.ANY)
    rows = LEN // 4
    half = rows // 2
    return pl.pallas_call(
        exchange_kernel,
        out_shape=jax.ShapeDtypeStruct((LEN, D), BF16),
        in_specs=[vmem, hbm],
        out_specs=vmem,
        scratch_shapes=[
            pltpu.VMEM((rows, D), BF16),
            pltpu.VMEM((half, D), BF16),
            pltpu.VMEM((half, D), BF16),
            pltpu.VMEM((2, half, D), BF16),
            pltpu.VMEM((2, half, D), BF16),
            pltpu.SemaphoreType.DMA((12,)),
            pltpu.SemaphoreType.DMA((12,)),
            pltpu.SemaphoreType.DMA((1,)),
        ],
        compiler_params=pltpu.CompilerParams(
            collective_id=1, has_side_effects=True, vmem_limit_bytes=40_000_000
        ),
        name="exchange",
    )(tan, curv)


def backward_kernel(
    counts,
    weighted,
    cos,
    sin,
    normed_in,
    qkv_in,
    mixed_in,
    probs_in,
    wo_in,
    out,
    normed,
    qkv,
    mixed,
    probs,
    wo,
    gout,
    gqkv,
    dprojt,
    sem,
):
    loads = [
        pltpu.make_async_copy(a, b, sem.at[i])
        for i, (a, b) in enumerate(
            ((wo_in, wo), (mixed_in, mixed), (probs_in, probs), (qkv_in, qkv), (normed_in, normed))
        )
    ]
    for c in loads:
        c.start()
    loads[0].wait()
    dmixed = nt(weighted[...], wo[...]).astype(BF16)
    loads[1].wait()
    mixedt = mixed[...].T
    for n in range(8):
        cols = slice(n * 512, (n + 1) * 512)
        gout[:, cols] = nn(mixedt, weighted[:, cols]).astype(BF16)
    loads[2].wait()
    loads[3].wait()
    c2, s2 = cos[...], sin[...]

    def unrot(x):
        return x * c2 - pltpu.roll(x, 64, 1) * s2

    k = qkv[:, QH * HD : (QH + 1) * HD]
    v = qkv[:, (QH + 1) * HD :]
    scale = HD**-0.5
    dkt = jnp.zeros((HD, LEN), F32)
    dvt = jnp.zeros((HD, LEN), F32)
    for h in range(QH):
        dm = dmixed[:, h * HD : (h + 1) * HD]
        q = qkv[:, h * HD : (h + 1) * HD]
        pb = probs[h]
        dp = nt(dm, v).astype(BF16).astype(F32)
        dvt = dvt + nn(dm.T, pb)
        pf = pb.astype(F32)
        pd = pf * dp
        ds = ((pd - pf * jnp.sum(pd, axis=-1, keepdims=True)) * scale).astype(BF16)
        dkt = dkt + nn(q.T, ds)
        dq = unrot(nn(ds, k).astype(BF16).astype(F32)).astype(BF16)
        dprojt[h * HD : (h + 1) * HD, :] = dq.T
    dk = unrot(dkt.astype(BF16).astype(F32).T).astype(BF16)
    dprojt[QH * HD : (QH + 1) * HD, :] = dk.T
    dprojt[(QH + 1) * HD :, :] = dvt.astype(BF16)
    loads[4].wait()
    for n in range(8):
        cols = slice(n * 512, (n + 1) * 512)
        gqkv[:, cols] = nn(dprojt[...], normed[:, cols]).astype(BF16)

    def device(d, start):
        n = counts[d]

        def one(t, carry):
            b = start + t

            @pl.when(b < NQKV)
            def _():
                r = pl.multiple_of((b // 6) * BLK, BLK)
                c = pl.multiple_of((b % 6) * BLK, BLK)
                pltpu.make_async_copy(
                    gqkv.at[pl.ds(c, BLK), pl.ds(r, BLK)], out.at[d, t], sem.at[5]
                ).start()

            @pl.when(b >= NQKV)
            def _():
                e = b - NQKV
                r = pl.multiple_of((e // 32) * BLK, BLK)
                c = pl.multiple_of((e % 32) * BLK, BLK)
                pltpu.make_async_copy(
                    gout.at[pl.ds(r, BLK), pl.ds(c, BLK)], out.at[d, t], sem.at[6]
                ).start()

            return carry

        lax.fori_loop(0, n, one, 0)
        return start + n

    lax.fori_loop(0, 32, device, 0)
    pltpu.make_async_copy(gqkv, gqkv, sem.at[5]).wait()
    pltpu.make_async_copy(gout, gout, sem.at[6]).wait()


def backward(counts, weighted, cos, sin, normed, qkv, mixed, probs, wo):
    vmem = pl.BlockSpec(memory_space=pltpu.VMEM)
    hbm = pl.BlockSpec(memory_space=pl.ANY)
    smem = pl.BlockSpec(memory_space=pltpu.SMEM)
    return pl.pallas_call(
        backward_kernel,
        out_shape=jax.ShapeDtypeStruct((32, SLOTS, BLK, BLK), BF16),
        in_specs=[smem, vmem, vmem, vmem] + [hbm] * 5,
        out_specs=hbm,
        scratch_shapes=[
            pltpu.VMEM((LEN, D), BF16),
            pltpu.VMEM((LEN, QKV), BF16),
            pltpu.VMEM((LEN, OUT), BF16),
            pltpu.VMEM((QH, LEN, LEN), BF16),
            pltpu.VMEM((OUT, D), BF16),
            pltpu.VMEM((OUT, D), BF16),
            pltpu.VMEM((QKV, D), BF16),
            pltpu.VMEM((QKV, LEN), BF16),
            pltpu.SemaphoreType.DMA((7,)),
        ],
        compiler_params=pltpu.CompilerParams(vmem_limit_bytes=VMEM_LIMIT),
        name="backward",
    )(counts, weighted, cos, sin, normed, qkv, mixed, probs, wo)


def scatter_kernel(
    grads, out, acc, sibling, r_far, r_low, r_high, red, t_far, t_low, t_high,
    send_sem, recv_sem, local_sem,
):
    me, core, y, z = place()
    sib = {"fsdp": index_of(z, y, 1 - core)}

    def at(axis, step):
        if axis == "y":
            return {"fsdp": index_of(z, wrap(y + step), core)}
        return {"fsdp": index_of(wrap(z + step), y, core)}

    greet([at("y", 1), at("y", -1), at("z", 1), at("z", -1), sib])
    first = ("z", "y")
    second = ("y", "z")
    here = {"y": y, "z": z}
    sends = []
    counter = [0]

    def send(src, dst, target):
        number = counter[0]
        counter[0] += 1
        copy = pltpu.make_async_remote_copy(
            src_ref=src,
            dst_ref=dst,
            send_sem=send_sem.at[number],
            recv_sem=recv_sem.at[number],
            device_id=target,
            device_id_type=MESH,
        )
        copy.start()
        sends.append(copy)
        return copy

    def source(part, f, lane):
        index = wrap(here[first[part]] + f)
        slots = pl.ds(part * HALF, HALF)
        if part == 0:
            return grads.at[index, :, lane, slots]
        return grads.at[:, index, lane, slots]

    order = (2, 1, -1, 0)
    local, cross = {}, {}
    for i, f in enumerate(order):
        for part in (0, 1):
            cross[part, f] = send(source(part, f, 1 - core), sibling.at[part, i], sib)
            local[part, f] = pltpu.make_async_copy(
                source(part, f, core), acc.at[part, i], local_sem.at[part * 4 + i]
            )
            local[part, f].start()

    def add_sibling(part, f):
        i = order.index(f)
        local[part, f].wait()
        cross[part, f].wait_recv()

        def step(s, carry):
            acc[part, i, s] = (
                acc[part, i, s].astype(F32) + sibling[part, i, s].astype(F32)
            ).astype(BF16)
            return carry

        lax.fori_loop(0, 4, step, 0)

    lo, hi = pl.ds(0, 3), pl.ds(3, 3)
    a = {}
    for part in (0, 1):
        add_sibling(part, 2)
        a[part, "fu"] = send(acc.at[part, 0, :, lo], r_far.at[part, 0], at(first[part], 1))
        a[part, "fd"] = send(acc.at[part, 0, :, hi], r_far.at[part, 1], at(first[part], -1))
    for part in (0, 1):
        add_sibling(part, 1)
        a[part, "lo1"] = send(acc.at[part, 1, :, hi], r_low.at[part, 1], at(first[part], 1))
    for part in (0, 1):
        add_sibling(part, -1)
        a[part, "hi0"] = send(acc.at[part, 2, :, lo], r_high.at[part, 0], at(first[part], -1))
    for part in (0, 1):
        a[part, "fu"].wait_recv()

        def step(s, carry, part=part):
            r_far[part, 0, s] = (
                r_far[part, 0, s].astype(F32) + acc[part, 1, s, lo].astype(F32)
            ).astype(BF16)
            return carry

        lax.fori_loop(0, 4, step, 0)
        a[part, "lo0"] = send(r_far.at[part, 0], r_low.at[part, 0], at(first[part], 1))
        a[part, "fd"].wait_recv()

        def step2(s, carry, part=part):
            r_far[part, 1, s] = (
                r_far[part, 1, s].astype(F32) + acc[part, 2, s, hi].astype(F32)
            ).astype(BF16)
            return carry

        lax.fori_loop(0, 4, step2, 0)
        a[part, "hi1"] = send(r_far.at[part, 1], r_high.at[part, 1], at(first[part], -1))
    for part in (0, 1):
        add_sibling(part, 0)
    for part in (0, 1):
        for name in ("lo1", "hi0", "lo0", "hi1"):
            a[part, name].wait_recv()
        for h in (0, 1):

            def step3(s, carry, part=part, h=h):
                red[part, s, pl.ds(3 * h, 3)] = (
                    acc[part, 3, s, pl.ds(3 * h, 3)].astype(F32)
                    + r_low[part, h, s].astype(F32)
                    + r_high[part, h, s].astype(F32)
                ).astype(BF16)
                return carry

            lax.fori_loop(0, 4, step3, 0)
        s_here = here[second[part]]
        far, nxt, prv = wrap(s_here + 2), wrap(s_here + 1), wrap(s_here - 1)
        up, down = at(second[part], 1), at(second[part], -1)
        a[part, "tu"] = send(red.at[part, far, lo], t_far.at[part, 0], up)
        a[part, "td"] = send(red.at[part, far, hi], t_far.at[part, 1], down)
        a[part, "tl1"] = send(red.at[part, nxt, hi], t_low.at[part, 1], up)
        a[part, "th0"] = send(red.at[part, prv, lo], t_high.at[part, 0], down)
    for part in (0, 1):
        s_here = here[second[part]]
        nxt, prv = wrap(s_here + 1), wrap(s_here - 1)
        up, down = at(second[part], 1), at(second[part], -1)
        a[part, "tu"].wait_recv()
        t_far[part, 0] = (t_far[part, 0].astype(F32) + red[part, nxt, lo].astype(F32)).astype(BF16)
        a[part, "tl0"] = send(t_far.at[part, 0], t_low.at[part, 0], up)
        a[part, "td"].wait_recv()
        t_far[part, 1] = (t_far[part, 1].astype(F32) + red[part, prv, hi].astype(F32)).astype(BF16)
        a[part, "th1"] = send(t_far.at[part, 1], t_high.at[part, 1], down)
    for part in (0, 1):
        s_here = here[second[part]]
        for name in ("tl1", "th0", "tl0", "th1"):
            a[part, name].wait_recv()
        for h in (0, 1):
            out[pl.ds(part * HALF + 3 * h, 3)] = (
                red[part, s_here, pl.ds(3 * h, 3)].astype(F32)
                + t_low[part, h].astype(F32)
                + t_high[part, h].astype(F32)
            )
    for copy in sends:
        copy.wait_send()


def scatter(grads):
    vmem = pl.BlockSpec(memory_space=pltpu.VMEM)
    hbm = pl.BlockSpec(memory_space=pl.ANY)
    block = (BLK, BLK)
    return pl.pallas_call(
        scatter_kernel,
        out_shape=jax.ShapeDtypeStruct((SLOTS,) + block, F32),
        in_specs=[hbm],
        out_specs=vmem,
        scratch_shapes=[
            pltpu.VMEM((2, 4, 4, HALF) + block, BF16),
            pltpu.VMEM((2, 4, 4, HALF) + block, BF16),
            pltpu.VMEM((2, 2, 4, 3) + block, BF16),
            pltpu.VMEM((2, 2, 4, 3) + block, BF16),
            pltpu.VMEM((2, 2, 4, 3) + block, BF16),
            pltpu.VMEM((2, 4, HALF) + block, BF16),
            pltpu.VMEM((2, 2, 3) + block, BF16),
            pltpu.VMEM((2, 2, 3) + block, BF16),
            pltpu.VMEM((2, 2, 3) + block, BF16),
            pltpu.SemaphoreType.DMA((32,)),
            pltpu.SemaphoreType.DMA((32,)),
            pltpu.SemaphoreType.DMA((8,)),
        ],
        compiler_params=pltpu.CompilerParams(
            collective_id=2, has_side_effects=True, vmem_limit_bytes=48_000_000
        ),
        name="scatter",
    )(grads.reshape(4, 4, 2, SLOTS, BLK, BLK))


def finish_kernel(counts, total, out):
    me = lax.axis_index("fsdp")
    start = lax.fori_loop(0, me, lambda d, s: s + counts[d], 0)
    n = counts[me]
    factor = 1.0 / np.sqrt(np.float32(LEN * 32))

    def one(t, carry):
        x = total[t] * factor
        x = jnp.where(start + t < NQKV, x.T, x)
        out[t] = jnp.where(t < n, x, 0.0)
        return carry

    lax.fori_loop(0, SLOTS, one, 0)


def finish(counts, total):
    vmem = pl.BlockSpec(memory_space=pltpu.VMEM)
    smem = pl.BlockSpec(memory_space=pltpu.SMEM)
    return pl.pallas_call(
        finish_kernel,
        out_shape=jax.ShapeDtypeStruct((SLOTS, BLK, BLK), F32),
        in_specs=[smem, vmem],
        out_specs=vmem,
        name="finish",
    )(counts, total)


def local(tokens, norm_gain, curvature, weight_slots, probe_slots, block_counts):
    counts = block_counts[0]
    cos, sin = tables()
    slots = gather(weight_slots[0], probe_slots[0])
    tan, normed, qkv, mixed, probs, wo = forward(
        counts, tokens[0], norm_gain.reshape(1, D), cos, sin, slots
    )
    weighted = exchange(tan, curvature[0])
    grads = backward(counts, weighted, cos, sin, normed, qkv, mixed, probs, wo)
    total = scatter(grads)
    return finish(counts, total)[None]


def solution(mesh):
    in_specs = (
        P("fsdp", None, None),
        P(),
        P("fsdp", None, None),
        P("seq", "fsdp", None, None),
        P("seq", "fsdp", None, None),
        P("seq", None),
    )
    out_specs = P("seq", "fsdp", None, None)
    return jax.shard_map(local, mesh=mesh, in_specs=in_specs, out_specs=out_specs, check_vma=False)
```

```python
import functools

import jax
import jax.numpy as jnp
import numpy as np
from jax import lax
from jax.experimental import pallas as pl
from jax.experimental.pallas import tpu as pltpu
from jax.sharding import PartitionSpec as P

D = 4096
HD = 128
BLK = 128
LEN = 512
QH = 4
QKV = 768
OUT = 512
NQKV = 192
NB = 320
SLOTS = 12
HALF = 6
CHUNK = 1024
THETA = 500000.0
EPS = 1e-05
NEGATIVE = -1e30
VMEM_LIMIT = 66_000_000
MESH = pl.DeviceIdType.MESH
F32 = jnp.float32
BF16 = jnp.bfloat16


def tables():
    half = HD // 2
    frequency = np.exp(-np.log(THETA) * 2.0 * np.arange(half) / HD)
    angles = np.arange(LEN)[:, None] * frequency[None, :]
    c, s = np.cos(angles), np.sin(angles)
    return (
        np.concatenate([c, c], axis=1).astype(np.float32),
        np.concatenate([-s, s], axis=1).astype(np.float32),
    )


def place():
    me = lax.axis_index("fsdp")
    core = lax.rem(me, 2)
    y = lax.rem(me // 2, 4)
    z = me // 8
    return me, core, y, z


def index_of(z, y, core):
    return (z * 4 + y) * 2 + core


def wrap(a):
    return lax.rem(a + 4, 4)


def greet(targets):
    barrier = pltpu.get_barrier_semaphore()
    for t in targets:
        pl.semaphore_signal(barrier, inc=1, device_id=t, device_id_type=MESH)
    pl.semaphore_wait(barrier, len(targets))


def gather_kernel(
    w_ref, p_ref, tokens_in, gain, out_ref, normed_out, tokens, normed, send_sem, recv_sem, local_sem
):
    me, core, y, z = place()
    get_tokens = pltpu.make_async_copy(tokens_in, tokens, local_sem.at[2])
    get_tokens.start()
    sib = index_of(z, y, 1 - core)

    def at(axis, step):
        if axis == "y":
            return {"fsdp": index_of(z, wrap(y + step), core)}
        return {"fsdp": index_of(wrap(z + step), y, core)}

    greet([at("y", 1), at("y", -1), at("z", 1), at("z", -1), {"fsdp": sib}])

    own = [
        pltpu.make_async_copy(w_ref, out_ref.at[me, 0], local_sem.at[0]),
        pltpu.make_async_copy(p_ref, out_ref.at[me, 1], local_sem.at[1]),
    ]
    for c in own:
        c.start()

    counter = [0]
    sends = []

    def sem():
        counter[0] += 1
        return counter[0] - 1

    def send(src, dst, number, target):
        copy = pltpu.make_async_remote_copy(
            src_ref=src,
            dst_ref=dst,
            send_sem=send_sem.at[number],
            recv_sem=recv_sem.at[number],
            device_id=target,
            device_id_type=MESH,
        )
        copy.start()
        sends.append(copy)
        return copy

    def piece(tensor, origin, part=None):
        if part is None:
            return out_ref.at[origin, tensor]
        return out_ref.at[origin, tensor, pl.ds(part * HALF, HALF)]

    first = ("y", "z")
    second = ("z", "y")

    def origin_of(tensor, f, s):
        if tensor == 0:
            return index_of(wrap(z + s), wrap(y + f), core)
        return index_of(wrap(z + f), wrap(y + s), core)

    number = {}
    for tensor in (0, 1):
        for role in ("f+", "f-", "fa", "fb"):
            number[tensor, role] = sem()
        for f in (0, 1, -1, 2):
            for role in ("s+", "s-", "sa", "sb"):
                number[tensor, role, f] = sem()
        for f in (0, 1, -1, 2):
            for s in (0, 1, -1, 2):
                number[tensor, "sib", f, s] = sem()

    arrivals = {}

    def go(tensor, role, src_origin, axis, step, part=None, src=None):
        ref = piece(tensor, src_origin, part)
        copy = send(ref if src is None else src, ref, number[(tensor,) + role], at(axis, step))
        arrivals[(tensor,) + role] = copy

    def to_sib(tensor, f, s, src=None):
        origin = origin_of(tensor, f, s)
        ref = piece(tensor, origin)
        copy = send(ref if src is None else src, ref, number[tensor, "sib", f, s], {"fsdp": sib})
        arrivals[tensor, "sib", f, s] = copy

    mine = (w_ref, p_ref)
    for tensor in (0, 1):
        go(tensor, ("f+",), me, first[tensor], 1, src=mine[tensor])
        go(tensor, ("f-",), me, first[tensor], -1, src=mine[tensor])
    for tensor in (0, 1):
        go(tensor, ("s+", 0), me, second[tensor], 1, src=mine[tensor])
        go(tensor, ("s-", 0), me, second[tensor], -1, src=mine[tensor])
    for tensor in (0, 1):
        to_sib(tensor, 0, 0, src=mine[tensor])

    get_tokens.wait()

    def norm(i, carry):
        rows = pl.ds(pl.multiple_of(i * 32, 32), 32)
        x = tokens[rows, :].astype(F32)
        factor = lax.rsqrt(jnp.mean(x * x, axis=-1, keepdims=True) + EPS)
        normed[rows, :] = (x * factor * gain[...]).astype(BF16)
        return carry

    lax.fori_loop(0, LEN // 32, norm, 0)
    own.append(pltpu.make_async_copy(normed, normed_out, local_sem.at[3]))
    own[-1].start()

    for tensor in (0, 1):
        arrivals[tensor, "f+"].wait_recv()
        lower = origin_of(tensor, -1, 0)
        go(tensor, ("fa",), lower, first[tensor], 1, part=0)
        go(tensor, ("s+", -1), lower, second[tensor], 1)
        go(tensor, ("s-", -1), lower, second[tensor], -1)
        arrivals[tensor, "f-"].wait_recv()
        upper = origin_of(tensor, 1, 0)
        go(tensor, ("fb",), upper, first[tensor], -1, part=1)
        go(tensor, ("s+", 1), upper, second[tensor], 1)
        go(tensor, ("s-", 1), upper, second[tensor], -1)
        to_sib(tensor, -1, 0)
        to_sib(tensor, 1, 0)

    def pass_on(tensor, f):
        arrivals[tensor, "s+", f].wait_recv()
        go(tensor, ("sa", f), origin_of(tensor, f, -1), second[tensor], 1, part=0)
        to_sib(tensor, f, -1)
        arrivals[tensor, "s-", f].wait_recv()
        go(tensor, ("sb", f), origin_of(tensor, f, 1), second[tensor], -1, part=1)
        to_sib(tensor, f, 1)

    for tensor in (0, 1):
        pass_on(tensor, 0)
    for tensor in (0, 1):
        arrivals[tensor, "fa"].wait_recv()
        arrivals[tensor, "fb"].wait_recv()
        far = origin_of(tensor, 2, 0)
        go(tensor, ("s+", 2), far, second[tensor], 1)
        go(tensor, ("s-", 2), far, second[tensor], -1)
        to_sib(tensor, 2, 0)
    for f in (-1, 1, 2):
        for tensor in (0, 1):
            pass_on(tensor, f)
            if f == -1:
                g = 0
            elif f == 1:
                g = -1
            else:
                g = 1
            arrivals[tensor, "sa", g].wait_recv()
            arrivals[tensor, "sb", g].wait_recv()
            to_sib(tensor, g, 2)
    for tensor in (0, 1):
        arrivals[tensor, "sa", 2].wait_recv()
        arrivals[tensor, "sb", 2].wait_recv()
        to_sib(tensor, 2, 2)
    for key, copy in arrivals.items():
        if key[1] == "sib":
            copy.wait_recv()
    for c in own:
        c.wait()
    for copy in sends:
        copy.wait_send()


def gather(w, p, tokens, gain):
    vmem = pl.BlockSpec(memory_space=pltpu.VMEM)
    hbm = pl.BlockSpec(memory_space=pl.ANY)
    return pl.pallas_call(
        gather_kernel,
        out_shape=[
            jax.ShapeDtypeStruct((32, 2, SLOTS, BLK, BLK), BF16),
            jax.ShapeDtypeStruct((LEN, D), BF16),
        ],
        in_specs=[vmem, vmem, hbm, vmem],
        out_specs=[hbm, hbm],
        scratch_shapes=[
            pltpu.VMEM((LEN, D), BF16),
            pltpu.VMEM((LEN, D), BF16),
            pltpu.SemaphoreType.DMA((72,)),
            pltpu.SemaphoreType.DMA((72,)),
            pltpu.SemaphoreType.DMA((4,)),
        ],
        compiler_params=pltpu.CompilerParams(
            collective_id=0, has_side_effects=True, vmem_limit_bytes=VMEM_LIMIT
        ),
        name="gather",
    )(w, p, tokens, gain)


def nt(a, b):
    return lax.dot_general(a, b, (((1,), (1,)), ((), ())), preferred_element_type=F32)


def nn(a, b):
    return jnp.dot(a, b, preferred_element_type=F32)


def causal_mask():
    row = lax.broadcasted_iota(jnp.int32, (LEN, LEN), 0)
    col = lax.broadcasted_iota(jnp.int32, (LEN, LEN), 1)
    return row >= col


def forward_kernel(
    counts,
    cos,
    sin,
    normed_in,
    slots,
    qkv_out,
    sides_out,
    probs_out,
    wo_out,
    normed,
    wqkv,
    wout,
    proj,
    sides,
    probs,
    qkv,
    sem,
):
    get_normed = pltpu.make_async_copy(normed_in, normed, sem.at[2])
    get_normed.start()

    def device(d, start):
        n = counts[d]

        def one(t, carry):
            b = start + t

            @pl.when(b < NQKV)
            def _():
                r = pl.multiple_of((b // 6) * BLK, BLK)
                c = pl.multiple_of((b % 6) * BLK, BLK)
                pltpu.make_async_copy(
                    slots.at[d, :, t], wqkv.at[:, pl.ds(r, BLK), pl.ds(c, BLK)], sem.at[0]
                ).start()

            @pl.when(b >= NQKV)
            def _():
                e = b - NQKV
                j = e % 32
                r = pl.multiple_of((e // 32) * BLK, BLK)
                c = pl.multiple_of((j % 8) * BLK, BLK)
                pltpu.make_async_copy(
                    slots.at[d, :, t],
                    wout.at[j // 8, :, pl.ds(r, BLK), pl.ds(c, BLK)],
                    sem.at[1],
                ).start()

            return carry

        lax.fori_loop(0, n, one, 0)
        return start + n

    lax.fori_loop(0, 32, device, 0)
    get_normed.wait()
    pltpu.make_async_copy(wqkv, wqkv, sem.at[0]).wait()

    for tensor in (0, 1):
        for n in range(3):
            cols = slice(n * 256, (n + 1) * 256)
            proj[tensor, :, cols] = nn(normed[...], wqkv[tensor, :, cols])
    pltpu.make_async_copy(wout, wout, sem.at[1]).wait()
    save_wo = pltpu.make_async_copy(wout, wo_out, sem.at[6])
    save_wo.start()

    c2, s2 = cos[...], sin[...]

    def rot(x):
        return x * c2 + pltpu.roll(x, 64, 1) * s2

    def head(tensor, h):
        x = proj[tensor, :, h * HD : (h + 1) * HD]
        if h < QH + 1:
            x = rot(x)
        return x.astype(BF16)

    for h in range(QH + 2):
        qkv[:, h * HD : (h + 1) * HD] = head(0, h)
    save_qkv = pltpu.make_async_copy(qkv, qkv_out, sem.at[3])
    save_qkv.start()
    k = qkv[:, QH * HD : (QH + 1) * HD]
    v = qkv[:, (QH + 1) * HD :]
    keys = jnp.concatenate([k, head(1, QH)], axis=1)
    values = jnp.concatenate([v, head(1, QH + 1)], axis=1)
    causal = causal_mask()
    scale = HD**-0.5
    for h in range(QH):
        q = qkv[:, h * HD : (h + 1) * HD]
        tq = head(1, h)
        s = jnp.where(causal, nt(q, k) * scale, NEGATIVE)
        m = jnp.max(s, axis=-1, keepdims=True)
        e = jnp.exp(s - m)
        p = e * (1.0 / jnp.sum(e, axis=-1, keepdims=True))
        ts = nt(jnp.concatenate([tq, q], axis=1), keys) * scale
        pt = p * ts
        tp = pt - p * jnp.sum(pt, axis=-1, keepdims=True)
        pb = p.astype(BF16)
        probs[h] = pb
        both = nn(pb, values)
        mixed_t = nn(tp.astype(BF16), v) + both[:, HD:]
        sides[0, :, h * HD : (h + 1) * HD] = mixed_t.astype(BF16)
        sides[1, :, h * HD : (h + 1) * HD] = both[:, :HD].astype(BF16)
    save_probs = pltpu.make_async_copy(probs, probs_out, sem.at[4])
    save_probs.start()
    save_sides = pltpu.make_async_copy(sides, sides_out, sem.at[5])
    save_sides.start()
    for c in (save_wo, save_qkv, save_probs, save_sides):
        c.wait()


def forward(counts, cos, sin, normed, slots):
    vmem = pl.BlockSpec(memory_space=pltpu.VMEM)
    hbm = pl.BlockSpec(memory_space=pl.ANY)
    smem = pl.BlockSpec(memory_space=pltpu.SMEM)
    shape = jax.ShapeDtypeStruct
    return pl.pallas_call(
        forward_kernel,
        out_shape=[
            shape((LEN, QKV), BF16),
            shape((2, LEN, OUT), BF16),
            shape((QH, LEN, LEN), BF16),
            shape((4, 2, OUT, CHUNK), BF16),
        ],
        in_specs=[smem, vmem, vmem, hbm, hbm],
        out_specs=[hbm, hbm, hbm, hbm],
        scratch_shapes=[
            pltpu.VMEM((LEN, D), BF16),
            pltpu.VMEM((2, D, QKV), BF16),
            pltpu.VMEM((4, 2, OUT, CHUNK), BF16),
            pltpu.VMEM((2, LEN, QKV), F32),
            pltpu.VMEM((2, LEN, OUT), BF16),
            pltpu.VMEM((QH, LEN, LEN), BF16),
            pltpu.VMEM((LEN, QKV), BF16),
            pltpu.SemaphoreType.DMA((7,)),
        ],
        compiler_params=pltpu.CompilerParams(vmem_limit_bytes=VMEM_LIMIT),
        name="forward",
    )(counts, cos, sin, normed, slots)


FAR, NXT, PRV, OWN = 0, 1, 2, 3


def main_kernel(
    counts, cos, sin, sides_in, wo_in, curv_in, probs_in, qkv_in, normed_in,
    out,
    starts, sides, wo, curv, probs, qkv, normed,
    tan, opp, low, high, wt, dmix, dprojt, gb, sb,
    acc, r_far, r_low, r_high, red, t_far, t_low, t_high, fin,
    send_sem, recv_sem, local_sem,
):
    me, core, y, z = place()
    x = lax.axis_index("seq")
    sib = {"fsdp": index_of(z, y, 1 - core)}
    up, down = {"seq": wrap(x + 1)}, {"seq": wrap(x - 1)}

    def at(axis, step):
        if axis == "y":
            return {"fsdp": index_of(z, wrap(y + step), core)}
        return {"fsdp": index_of(wrap(z + step), y, core)}

    chunk = (wrap(x + 2), wrap(x + 1), wrap(x - 1), x)
    curv_cols = pl.ds(pl.multiple_of(x * CHUNK, CHUNK), CHUNK)
    loads = [
        pltpu.make_async_copy(a, b, local_sem.at[i])
        for i, (a, b) in enumerate(
            [(wo_in.at[chunk[rel]], wo.at[rel]) for rel in range(4)]
            + [
                (sides_in, sides),
                (curv_in.at[:, curv_cols], curv),
                (probs_in, probs),
                (qkv_in, qkv),
                (normed_in, normed),
            ]
        )
    ]
    for i in (4, 0, 1, 2, 3, 5, 6, 7, 8):
        loads[i].start()
    greet([up, down, at("y", 1), at("y", -1), at("z", 1), at("z", -1), sib])

    sends = []
    counter = [0]

    def send(src, dst, target):
        number = counter[0]
        counter[0] += 1
        copy = pltpu.make_async_remote_copy(
            src_ref=src,
            dst_ref=dst,
            send_sem=send_sem.at[number],
            recv_sem=recv_sem.at[number],
            device_id=target,
            device_id_type=MESH,
        )
        copy.start()
        sends.append(copy)
        return copy

    half = LEN // 2
    rows = (pl.ds(0, half), pl.ds(half, half))

    def term(rel, part):
        r = rows[part]
        tan[rel, r] = (nn(sides[0, r], wo[rel, 0]) + nn(sides[1, r], wo[rel, 1])).astype(BF16)

    loads[4].wait()
    loads[FAR].wait()
    term(FAR, 0)
    a0 = send(tan.at[FAR, rows[0]], opp.at[0], up)
    term(FAR, 1)
    b0 = send(tan.at[FAR, rows[1]], opp.at[1], down)
    loads[NXT].wait()
    term(NXT, 1)
    a1 = send(tan.at[NXT, rows[1]], low.at[1], up)
    loads[PRV].wait()
    term(PRV, 0)
    b1 = send(tan.at[PRV, rows[0]], high.at[0], down)
    term(NXT, 0)
    term(PRV, 1)
    loads[OWN].wait()
    term(OWN, 0)
    term(OWN, 1)
    a0.wait_recv()
    opp[0] = (opp[0].astype(F32) + tan[NXT, rows[0]].astype(F32)).astype(BF16)
    a2 = send(opp.at[0], low.at[0], up)
    b0.wait_recv()
    opp[1] = (opp[1].astype(F32) + tan[PRV, rows[1]].astype(F32)).astype(BF16)
    b2 = send(opp.at[1], high.at[1], down)
    loads[5].wait()

    def prefix(d, s):
        starts[d] = s
        return s + counts[d]

    lax.fori_loop(0, 32, prefix, 0)

    def weigh(part):
        r = rows[part]
        total = tan[OWN, r].astype(F32) + low[part].astype(F32) + high[part].astype(F32)
        wt[OWN, r] = (total * curv[r].astype(F32)).astype(BF16)

    def hand_on(src, dst, part, target):
        return send(wt.at[src, rows[part]], wt.at[dst, rows[part]], target)

    a1.wait_recv()
    b2.wait_recv()
    weigh(1)
    c1 = hand_on(OWN, PRV, 1, up)
    d1 = hand_on(OWN, NXT, 1, down)
    b1.wait_recv()
    a2.wait_recv()
    weigh(0)
    d0 = hand_on(OWN, NXT, 0, down)
    c0 = hand_on(OWN, PRV, 0, up)

    mixedt = sides[1].T

    def consume(rel):
        part = nt(wt[rel], wo[rel, 0])
        if rel == OWN:
            dmix[...] = part
        else:
            dmix[...] += part
        g = nn(mixedt, wt[rel]).astype(BF16)
        for i in range(4):
            for j in range(8):
                gb[j % 2, NQKV // 2 + 16 * i + 4 * chunk[rel] + j // 2] = g[
                    i * BLK : (i + 1) * BLK, j * BLK : (j + 1) * BLK
                ]

    consume(OWN)
    c1.wait_recv()
    e1 = hand_on(PRV, FAR, 1, up)
    d1.wait_recv()
    d0.wait_recv()
    e0 = hand_on(NXT, FAR, 0, down)
    consume(NXT)
    c0.wait_recv()
    consume(PRV)
    e1.wait_recv()
    e0.wait_recv()
    consume(FAR)
    n_out = NB // 2 - NQKV // 2
    out_part = pl.ds(NQKV // 2, n_out)
    swap_out = send(gb.at[1 - core, out_part], sb.at[out_part], sib)

    for i in (6, 7, 8):
        loads[i].wait()
    c2, s2 = cos[...], sin[...]

    def unrot(x):
        return x * c2 - pltpu.roll(x, 64, 1) * s2

    k = qkv[:, QH * HD : (QH + 1) * HD]
    v = qkv[:, (QH + 1) * HD :]
    scale = HD**-0.5
    dkt = jnp.zeros((HD, LEN), F32)
    dvt = jnp.zeros((HD, LEN), F32)
    for h in range(QH):
        dm = dmix[:, h * HD : (h + 1) * HD].astype(BF16)
        q = qkv[:, h * HD : (h + 1) * HD]
        pb = probs[h]
        dp = nt(dm, v).astype(BF16).astype(F32)
        dvt = dvt + nn(dm.T, pb)
        pf = pb.astype(F32)
        pd = pf * dp
        ds = ((pd - pf * jnp.sum(pd, axis=-1, keepdims=True)) * scale).astype(BF16)
        dkt = dkt + nn(q.T, ds)
        dq = unrot(nn(ds, k).astype(BF16).astype(F32)).astype(BF16)
        dprojt[h * HD : (h + 1) * HD, :] = dq.T
    dk = unrot(dkt.astype(BF16).astype(F32).T).astype(BF16)
    dprojt[QH * HD : (QH + 1) * HD, :] = dk.T
    dprojt[(QH + 1) * HD :, :] = dvt.astype(BF16)

    def add_sibling(base, count):
        def step(i, carry):
            b = base + i * 4
            gb[core, pl.ds(b, 4)] = (
                gb[core, pl.ds(b, 4)].astype(F32) + sb[pl.ds(b, 4)].astype(F32)
            ).astype(BF16)
            return carry

        lax.fori_loop(0, count // 4, step, 0)

    swaps = []
    for n in range(8):
        cols = slice(n * 512, (n + 1) * 512)
        g = nn(dprojt[...], normed[:, cols]).astype(BF16)
        for r in range(4):
            for c in range(6):
                gb[c % 2, 3 * (4 * n + r) + c // 2] = g[
                    c * BLK : (c + 1) * BLK, r * BLK : (r + 1) * BLK
                ]
        piece = pl.ds(12 * n, 12)
        swaps.append(send(gb.at[1 - core, piece], sb.at[piece], sib))
    swap_out.wait_recv()
    add_sibling(NQKV // 2, n_out)
    for n in range(8):
        swaps[n].wait_recv()
        add_sibling(12 * n, 12)

    first = ("z", "y")
    second = ("y", "z")
    here = {"y": y, "z": z}
    steps = (2, 1, -1, 0)

    def fill(part, rel):
        f = wrap(here[first[part]] + steps[rel])

        def step(s, carry):
            if part == 0:
                d = index_of(f, s, part)
            else:
                d = index_of(s, f, part)
            base = (starts[d] + 1 - core) // 2
            for i in range(HALF):
                acc[part, rel, s, i] = gb[core, jnp.minimum(base + i, NB // 2 - 1)]
            return carry

        lax.fori_loop(0, 4, step, 0)

    lo, hi = pl.ds(0, 3), pl.ds(3, 3)
    a = {}
    for part in (0, 1):
        fill(part, FAR)
        a[part, "fu"] = send(acc.at[part, FAR, :, lo], r_far.at[part, 0], at(first[part], 1))
        a[part, "fd"] = send(acc.at[part, FAR, :, hi], r_far.at[part, 1], at(first[part], -1))
    for part in (0, 1):
        fill(part, NXT)
        a[part, "lo1"] = send(acc.at[part, NXT, :, hi], r_low.at[part, 1], at(first[part], 1))
    for part in (0, 1):
        fill(part, PRV)
        a[part, "hi0"] = send(acc.at[part, PRV, :, lo], r_high.at[part, 0], at(first[part], -1))
    for part in (0, 1):
        fill(part, OWN)
    for part in (0, 1):
        for p, name, rel, span, name2, dst, step_to in (
            (0, "fu", NXT, lo, "lo0", r_low, 1),
            (1, "fd", PRV, hi, "hi1", r_high, -1),
        ):
            a[part, name].wait_recv()

            def step(s, carry, part=part, p=p, rel=rel, span=span):
                r_far[part, p, s] = (
                    r_far[part, p, s].astype(F32) + acc[part, rel, s, span].astype(F32)
                ).astype(BF16)
                return carry

            lax.fori_loop(0, 4, step, 0)
            a[part, name2] = send(r_far.at[part, p], dst.at[part, p], at(first[part], step_to))
    for part in (0, 1):
        for name in ("lo1", "hi0", "lo0", "hi1"):
            a[part, name].wait_recv()
        for h in (0, 1):

            def step3(s, carry, part=part, h=h):
                red[part, s, pl.ds(3 * h, 3)] = (
                    acc[part, OWN, s, pl.ds(3 * h, 3)].astype(F32)
                    + r_low[part, h, s].astype(F32)
                    + r_high[part, h, s].astype(F32)
                ).astype(BF16)
                return carry

            lax.fori_loop(0, 4, step3, 0)
        s_here = here[second[part]]
        far, nxt, prv = wrap(s_here + 2), wrap(s_here + 1), wrap(s_here - 1)
        to_up, to_down = at(second[part], 1), at(second[part], -1)
        a[part, "tu"] = send(red.at[part, far, lo], t_far.at[part, 0], to_up)
        a[part, "td"] = send(red.at[part, far, hi], t_far.at[part, 1], to_down)
        a[part, "tl1"] = send(red.at[part, nxt, hi], t_low.at[part, 1], to_up)
        a[part, "th0"] = send(red.at[part, prv, lo], t_high.at[part, 0], to_down)
    for part in (0, 1):
        s_here = here[second[part]]
        nxt, prv = wrap(s_here + 1), wrap(s_here - 1)
        to_up, to_down = at(second[part], 1), at(second[part], -1)
        a[part, "tu"].wait_recv()
        t_far[part, 0] = (t_far[part, 0].astype(F32) + red[part, nxt, lo].astype(F32)).astype(BF16)
        a[part, "tl0"] = send(t_far.at[part, 0], t_low.at[part, 0], to_up)
        a[part, "td"].wait_recv()
        t_far[part, 1] = (t_far[part, 1].astype(F32) + red[part, prv, hi].astype(F32)).astype(BF16)
        a[part, "th1"] = send(t_far.at[part, 1], t_high.at[part, 1], to_down)
    for part in (0, 1):
        s_here = here[second[part]]
        for name in ("tl1", "th0", "tl0", "th1"):
            a[part, name].wait_recv()
        for h in (0, 1):
            fin[part, pl.ds(3 * h, 3)] = (
                red[part, s_here, pl.ds(3 * h, 3)].astype(F32)
                + t_low[part, h].astype(F32)
                + t_high[part, h].astype(F32)
            )
    last = send(fin.at[1 - core], out.at[core], sib)
    out[core] = fin[core]
    last.wait_recv()
    for copy in sends:
        copy.wait_send()


def main(counts, cos, sin, sides, wo, curv, probs, qkv, normed):
    vmem = pl.BlockSpec(memory_space=pltpu.VMEM)
    hbm = pl.BlockSpec(memory_space=pl.ANY)
    smem = pl.BlockSpec(memory_space=pltpu.SMEM)
    block = (BLK, BLK)
    half = LEN // 2
    v = pltpu.VMEM
    return pl.pallas_call(
        main_kernel,
        out_shape=jax.ShapeDtypeStruct((2, HALF) + block, F32),
        in_specs=[smem, vmem, vmem] + [hbm] * 6,
        out_specs=vmem,
        scratch_shapes=[
            pltpu.SMEM((32,), jnp.int32),
            v((2, LEN, OUT), BF16),
            v((4, 2, OUT, CHUNK), BF16),
            v((LEN, CHUNK), BF16),
            v((QH, LEN, LEN), BF16),
            v((LEN, QKV), BF16),
            v((LEN, D), BF16),
            v((4, LEN, CHUNK), BF16),
            v((2, half, CHUNK), BF16),
            v((2, half, CHUNK), BF16),
            v((2, half, CHUNK), BF16),
            v((4, LEN, CHUNK), BF16),
            v((LEN, OUT), F32),
            v((QKV, LEN), BF16),
            v((2, NB // 2) + block, BF16),
            v((NB // 2,) + block, BF16),
            v((2, 4, 4, HALF) + block, BF16),
            v((2, 2, 4, 3) + block, BF16),
            v((2, 2, 4, 3) + block, BF16),
            v((2, 2, 4, 3) + block, BF16),
            v((2, 4, HALF) + block, BF16),
            v((2, 2, 3) + block, BF16),
            v((2, 2, 3) + block, BF16),
            v((2, 2, 3) + block, BF16),
            v((2, HALF) + block, F32),
            pltpu.SemaphoreType.DMA((64,)),
            pltpu.SemaphoreType.DMA((64,)),
            pltpu.SemaphoreType.DMA((9,)),
        ],
        compiler_params=pltpu.CompilerParams(
            collective_id=1, has_side_effects=True, vmem_limit_bytes=67_000_000
        ),
        name="main",
    )(counts, cos, sin, sides, wo, curv, probs, qkv, normed)


def finish_kernel(counts, total, out):
    me = lax.axis_index("fsdp")
    start = lax.fori_loop(0, me, lambda d, s: s + counts[d], 0)
    n = counts[me]
    factor = 1.0 / np.sqrt(np.float32(LEN * 32))

    def one(t, carry):
        b = start + t
        parity = b % 2
        x = total[parity, b // 2 - (start + 1 - parity) // 2] * factor
        x = jnp.where(b < NQKV, x.T, x)
        out[t] = jnp.where(t < n, x, 0.0)
        return carry

    lax.fori_loop(0, SLOTS, one, 0)


def finish(counts, total):
    vmem = pl.BlockSpec(memory_space=pltpu.VMEM)
    smem = pl.BlockSpec(memory_space=pltpu.SMEM)
    return pl.pallas_call(
        finish_kernel,
        out_shape=jax.ShapeDtypeStruct((SLOTS, BLK, BLK), F32),
        in_specs=[smem, vmem],
        out_specs=vmem,
        name="finish",
    )(counts, total)


def local(tokens, norm_gain, curvature, weight_slots, probe_slots, block_counts):
    counts = block_counts[0]
    cos, sin = tables()
    slots, normed = gather(weight_slots[0], probe_slots[0], tokens[0], norm_gain.reshape(1, D))
    qkv, sides, probs, wo = forward(counts, cos, sin, normed, slots)
    total = main(counts, cos, sin, sides, wo, curvature[0], probs, qkv, normed)
    return finish(counts, total)[None]


def solution(mesh):
    in_specs = (
        P("fsdp", None, None),
        P(),
        P("fsdp", None, None),
        P("seq", "fsdp", None, None),
        P("seq", "fsdp", None, None),
        P("seq", None),
    )
    out_specs = P("seq", "fsdp", None, None)
    return jax.shard_map(local, mesh=mesh, in_specs=in_specs, out_specs=out_specs, check_vma=False)
```

```python
import functools

import jax
import jax.numpy as jnp
import numpy as np
from jax import lax
from jax.experimental import pallas as pl
from jax.experimental.pallas import tpu as pltpu
from jax.sharding import PartitionSpec as P

D = 4096
HD = 128
BLK = 128
LEN = 512
QH = 4
QKV = 768
OUT = 512
NQKV = 192
NB = 320
SLOTS = 12
HALF = 6
CHUNK = 1024
SUB = 512
THETA = 500000.0
EPS = 1e-05
NEGATIVE = -1e30
VMEM_LIMIT = 66_000_000
MESH = pl.DeviceIdType.MESH
F32 = jnp.float32
BF16 = jnp.bfloat16


def tables():
    half = HD // 2
    frequency = np.exp(-np.log(THETA) * 2.0 * np.arange(half) / HD)
    angles = np.arange(LEN)[:, None] * frequency[None, :]
    c, s = np.cos(angles), np.sin(angles)
    return (
        np.concatenate([c, c], axis=1).astype(np.float32),
        np.concatenate([-s, s], axis=1).astype(np.float32),
    )


def place():
    me = lax.axis_index("fsdp")
    core = lax.rem(me, 2)
    y = lax.rem(me // 2, 4)
    z = me // 8
    return me, core, y, z


def index_of(z, y, core):
    return (z * 4 + y) * 2 + core


def wrap(a):
    return lax.rem(a + 4, 4)


def greet(targets):
    barrier = pltpu.get_barrier_semaphore()
    for t in targets:
        pl.semaphore_signal(barrier, inc=1, device_id=t, device_id_type=MESH)
    pl.semaphore_wait(barrier, len(targets))


def gather_kernel(
    counts, w_ref, p_ref, tokens_in, gain, out_ref, normed_out, table,
    tokens, normed, send_sem, recv_sem, local_sem,
):
    me, core, y, z = place()
    get_tokens = pltpu.make_async_copy(tokens_in, tokens, local_sem.at[2])
    get_tokens.start()
    sib = index_of(z, y, 1 - core)

    def at(axis, step):
        if axis == "y":
            return {"fsdp": index_of(z, wrap(y + step), core)}
        return {"fsdp": index_of(wrap(z + step), y, core)}

    greet([at("y", 1), at("y", -1), at("z", 1), at("z", -1), {"fsdp": sib}])

    own = [
        pltpu.make_async_copy(w_ref, out_ref.at[0, pl.ds(me * SLOTS, SLOTS)], local_sem.at[0]),
        pltpu.make_async_copy(p_ref, out_ref.at[1, pl.ds(me * SLOTS, SLOTS)], local_sem.at[1]),
    ]
    for c in own:
        c.start()

    counter = [0]
    sends = []

    def sem():
        counter[0] += 1
        return counter[0] - 1

    def send(src, dst, number, target):
        copy = pltpu.make_async_remote_copy(
            src_ref=src,
            dst_ref=dst,
            send_sem=send_sem.at[number],
            recv_sem=recv_sem.at[number],
            device_id=target,
            device_id_type=MESH,
        )
        copy.start()
        sends.append(copy)
        return copy

    def piece(tensor, origin, part=None):
        if part is None:
            return out_ref.at[tensor, pl.ds(origin * SLOTS, SLOTS)]
        return out_ref.at[tensor, pl.ds(origin * SLOTS + part * HALF, HALF)]

    first = ("y", "z")
    second = ("z", "y")

    def origin_of(tensor, f, s):
        if tensor == 0:
            return index_of(wrap(z + s), wrap(y + f), core)
        return index_of(wrap(z + f), wrap(y + s), core)

    number = {}
    for tensor in (0, 1):
        for role in ("f+", "f-", "fa", "fb"):
            number[tensor, role] = sem()
        for f in (0, 1, -1, 2):
            for role in ("s+", "s-", "sa", "sb"):
                number[tensor, role, f] = sem()
        for f in (0, 1, -1, 2):
            for s in (0, 1, -1, 2):
                number[tensor, "sib", f, s] = sem()

    arrivals = {}

    def go(tensor, role, src_origin, axis, step, part=None, src=None):
        ref = piece(tensor, src_origin, part)
        copy = send(ref if src is None else src, ref, number[(tensor,) + role], at(axis, step))
        arrivals[(tensor,) + role] = copy

    def to_sib(tensor, f, s, src=None):
        origin = origin_of(tensor, f, s)
        ref = piece(tensor, origin)
        copy = send(ref if src is None else src, ref, number[tensor, "sib", f, s], {"fsdp": sib})
        arrivals[tensor, "sib", f, s] = copy

    mine = (w_ref, p_ref)
    for tensor in (0, 1):
        go(tensor, ("f+",), me, first[tensor], 1, src=mine[tensor])
        go(tensor, ("f-",), me, first[tensor], -1, src=mine[tensor])
    for tensor in (0, 1):
        go(tensor, ("s+", 0), me, second[tensor], 1, src=mine[tensor])
        go(tensor, ("s-", 0), me, second[tensor], -1, src=mine[tensor])
    for tensor in (0, 1):
        to_sib(tensor, 0, 0, src=mine[tensor])

    b = lax.broadcasted_iota(jnp.int32, (8, 128), 0) * 128 + lax.broadcasted_iota(
        jnp.int32, (8, 128), 1
    )
    slot, end = b, 0
    for d in range(32):
        end = end + counts[d]
        slot = slot + jnp.where(b >= end, SLOTS - counts[d], 0)
    table[...] = slot
    get_tokens.wait()

    def norm(i, carry):
        rows = pl.ds(pl.multiple_of(i * 32, 32), 32)
        x = tokens[rows, :].astype(F32)
        factor = lax.rsqrt(jnp.mean(x * x, axis=-1, keepdims=True) + EPS)
        normed[rows, :] = (x * factor * gain[...]).astype(BF16)
        return carry

    lax.fori_loop(0, LEN // 32, norm, 0)
    own.append(pltpu.make_async_copy(normed, normed_out, local_sem.at[3]))
    own[-1].start()

    for tensor in (0, 1):
        arrivals[tensor, "f+"].wait_recv()
        lower = origin_of(tensor, -1, 0)
        go(tensor, ("fa",), lower, first[tensor], 1, part=0)
        go(tensor, ("s+", -1), lower, second[tensor], 1)
        go(tensor, ("s-", -1), lower, second[tensor], -1)
        arrivals[tensor, "f-"].wait_recv()
        upper = origin_of(tensor, 1, 0)
        go(tensor, ("fb",), upper, first[tensor], -1, part=1)
        go(tensor, ("s+", 1), upper, second[tensor], 1)
        go(tensor, ("s-", 1), upper, second[tensor], -1)
        to_sib(tensor, -1, 0)
        to_sib(tensor, 1, 0)

    def pass_on(tensor, f):
        arrivals[tensor, "s+", f].wait_recv()
        go(tensor, ("sa", f), origin_of(tensor, f, -1), second[tensor], 1, part=0)
        to_sib(tensor, f, -1)
        arrivals[tensor, "s-", f].wait_recv()
        go(tensor, ("sb", f), origin_of(tensor, f, 1), second[tensor], -1, part=1)
        to_sib(tensor, f, 1)

    for tensor in (0, 1):
        pass_on(tensor, 0)
    for tensor in (0, 1):
        arrivals[tensor, "fa"].wait_recv()
        arrivals[tensor, "fb"].wait_recv()
        far = origin_of(tensor, 2, 0)
        go(tensor, ("s+", 2), far, second[tensor], 1)
        go(tensor, ("s-", 2), far, second[tensor], -1)
        to_sib(tensor, 2, 0)
    for f in (-1, 1, 2):
        for tensor in (0, 1):
            pass_on(tensor, f)
            if f == -1:
                g = 0
            elif f == 1:
                g = -1
            else:
                g = 1
            arrivals[tensor, "sa", g].wait_recv()
            arrivals[tensor, "sb", g].wait_recv()
            to_sib(tensor, g, 2)
    for tensor in (0, 1):
        arrivals[tensor, "sa", 2].wait_recv()
        arrivals[tensor, "sb", 2].wait_recv()
        to_sib(tensor, 2, 2)
    for key, copy in arrivals.items():
        if key[1] == "sib":
            copy.wait_recv()
    for c in own:
        c.wait()
    for copy in sends:
        copy.wait_send()


def gather(counts, w, p, tokens, gain):
    vmem = pl.BlockSpec(memory_space=pltpu.VMEM)
    hbm = pl.BlockSpec(memory_space=pl.ANY)
    smem = pl.BlockSpec(memory_space=pltpu.SMEM)
    return pl.pallas_call(
        gather_kernel,
        out_shape=[
            jax.ShapeDtypeStruct((2, 32 * SLOTS, BLK, BLK), BF16),
            jax.ShapeDtypeStruct((LEN, D), BF16),
            jax.ShapeDtypeStruct((8, 128), jnp.int32),
        ],
        in_specs=[smem, vmem, vmem, hbm, vmem],
        out_specs=[hbm, hbm, vmem],
        scratch_shapes=[
            pltpu.VMEM((LEN, D), BF16),
            pltpu.VMEM((LEN, D), BF16),
            pltpu.SemaphoreType.DMA((72,)),
            pltpu.SemaphoreType.DMA((72,)),
            pltpu.SemaphoreType.DMA((4,)),
        ],
        compiler_params=pltpu.CompilerParams(
            collective_id=0, has_side_effects=True, vmem_limit_bytes=VMEM_LIMIT
        ),
        name="gather",
    )(counts, w, p, tokens, gain)


def nt(a, b):
    return lax.dot_general(a, b, (((1,), (1,)), ((), ())), preferred_element_type=F32)


def nn(a, b):
    return jnp.dot(a, b, preferred_element_type=F32)


def causal_mask():
    row = lax.broadcasted_iota(jnp.int32, (LEN, LEN), 0)
    col = lax.broadcasted_iota(jnp.int32, (LEN, LEN), 1)
    return row >= col


def forward_kernel(
    table,
    cos,
    sin,
    normed_in,
    slots,
    qkv_out,
    sides_out,
    probs_out,
    wo_out,
    normed,
    wqkv,
    wout,
    proj,
    sides,
    probs,
    qkv,
    sem,
):
    get_normed = pltpu.make_async_copy(normed_in, normed, sem.at[7])
    get_normed.start()

    for pair in range(3):

        def rows(r, carry, pair=pair):
            for c in range(2):
                slot = table[r * 6 + 2 * pair + c]
                pltpu.make_async_copy(
                    slots.at[:, slot],
                    wqkv.at[pair, :, pl.ds(pl.multiple_of(r * BLK, BLK), BLK), c * BLK : (c + 1) * BLK],
                    sem.at[pair],
                ).start()
            return carry

        lax.fori_loop(0, 32, rows, 0, unroll=4)

    def project(pair):
        pltpu.make_async_copy(wqkv.at[pair], wqkv.at[pair], sem.at[pair]).wait()
        for tensor in (0, 1):
            proj[tensor, :, pair * 256 : (pair + 1) * 256] = nn(normed[...], wqkv[pair, tensor])

    get_normed.wait()
    project(0)

    def out_rows(i, carry):
        for j in range(32):
            slot = table[NQKV + i * 32 + j]
            pltpu.make_async_copy(
                slots.at[:, slot],
                wout.at[
                    j // 8,
                    :,
                    pl.ds(pl.multiple_of(i * BLK, BLK), BLK),
                    (j % 8) * BLK : (j % 8 + 1) * BLK,
                ],
                sem.at[3],
            ).start()
        return carry

    lax.fori_loop(0, 4, out_rows, 0)
    project(1)
    project(2)
    pltpu.make_async_copy(wout, wout, sem.at[3]).wait()
    save_wo = pltpu.make_async_copy(wout, wo_out, sem.at[6])
    save_wo.start()

    c2, s2 = cos[...], sin[...]

    def rot(x):
        return x * c2 + pltpu.roll(x, 64, 1) * s2

    def head(tensor, h):
        x = proj[tensor, :, h * HD : (h + 1) * HD]
        if h < QH + 1:
            x = rot(x)
        return x.astype(BF16)

    for h in range(QH + 2):
        qkv[:, h * HD : (h + 1) * HD] = head(0, h)
    save_qkv = pltpu.make_async_copy(qkv, qkv_out, sem.at[8])
    save_qkv.start()
    k = qkv[:, QH * HD : (QH + 1) * HD]
    v = qkv[:, (QH + 1) * HD :]
    keys = jnp.concatenate([k, head(1, QH)], axis=1)
    values = jnp.concatenate([v, head(1, QH + 1)], axis=1)
    causal = causal_mask()
    scale = HD**-0.5
    for h in range(QH):
        q = qkv[:, h * HD : (h + 1) * HD]
        tq = head(1, h)
        s = jnp.where(causal, nt(q, k) * scale, NEGATIVE)
        m = jnp.max(s, axis=-1, keepdims=True)
        e = jnp.exp(s - m)
        p = e * (1.0 / jnp.sum(e, axis=-1, keepdims=True))
        ts = nt(jnp.concatenate([tq, q], axis=1), keys) * scale
        pt = p * ts
        tp = pt - p * jnp.sum(pt, axis=-1, keepdims=True)
        pb = p.astype(BF16)
        probs[h] = pb
        both = nn(pb, values)
        mixed_t = nn(tp.astype(BF16), v) + both[:, HD:]
        sides[0, :, h * HD : (h + 1) * HD] = mixed_t.astype(BF16)
        sides[1, :, h * HD : (h + 1) * HD] = both[:, :HD].astype(BF16)
    save_probs = pltpu.make_async_copy(probs, probs_out, sem.at[4])
    save_probs.start()
    save_sides = pltpu.make_async_copy(sides, sides_out, sem.at[5])
    save_sides.start()
    for c in (save_wo, save_qkv, save_probs, save_sides):
        c.wait()


def forward(table, cos, sin, normed, slots):
    vmem = pl.BlockSpec(memory_space=pltpu.VMEM)
    hbm = pl.BlockSpec(memory_space=pl.ANY)
    smem = pl.BlockSpec(memory_space=pltpu.SMEM)
    shape = jax.ShapeDtypeStruct
    return pl.pallas_call(
        forward_kernel,
        out_shape=[
            shape((LEN, QKV), BF16),
            shape((2, LEN, OUT), BF16),
            shape((QH, LEN, LEN), BF16),
            shape((4, 2, OUT, CHUNK), BF16),
        ],
        in_specs=[smem, vmem, vmem, hbm, hbm],
        out_specs=[hbm, hbm, hbm, hbm],
        scratch_shapes=[
            pltpu.VMEM((LEN, D), BF16),
            pltpu.VMEM((3, 2, D, 256), BF16),
            pltpu.VMEM((4, 2, OUT, CHUNK), BF16),
            pltpu.VMEM((2, LEN, QKV), F32),
            pltpu.VMEM((2, LEN, OUT), BF16),
            pltpu.VMEM((QH, LEN, LEN), BF16),
            pltpu.VMEM((LEN, QKV), BF16),
            pltpu.SemaphoreType.DMA((9,)),
        ],
        compiler_params=pltpu.CompilerParams(vmem_limit_bytes=VMEM_LIMIT),
        name="forward",
    )(table, cos, sin, normed, slots)


FAR, NXT, PRV, OWN = 0, 1, 2, 3


def main_kernel(
    counts, cos, sin, sides_in, wo_in, curv_in, probs_in, qkv_in, normed_in,
    out,
    starts, sides, wo, curv, probs, qkv, normed,
    tan, opp, low, high, wt, dmix, dprojt, gb, sb,
    acc, r_far, r_low, r_high, red, t_far, t_low, t_high, fin, tot,
    send_sem, recv_sem, local_sem,
):
    me, core, y, z = place()
    x = lax.axis_index("seq")
    sib = {"fsdp": index_of(z, y, 1 - core)}
    up, down = {"seq": wrap(x + 1)}, {"seq": wrap(x - 1)}

    def at(axis, step):
        if axis == "y":
            return {"fsdp": index_of(z, wrap(y + step), core)}
        return {"fsdp": index_of(wrap(z + step), y, core)}

    chunk = (wrap(x + 2), wrap(x + 1), wrap(x - 1), x)
    curv_cols = pl.ds(pl.multiple_of(x * CHUNK, CHUNK), CHUNK)
    loads = [
        pltpu.make_async_copy(a, b, local_sem.at[i])
        for i, (a, b) in enumerate(
            [(wo_in.at[chunk[rel]], wo.at[rel]) for rel in range(4)]
            + [
                (sides_in, sides),
                (curv_in.at[:, curv_cols], curv),
                (probs_in, probs),
                (qkv_in, qkv),
                (normed_in, normed),
            ]
        )
    ]
    for i in (4, 0, 1, 2, 3, 5, 6, 7, 8):
        loads[i].start()
    greet([up, down, at("y", 1), at("y", -1), at("z", 1), at("z", -1), sib])

    sends = []
    counter = [0]

    def send(src, dst, target):
        number = counter[0]
        counter[0] += 1
        copy = pltpu.make_async_remote_copy(
            src_ref=src,
            dst_ref=dst,
            send_sem=send_sem.at[number],
            recv_sem=recv_sem.at[number],
            device_id=target,
            device_id_type=MESH,
        )
        copy.start()
        sends.append(copy)
        return copy

    def prefix(d, s):
        starts[d] = s
        return s + counts[d]

    lax.fori_loop(0, 32, prefix, 0)

    half = LEN // 2
    rows = (pl.ds(0, half), pl.ds(half, half))

    def term(rel, part, s):
        r = rows[part]
        cols = slice(s * SUB, (s + 1) * SUB)
        tan[rel, s, r] = (
            nn(sides[0, r], wo[rel, 0, :, cols]) + nn(sides[1, r], wo[rel, 1, :, cols])
        ).astype(BF16)

    a0, a1, a2, b0, b1, b2 = {}, {}, {}, {}, {}, {}
    loads[4].wait()
    loads[FAR].wait()
    for s in (0, 1):
        term(FAR, 0, s)
        a0[s] = send(tan.at[FAR, s, rows[0]], opp.at[0, s], up)
        term(FAR, 1, s)
        b0[s] = send(tan.at[FAR, s, rows[1]], opp.at[1, s], down)
        if s == 0:
            loads[NXT].wait()
            term(NXT, 1, s)
            a1[s] = send(tan.at[NXT, s, rows[1]], low.at[1, s], up)
            loads[PRV].wait()
            term(PRV, 0, s)
            b1[s] = send(tan.at[PRV, s, rows[0]], high.at[0, s], down)
    term(NXT, 0, 0)
    term(PRV, 1, 0)
    term(NXT, 1, 1)
    term(PRV, 0, 1)
    term(NXT, 0, 1)
    term(PRV, 1, 1)
    loads[OWN].wait()
    for s in (0, 1):
        for part in (0, 1):
            term(OWN, part, s)
    for s in (0, 1):
        a0[s].wait_recv()
        opp[0, s] = (opp[0, s].astype(F32) + tan[NXT, s, rows[0]].astype(F32)).astype(BF16)
        a2[s] = send(opp.at[0, s], low.at[0, s], up)
        b0[s].wait_recv()
        opp[1, s] = (opp[1, s].astype(F32) + tan[PRV, s, rows[1]].astype(F32)).astype(BF16)
        b2[s] = send(opp.at[1, s], high.at[1, s], down)
        if s == 0:
            a1[1] = send(tan.at[NXT, 1, rows[1]], low.at[1, 1], up)
            b1[1] = send(tan.at[PRV, 1, rows[0]], high.at[0, 1], down)
    loads[5].wait()

    def weigh(part, s):
        r = rows[part]
        total = tan[OWN, s, r].astype(F32) + low[part, s].astype(F32) + high[part, s].astype(F32)
        c = curv[r, s * SUB : (s + 1) * SUB].astype(F32)
        wt[OWN, s, r] = (total * c).astype(BF16)

    def hand_on(src, dst, part, s, target):
        return send(wt.at[src, s, rows[part]], wt.at[dst, s, rows[part]], target)

    mixedt = sides[1].T

    def consume(rel, s):
        part = nt(wt[rel, s], wo[rel, 0, :, s * SUB : (s + 1) * SUB])
        if rel == OWN and s == 0:
            dmix[...] = part
        else:
            dmix[...] += part
        g = nn(mixedt, wt[rel, s]).astype(BF16)
        for i in range(4):
            for j in range(4):
                gb[j % 2, NQKV // 2 + 16 * i + 4 * chunk[rel] + 2 * s + j // 2] = g[
                    i * BLK : (i + 1) * BLK, j * BLK : (j + 1) * BLK
                ]

    c0, c1, d0, d1, e0, e1 = {}, {}, {}, {}, {}, {}
    for s in (0, 1):
        a1[s].wait_recv()
        b2[s].wait_recv()
        weigh(1, s)
        c1[s] = hand_on(OWN, PRV, 1, s, up)
        d1[s] = hand_on(OWN, NXT, 1, s, down)
        b1[s].wait_recv()
        a2[s].wait_recv()
        weigh(0, s)
        d0[s] = hand_on(OWN, NXT, 0, s, down)
        c0[s] = hand_on(OWN, PRV, 0, s, up)
        if s == 0:
            consume(OWN, 0)
    for s in (0, 1):
        c1[s].wait_recv()
        e1[s] = hand_on(PRV, FAR, 1, s, up)
        d0[s].wait_recv()
        e0[s] = hand_on(NXT, FAR, 0, s, down)
        if s == 0:
            consume(OWN, 1)
        d1[s].wait_recv()
        consume(NXT, s)
        c0[s].wait_recv()
        consume(PRV, s)
    for s in (0, 1):
        e1[s].wait_recv()
        e0[s].wait_recv()
        consume(FAR, s)
    n_out = NB // 2 - NQKV // 2
    out_part = pl.ds(NQKV // 2, n_out)
    swap_out = send(gb.at[1 - core, out_part], sb.at[out_part], sib)

    for i in (6, 7, 8):
        loads[i].wait()
    c2, s2 = cos[...], sin[...]

    def unrot(x):
        return x * c2 - pltpu.roll(x, 64, 1) * s2

    k = qkv[:, QH * HD : (QH + 1) * HD]
    v = qkv[:, (QH + 1) * HD :]
    scale = HD**-0.5
    dkt = jnp.zeros((HD, LEN), F32)
    dvt = jnp.zeros((HD, LEN), F32)
    for h in range(QH):
        dm = dmix[:, h * HD : (h + 1) * HD].astype(BF16)
        q = qkv[:, h * HD : (h + 1) * HD]
        pb = probs[h]
        dp = nt(dm, v).astype(BF16).astype(F32)
        dvt = dvt + nn(dm.T, pb)
        pf = pb.astype(F32)
        pd = pf * dp
        ds = ((pd - pf * jnp.sum(pd, axis=-1, keepdims=True)) * scale).astype(BF16)
        dkt = dkt + nn(q.T, ds)
        dq = unrot(nn(ds, k).astype(BF16).astype(F32)).astype(BF16)
        dprojt[h * HD : (h + 1) * HD, :] = dq.T
    dk = unrot(dkt.astype(BF16).astype(F32).T).astype(BF16)
    dprojt[QH * HD : (QH + 1) * HD, :] = dk.T
    dprojt[(QH + 1) * HD :, :] = dvt.astype(BF16)

    swaps = [swap_out]
    for n in range(8):
        cols = slice(n * 512, (n + 1) * 512)
        g = nn(dprojt[...], normed[:, cols]).astype(BF16)
        for r in range(4):
            for c in range(6):
                gb[c % 2, 3 * (4 * n + r) + c // 2] = g[
                    c * BLK : (c + 1) * BLK, r * BLK : (r + 1) * BLK
                ]
        piece = pl.ds(12 * n, 12)
        swaps.append(send(gb.at[1 - core, piece], sb.at[piece], sib))
    for copy in swaps:
        copy.wait_recv()

    first = ("z", "y")
    second = ("y", "z")
    here = {"y": y, "z": z}
    steps = (2, 1, -1, 0)

    def fill(part, rel):
        f = wrap(here[first[part]] + steps[rel])
        for srel in range(4):
            s = wrap(here[second[part]] + steps[srel])
            d = index_of(f, s, part) if part == 0 else index_of(s, f, part)
            base = (starts[d] + 1 - core) // 2
            for i in range(HALF):
                j = jnp.minimum(base + i, NB // 2 - 1)
                acc[part, rel, srel, i] = (
                    gb[core, j].astype(F32) + sb[j].astype(F32)
                ).astype(BF16)

    lo, hi = pl.ds(0, 3), pl.ds(3, 3)
    subs = (pl.ds(0, 1), pl.ds(1, 2), pl.ds(3, 1))
    a = {}

    def go(part, name, u, src, dst, axis, step):
        a[part, name, u] = send(src, dst, at(axis[part], step))

    def send_far(part, u):
        sub = subs[u]
        go(part, "fu", u, acc.at[part, FAR, sub, lo], r_far.at[part, 0, sub], first, 1)
        go(part, "fd", u, acc.at[part, FAR, sub, hi], r_far.at[part, 1, sub], first, -1)

    def send_near(part, u):
        sub = subs[u]
        go(part, "lo1", u, acc.at[part, NXT, sub, hi], r_low.at[part, 1, sub], first, 1)
        go(part, "hi0", u, acc.at[part, PRV, sub, lo], r_high.at[part, 0, sub], first, -1)

    def middle(part, u):
        sub = subs[u]
        a[part, "fu", u].wait_recv()
        r_far[part, 0, sub] = (
            r_far[part, 0, sub].astype(F32) + acc[part, NXT, sub, lo].astype(F32)
        ).astype(BF16)
        go(part, "lo0", u, r_far.at[part, 0, sub], r_low.at[part, 0, sub], first, 1)
        a[part, "fd", u].wait_recv()
        r_far[part, 1, sub] = (
            r_far[part, 1, sub].astype(F32) + acc[part, PRV, sub, hi].astype(F32)
        ).astype(BF16)
        go(part, "hi1", u, r_far.at[part, 1, sub], r_high.at[part, 1, sub], first, -1)

    def reduce(part, u):
        sub = subs[u]
        for name in ("lo1", "hi0", "lo0", "hi1"):
            a[part, name, u].wait_recv()
        for h in (lo, hi):
            which = 0 if h is lo else 1
            red[part, sub, h] = (
                acc[part, OWN, sub, h].astype(F32)
                + r_low[part, which, sub].astype(F32)
                + r_high[part, which, sub].astype(F32)
            ).astype(BF16)

    both = (0, 1)
    for part in both:
        fill(part, FAR)
        send_far(part, 0)
    for part in both:
        fill(part, NXT)
        fill(part, PRV)
        send_near(part, 0)
    for part in both:
        send_far(part, 1)
        send_near(part, 1)
    for part in both:
        fill(part, OWN)
    for part in both:
        middle(part, 0)
    for part in both:
        send_far(part, 2)
        send_near(part, 2)
    for part in both:
        middle(part, 1)
    for part in both:
        reduce(part, 0)
        go(part, "tu", 0, red.at[part, FAR, lo], t_far.at[part, 0], second, 1)
        go(part, "td", 0, red.at[part, FAR, hi], t_far.at[part, 1], second, -1)
    for part in both:
        middle(part, 2)
    for part in both:
        reduce(part, 1)
        go(part, "tl1", 0, red.at[part, NXT, hi], t_low.at[part, 1], second, 1)
        go(part, "th0", 0, red.at[part, PRV, lo], t_high.at[part, 0], second, -1)
    for part in both:
        a[part, "tu", 0].wait_recv()
        t_far[part, 0] = (
            t_far[part, 0].astype(F32) + red[part, NXT, lo].astype(F32)
        ).astype(BF16)
        go(part, "tl0", 0, t_far.at[part, 0], t_low.at[part, 0], second, 1)
        a[part, "td", 0].wait_recv()
        t_far[part, 1] = (
            t_far[part, 1].astype(F32) + red[part, PRV, hi].astype(F32)
        ).astype(BF16)
        go(part, "th1", 0, t_far.at[part, 1], t_high.at[part, 1], second, -1)
    for part in both:
        reduce(part, 2)
    for part in both:
        for name in ("tl1", "th0", "tl0", "th1"):
            a[part, name, 0].wait_recv()
        for h in (0, 1):
            fin[part, pl.ds(3 * h, 3)] = (
                red[part, OWN, pl.ds(3 * h, 3)].astype(F32)
                + t_low[part, h].astype(F32)
                + t_high[part, h].astype(F32)
            )
    last = send(fin.at[1 - core], tot.at[core], sib)
    tot[core] = fin[core]
    last.wait_recv()

    start, n = starts[me], counts[me]
    factor = 1.0 / np.sqrt(np.float32(LEN * 32))
    for t in range(SLOTS):
        b = start + t
        parity = lax.rem(b, 2)
        v = tot[parity, b // 2 - (start + 1 - parity) // 2] * factor
        v = jnp.where(b < NQKV, v.T, v)
        out[t] = jnp.where(t < n, v, 0.0)
    for copy in sends:
        copy.wait_send()


def main(counts, cos, sin, sides, wo, curv, probs, qkv, normed):
    vmem = pl.BlockSpec(memory_space=pltpu.VMEM)
    hbm = pl.BlockSpec(memory_space=pl.ANY)
    smem = pl.BlockSpec(memory_space=pltpu.SMEM)
    block = (BLK, BLK)
    half = LEN // 2
    v = pltpu.VMEM
    return pl.pallas_call(
        main_kernel,
        out_shape=jax.ShapeDtypeStruct((SLOTS,) + block, F32),
        in_specs=[smem, vmem, vmem] + [hbm] * 6,
        out_specs=vmem,
        scratch_shapes=[
            pltpu.SMEM((32,), jnp.int32),
            v((2, LEN, OUT), BF16),
            v((4, 2, OUT, CHUNK), BF16),
            v((LEN, CHUNK), BF16),
            v((QH, LEN, LEN), BF16),
            v((LEN, QKV), BF16),
            v((LEN, D), BF16),
            v((4, 2, LEN, SUB), BF16),
            v((2, 2, half, SUB), BF16),
            v((2, 2, half, SUB), BF16),
            v((2, 2, half, SUB), BF16),
            v((4, 2, LEN, SUB), BF16),
            v((LEN, OUT), F32),
            v((QKV, LEN), BF16),
            v((2, NB // 2) + block, BF16),
            v((NB // 2,) + block, BF16),
            v((2, 4, 4, HALF) + block, BF16),
            v((2, 2, 4, 3) + block, BF16),
            v((2, 2, 4, 3) + block, BF16),
            v((2, 2, 4, 3) + block, BF16),
            v((2, 4, HALF) + block, BF16),
            v((2, 2, 3) + block, BF16),
            v((2, 2, 3) + block, BF16),
            v((2, 2, 3) + block, BF16),
            v((2, HALF) + block, F32),
            v((2, HALF) + block, F32),
            pltpu.SemaphoreType.DMA((82,)),
            pltpu.SemaphoreType.DMA((82,)),
            pltpu.SemaphoreType.DMA((9,)),
        ],
        compiler_params=pltpu.CompilerParams(
            collective_id=1, has_side_effects=True, vmem_limit_bytes=67_000_000
        ),
        name="main",
    )(counts, cos, sin, sides, wo, curv, probs, qkv, normed)


def local(tokens, norm_gain, curvature, weight_slots, probe_slots, block_counts):
    counts = block_counts[0]
    cos, sin = tables()
    slots, normed, table = gather(
        counts, weight_slots[0], probe_slots[0], tokens[0], norm_gain.reshape(1, D)
    )
    qkv, sides, probs, wo = forward(table.reshape(1024), cos, sin, normed, slots)
    out = main(counts, cos, sin, sides, wo, curvature[0], probs, qkv, normed)
    return out[None]


def solution(mesh):
    in_specs = (
        P("fsdp", None, None),
        P(),
        P("fsdp", None, None),
        P("seq", "fsdp", None, None),
        P("seq", "fsdp", None, None),
        P("seq", None),
    )
    out_specs = P("seq", "fsdp", None, None)
    return jax.shard_map(local, mesh=mesh, in_specs=in_specs, out_specs=out_specs, check_vma=False)
```

```python
import functools

import jax
import jax.numpy as jnp
import numpy as np
from jax import lax
from jax.experimental import pallas as pl
from jax.experimental.pallas import tpu as pltpu
from jax.sharding import PartitionSpec as P

D = 4096
HD = 128
BLK = 128
LEN = 512
QH = 4
QKV = 768
OUT = 512
NQKV = 192
NB = 320
SLOTS = 12
HALF = 6
CHUNK = 1024
SUB = 512
THETA = 500000.0
EPS = 1e-05
NEGATIVE = -1e30
VMEM_LIMIT = 66_000_000
MESH = pl.DeviceIdType.MESH
F32 = jnp.float32
BF16 = jnp.bfloat16


def tables():
    half = HD // 2
    frequency = np.exp(-np.log(THETA) * 2.0 * np.arange(half) / HD)
    angles = np.arange(LEN)[:, None] * frequency[None, :]
    c, s = np.cos(angles), np.sin(angles)
    return (
        np.concatenate([c, c], axis=1).astype(np.float32),
        np.concatenate([-s, s], axis=1).astype(np.float32),
    )


def place():
    me = lax.axis_index("fsdp")
    core = lax.rem(me, 2)
    y = lax.rem(me // 2, 4)
    z = me // 8
    return me, core, y, z


def index_of(z, y, core):
    return (z * 4 + y) * 2 + core


def wrap(a):
    return lax.rem(a + 4, 4)


def greet(targets):
    barrier = pltpu.get_barrier_semaphore()
    for t in targets:
        pl.semaphore_signal(barrier, inc=1, device_id=t, device_id_type=MESH)
    pl.semaphore_wait(barrier, len(targets))


def nt(a, b):
    return lax.dot_general(a, b, (((1,), (1,)), ((), ())), preferred_element_type=F32)


def nn(a, b):
    return jnp.dot(a, b, preferred_element_type=F32)


def causal_mask():
    row = lax.broadcasted_iota(jnp.int32, (LEN, LEN), 0)
    col = lax.broadcasted_iota(jnp.int32, (LEN, LEN), 1)
    return row >= col


def forward_kernel(
    counts, w_ref, p_ref, gain, tokens_in, cos_in, sin_in,
    normed_out, qkv_out, sides_out, probs_out, wo_out,
    table, slots_w, slots_p, normed, cos, sin, wqkv, pqkv, wout, proj, sides, probs, qkv,
    send_sem, recv_sem, local_sem,
):
    me, core, y, z = place()
    sib = {"fsdp": index_of(z, y, 1 - core)}

    def at(axis, step):
        if axis == "y":
            return {"fsdp": index_of(z, wrap(y + step), core)}
        return {"fsdp": index_of(wrap(z + step), y, core)}

    my_slots = pl.ds(me * SLOTS, SLOTS)
    local = [
        pltpu.make_async_copy(a, b, local_sem.at[i])
        for i, (a, b) in enumerate(
            (
                (tokens_in, normed),
                (cos_in, cos),
                (sin_in, sin),
                (w_ref, slots_w.at[my_slots]),
                (p_ref, slots_p.at[my_slots]),
            )
        )
    ]
    for copy in local:
        copy.start()
    greet([at("y", 1), at("y", -1), at("z", 1), at("z", -1), sib])

    first = ("y", "z", "y", "z")
    second = ("z", "y", "z", "y")
    mine = (w_ref, w_ref, p_ref, p_ref)
    landed = (slots_w, slots_w, slots_p, slots_p)
    counter = [0]
    sends = []
    arrivals = {}

    def send(key, src, dst, target):
        number = counter[0]
        counter[0] += 1
        copy = pltpu.make_async_remote_copy(
            src_ref=src,
            dst_ref=dst,
            send_sem=send_sem.at[number],
            recv_sem=recv_sem.at[number],
            device_id=target,
            device_id_type=MESH,
        )
        copy.start()
        sends.append(copy)
        arrivals[key] = copy

    def span(p, side):
        start = (p % 2) * HALF
        return (start, HALF) if side is None else (start + 3 * side, 3)

    def piece(p, origin, side=None):
        start, size = span(p, side)
        return landed[p].at[pl.ds(origin * SLOTS + start, size)]

    def origin_of(p, f, s):
        if p % 2 == 0:
            return index_of(wrap(z + s), wrap(y + f), core)
        return index_of(wrap(z + f), wrap(y + s), core)

    def go(p, role, f, s, axis, step, side=None):
        ref = piece(p, origin_of(p, f, s), side)
        src = ref
        if f == 0 and s == 0:
            src = mine[p].at[pl.ds(*span(p, side))]
        send((p,) + role, src, ref, at(axis[p], step))

    def to_sib(p, f, s):
        ref = piece(p, origin_of(p, f, s))
        src = ref
        if f == 0 and s == 0:
            src = mine[p].at[pl.ds(*span(p, None))]
        send((p, "sib", f, s), src, ref, sib)

    def got(*key):
        arrivals[key].wait_recv()

    def begin(parts):
        for p in parts:
            go(p, ("f+",), 0, 0, first, 1)
            go(p, ("f-",), 0, 0, first, -1)
        for p in parts:
            go(p, ("s+", 0), 0, 0, second, 1)
            go(p, ("s-", 0), 0, 0, second, -1)
        for p in parts:
            to_sib(p, 0, 0)

    def neighbours(p):
        got(p, "f+")
        go(p, ("fa",), -1, 0, first, 1, 0)
        go(p, ("s+", -1), -1, 0, second, 1)
        go(p, ("s-", -1), -1, 0, second, -1)
        got(p, "f-")
        go(p, ("fb",), 1, 0, first, -1, 1)
        go(p, ("s+", 1), 1, 0, second, 1)
        go(p, ("s-", 1), 1, 0, second, -1)
        to_sib(p, -1, 0)
        to_sib(p, 1, 0)

    def pass_on(p, f):
        got(p, "s+", f)
        go(p, ("sa", f), f, -1, second, 1, 0)
        to_sib(p, f, -1)
        got(p, "s-", f)
        go(p, ("sb", f), f, 1, second, -1, 1)
        to_sib(p, f, 1)

    def opposite(p):
        got(p, "fa")
        got(p, "fb")
        go(p, ("s+", 2), 2, 0, second, 1)
        go(p, ("s-", 2), 2, 0, second, -1)
        to_sib(p, 2, 0)

    def corner(p, f):
        got(p, "sa", f)
        got(p, "sb", f)
        to_sib(p, f, 2)

    def sibling_done(parts):
        for p in parts:
            for f in (0, -1, 1, 2):
                for s in (0, -1, 1, 2):
                    got(p, "sib", f, s)

    w, pr = (0, 1), (2, 3)
    begin(w)

    def locate(b, carry):
        d, t = carry
        table[b] = d * SLOTS + t
        more = t + 1 < counts[d]
        return jnp.where(more, d, jnp.minimum(d + 1, 31)), jnp.where(more, t + 1, 0)

    lax.fori_loop(0, NB, locate, (0, 0))
    local[0].wait()

    def norm(i, carry):
        rows = pl.ds(pl.multiple_of(i * 32, 32), 32)
        x = normed[rows, :].astype(F32)
        factor = lax.rsqrt(jnp.mean(x * x, axis=-1, keepdims=True) + EPS)
        normed[rows, :] = (x * factor * gain[...]).astype(BF16)
        return carry

    lax.fori_loop(0, LEN // 32, norm, 0)
    saves = [pltpu.make_async_copy(normed, normed_out, local_sem.at[5])]
    saves[-1].start()
    for i in (1, 2, 3, 4):
        local[i].wait()

    def cols_of(h):
        return pl.ds(h * HD if isinstance(h, int) else pl.multiple_of(h * HD, HD), HD)

    def assemble_qkv(src, dst, start, stop):
        def step(r, carry):
            rows = pl.ds(pl.multiple_of(r * BLK, BLK), BLK)
            for c in range(6):
                dst[rows, c * BLK : (c + 1) * BLK] = src[table[r * 6 + c]]
            return carry

        lax.fori_loop(start, stop, step, 0)

    def assemble_out(src, tensor):
        def step(i, carry):
            rows = pl.ds(pl.multiple_of(i * BLK, BLK), BLK)
            for j in range(32):
                wout[tensor, j // 8, rows, (j % 8) * BLK : (j % 8 + 1) * BLK] = src[
                    table[NQKV + i * 32 + j]
                ]
            return carry

        lax.fori_loop(0, 4, step, 0)
        saves.append(
            pltpu.make_async_copy(wout.at[tensor], wo_out.at[tensor], local_sem.at[6 + tensor])
        )
        saves[-1].start()

    def project(matrix, n):
        cols = slice(n * 256, (n + 1) * 256)
        proj[:, cols] = nn(normed[...], matrix[:, cols])

    def head(h, turn=True):
        x = proj[:, cols_of(h)]
        if turn:
            x = x * cos[...] + pltpu.roll(x, 64, 1) * sin[...]
        return x.astype(BF16)

    def heads():
        for h in range(QH + 2):
            qkv[:, cols_of(h)] = head(h, h < QH + 1)
        saves.append(pltpu.make_async_copy(qkv, qkv_out, local_sem.at[8]))
        saves[-1].start()

    scale = HD**-0.5

    def primal(h, carry):
        k = qkv[:, cols_of(QH)]
        v = qkv[:, cols_of(QH + 1)]
        s = jnp.where(causal_mask(), nt(qkv[:, cols_of(h)], k) * scale, NEGATIVE)
        m = jnp.max(s, axis=-1, keepdims=True)
        e = jnp.exp(s - m)
        p = (e * (1.0 / jnp.sum(e, axis=-1, keepdims=True))).astype(BF16)
        probs[h] = p
        sides[1, :, cols_of(h)] = nn(p, v).astype(BF16)
        return carry

    neighbours(0)
    neighbours(1)
    pass_on(0, 0)
    pass_on(1, 0)
    opposite(0)
    opposite(1)
    begin(pr)
    for f, g in ((-1, 0), (1, -1), (2, 1)):
        for p in w:
            pass_on(p, f)
            corner(p, g)
    neighbours(2)
    neighbours(3)
    corner(0, 2)
    corner(1, 2)
    pass_on(2, 0)
    pass_on(3, 0)
    sibling_done(w)
    assemble_qkv(slots_w, wqkv, 0, 32)
    opposite(2)
    opposite(3)
    project(wqkv, 0)
    pass_on(2, -1)
    pass_on(3, -1)
    project(wqkv, 1)
    corner(2, 0)
    corner(3, 0)
    project(wqkv, 2)
    pass_on(2, 1)
    pass_on(3, 1)
    heads()
    corner(2, -1)
    corner(3, -1)
    lax.fori_loop(0, 2, primal, 0)
    pass_on(2, 2)
    pass_on(3, 2)
    lax.fori_loop(2, 4, primal, 0)
    corner(2, 1)
    corner(3, 1)
    saves.append(pltpu.make_async_copy(probs, probs_out, local_sem.at[9]))
    saves[-1].start()
    assemble_out(slots_w, 0)
    corner(2, 2)
    corner(3, 2)
    sibling_done(pr)

    assemble_qkv(slots_p, pqkv, 0, 32)
    for n in range(3):
        project(pqkv, n)
    assemble_out(slots_p, 1)
    k = qkv[:, cols_of(QH)]
    v = qkv[:, cols_of(QH + 1)]
    keys = jnp.concatenate([k, head(QH)], axis=1)
    values = head(QH + 1, False)

    def tangent(h, carry):
        pb = probs[h]
        p = pb.astype(F32)
        ts = nt(jnp.concatenate([head(h), qkv[:, cols_of(h)]], axis=1), keys) * scale
        pt = p * ts
        tp = pt - p * jnp.sum(pt, axis=-1, keepdims=True)
        sides[0, :, cols_of(h)] = (nn(tp.astype(BF16), v) + nn(pb, values)).astype(BF16)
        return carry

    lax.fori_loop(0, QH, tangent, 0)
    saves.append(pltpu.make_async_copy(sides, sides_out, local_sem.at[10]))
    saves[-1].start()
    for copy in saves:
        copy.wait()
    for copy in sends:
        copy.wait_send()


def forward(counts, w, p, gain, tokens, cos, sin):
    vmem = pl.BlockSpec(memory_space=pltpu.VMEM)
    hbm = pl.BlockSpec(memory_space=pl.ANY)
    smem = pl.BlockSpec(memory_space=pltpu.SMEM)
    shape = jax.ShapeDtypeStruct
    v = pltpu.VMEM
    return pl.pallas_call(
        forward_kernel,
        out_shape=[
            shape((LEN, D), BF16),
            shape((LEN, QKV), BF16),
            shape((2, LEN, OUT), BF16),
            shape((QH, LEN, LEN), BF16),
            shape((2, 4, OUT, CHUNK), BF16),
        ],
        in_specs=[smem, vmem, vmem, vmem, hbm, hbm, hbm],
        out_specs=[hbm] * 5,
        scratch_shapes=[
            pltpu.SMEM((NB,), jnp.int32),
            v((32 * SLOTS, BLK, BLK), BF16),
            v((32 * SLOTS, BLK, BLK), BF16),
            v((LEN, D), BF16),
            v((LEN, HD), F32),
            v((LEN, HD), F32),
            v((D, QKV), BF16),
            v((D, QKV), BF16),
            v((2, 4, OUT, CHUNK), BF16),
            v((LEN, QKV), F32),
            v((2, LEN, OUT), BF16),
            v((QH, LEN, LEN), BF16),
            v((LEN, QKV), BF16),
            pltpu.SemaphoreType.DMA((144,)),
            pltpu.SemaphoreType.DMA((144,)),
            pltpu.SemaphoreType.DMA((11,)),
        ],
        compiler_params=pltpu.CompilerParams(
            collective_id=0, has_side_effects=True, vmem_limit_bytes=67_000_000
        ),
        name="forward",
    )(counts, w, p, gain, tokens, cos, sin)


FAR, NXT, PRV, OWN = 0, 1, 2, 3


def main_kernel(
    counts, cos, sin, sides_in, wo_in, curv_in, probs_in, qkv_in, normed_in,
    out,
    starts, sides, wo, curv, probs, qkv, normed,
    tan, opp, low, high, wt, dmix, dprojt, gb, sb,
    acc, r_far, r_low, r_high, red, t_far, t_low, t_high, fin, tot,
    send_sem, recv_sem, local_sem,
):
    me, core, y, z = place()
    x = lax.axis_index("seq")
    sib = {"fsdp": index_of(z, y, 1 - core)}
    up, down = {"seq": wrap(x + 1)}, {"seq": wrap(x - 1)}

    def at(axis, step):
        if axis == "y":
            return {"fsdp": index_of(z, wrap(y + step), core)}
        return {"fsdp": index_of(wrap(z + step), y, core)}

    chunk = (wrap(x + 2), wrap(x + 1), wrap(x - 1), x)
    curv_cols = pl.ds(pl.multiple_of(x * CHUNK, CHUNK), CHUNK)
    loads = [
        pltpu.make_async_copy(a, b, local_sem.at[i])
        for i, (a, b) in enumerate(
            [(wo_in.at[:, chunk[rel]], wo.at[rel]) for rel in range(4)]
            + [
                (sides_in, sides),
                (curv_in.at[:, curv_cols], curv),
                (probs_in, probs),
                (qkv_in, qkv),
                (normed_in, normed),
            ]
        )
    ]
    for i in (4, 0, 1, 2, 3, 5, 6, 7, 8):
        loads[i].start()
    greet([up, down, at("y", 1), at("y", -1), at("z", 1), at("z", -1), sib])

    sends = []
    counter = [0]

    def send(src, dst, target):
        number = counter[0]
        counter[0] += 1
        copy = pltpu.make_async_remote_copy(
            src_ref=src,
            dst_ref=dst,
            send_sem=send_sem.at[number],
            recv_sem=recv_sem.at[number],
            device_id=target,
            device_id_type=MESH,
        )
        copy.start()
        sends.append(copy)
        return copy

    def prefix(d, s):
        starts[d] = s
        return s + counts[d]

    lax.fori_loop(0, 32, prefix, 0)

    half = LEN // 2
    rows = (pl.ds(0, half), pl.ds(half, half))

    def term(rel, part, s):
        r = rows[part]
        cols = slice(s * SUB, (s + 1) * SUB)
        tan[rel, s, r] = (
            nn(sides[0, r], wo[rel, 0, :, cols]) + nn(sides[1, r], wo[rel, 1, :, cols])
        ).astype(BF16)

    a0, a1, a2, b0, b1, b2 = {}, {}, {}, {}, {}, {}
    loads[4].wait()
    loads[FAR].wait()
    for s in (0, 1):
        term(FAR, 0, s)
        a0[s] = send(tan.at[FAR, s, rows[0]], opp.at[0, s], up)
        term(FAR, 1, s)
        b0[s] = send(tan.at[FAR, s, rows[1]], opp.at[1, s], down)
        if s == 0:
            loads[NXT].wait()
            term(NXT, 1, s)
            a1[s] = send(tan.at[NXT, s, rows[1]], low.at[1, s], up)
            loads[PRV].wait()
            term(PRV, 0, s)
            b1[s] = send(tan.at[PRV, s, rows[0]], high.at[0, s], down)
    term(NXT, 0, 0)
    term(PRV, 1, 0)
    term(NXT, 1, 1)
    term(PRV, 0, 1)
    term(NXT, 0, 1)
    term(PRV, 1, 1)
    loads[OWN].wait()
    for s in (0, 1):
        for part in (0, 1):
            term(OWN, part, s)
    for s in (0, 1):
        a0[s].wait_recv()
        opp[0, s] = (opp[0, s].astype(F32) + tan[NXT, s, rows[0]].astype(F32)).astype(BF16)
        a2[s] = send(opp.at[0, s], low.at[0, s], up)
        b0[s].wait_recv()
        opp[1, s] = (opp[1, s].astype(F32) + tan[PRV, s, rows[1]].astype(F32)).astype(BF16)
        b2[s] = send(opp.at[1, s], high.at[1, s], down)
        if s == 0:
            a1[1] = send(tan.at[NXT, 1, rows[1]], low.at[1, 1], up)
            b1[1] = send(tan.at[PRV, 1, rows[0]], high.at[0, 1], down)
    loads[5].wait()

    def weigh(part, s):
        r = rows[part]
        total = tan[OWN, s, r].astype(F32) + low[part, s].astype(F32) + high[part, s].astype(F32)
        c = curv[r, s * SUB : (s + 1) * SUB].astype(F32)
        wt[OWN, s, r] = (total * c).astype(BF16)

    def hand_on(src, dst, part, s, target):
        return send(wt.at[src, s, rows[part]], wt.at[dst, s, rows[part]], target)

    mixedt = sides[1].T

    def consume(rel, s):
        part = nt(wt[rel, s], wo[rel, 0, :, s * SUB : (s + 1) * SUB])
        if rel == OWN and s == 0:
            dmix[...] = part
        else:
            dmix[...] += part
        g = nn(mixedt, wt[rel, s]).astype(BF16)
        for i in range(4):
            for j in range(4):
                gb[j % 2, NQKV // 2 + 16 * i + 4 * chunk[rel] + 2 * s + j // 2] = g[
                    i * BLK : (i + 1) * BLK, j * BLK : (j + 1) * BLK
                ]

    c0, c1, d0, d1, e0, e1 = {}, {}, {}, {}, {}, {}
    for s in (0, 1):
        a1[s].wait_recv()
        b2[s].wait_recv()
        weigh(1, s)
        c1[s] = hand_on(OWN, PRV, 1, s, up)
        d1[s] = hand_on(OWN, NXT, 1, s, down)
        b1[s].wait_recv()
        a2[s].wait_recv()
        weigh(0, s)
        d0[s] = hand_on(OWN, NXT, 0, s, down)
        c0[s] = hand_on(OWN, PRV, 0, s, up)
        if s == 0:
            consume(OWN, 0)
    for s in (0, 1):
        c1[s].wait_recv()
        e1[s] = hand_on(PRV, FAR, 1, s, up)
        d0[s].wait_recv()
        e0[s] = hand_on(NXT, FAR, 0, s, down)
        if s == 0:
            consume(OWN, 1)
        d1[s].wait_recv()
        consume(NXT, s)
        c0[s].wait_recv()
        consume(PRV, s)
    for s in (0, 1):
        e1[s].wait_recv()
        e0[s].wait_recv()
        consume(FAR, s)
    n_out = NB // 2 - NQKV // 2
    out_part = pl.ds(NQKV // 2, n_out)
    swap_out = send(gb.at[1 - core, out_part], sb.at[out_part], sib)

    for i in (6, 7, 8):
        loads[i].wait()
    c2, s2 = cos[...], sin[...]

    def unrot(x):
        return x * c2 - pltpu.roll(x, 64, 1) * s2

    k = qkv[:, QH * HD : (QH + 1) * HD]
    v = qkv[:, (QH + 1) * HD :]
    scale = HD**-0.5
    dkt = jnp.zeros((HD, LEN), F32)
    dvt = jnp.zeros((HD, LEN), F32)
    for h in range(QH):
        dm = dmix[:, h * HD : (h + 1) * HD].astype(BF16)
        q = qkv[:, h * HD : (h + 1) * HD]
        pb = probs[h]
        dp = nt(dm, v).astype(BF16).astype(F32)
        dvt = dvt + nn(dm.T, pb)
        pf = pb.astype(F32)
        pd = pf * dp
        ds = ((pd - pf * jnp.sum(pd, axis=-1, keepdims=True)) * scale).astype(BF16)
        dkt = dkt + nn(q.T, ds)
        dq = unrot(nn(ds, k).astype(BF16).astype(F32)).astype(BF16)
        dprojt[h * HD : (h + 1) * HD, :] = dq.T
    dk = unrot(dkt.astype(BF16).astype(F32).T).astype(BF16)
    dprojt[QH * HD : (QH + 1) * HD, :] = dk.T
    dprojt[(QH + 1) * HD :, :] = dvt.astype(BF16)

    swaps = [swap_out]
    for n in range(8):
        cols = slice(n * 512, (n + 1) * 512)
        g = nn(dprojt[...], normed[:, cols]).astype(BF16)
        for r in range(4):
            for c in range(6):
                gb[c % 2, 3 * (4 * n + r) + c // 2] = g[
                    c * BLK : (c + 1) * BLK, r * BLK : (r + 1) * BLK
                ]
        piece = pl.ds(12 * n, 12)
        swaps.append(send(gb.at[1 - core, piece], sb.at[piece], sib))
    for copy in swaps:
        copy.wait_recv()

    first = ("z", "y")
    second = ("y", "z")
    here = {"y": y, "z": z}
    steps = (2, 1, -1, 0)

    def fill(part, rel):
        f = wrap(here[first[part]] + steps[rel])
        for srel in range(4):
            s = wrap(here[second[part]] + steps[srel])
            d = index_of(f, s, part) if part == 0 else index_of(s, f, part)
            base = (starts[d] + 1 - core) // 2
            for i in range(HALF):
                j = jnp.minimum(base + i, NB // 2 - 1)
                acc[part, rel, srel, i] = (
                    gb[core, j].astype(F32) + sb[j].astype(F32)
                ).astype(BF16)

    lo, hi = pl.ds(0, 3), pl.ds(3, 3)
    subs = (pl.ds(0, 1), pl.ds(1, 2), pl.ds(3, 1))
    a = {}

    def go(part, name, u, src, dst, axis, step):
        a[part, name, u] = send(src, dst, at(axis[part], step))

    def send_far(part, u):
        sub = subs[u]
        go(part, "fu", u, acc.at[part, FAR, sub, lo], r_far.at[part, 0, sub], first, 1)
        go(part, "fd", u, acc.at[part, FAR, sub, hi], r_far.at[part, 1, sub], first, -1)

    def send_near(part, u):
        sub = subs[u]
        go(part, "lo1", u, acc.at[part, NXT, sub, hi], r_low.at[part, 1, sub], first, 1)
        go(part, "hi0", u, acc.at[part, PRV, sub, lo], r_high.at[part, 0, sub], first, -1)

    def middle(part, u):
        sub = subs[u]
        a[part, "fu", u].wait_recv()
        r_far[part, 0, sub] = (
            r_far[part, 0, sub].astype(F32) + acc[part, NXT, sub, lo].astype(F32)
        ).astype(BF16)
        go(part, "lo0", u, r_far.at[part, 0, sub], r_low.at[part, 0, sub], first, 1)
        a[part, "fd", u].wait_recv()
        r_far[part, 1, sub] = (
            r_far[part, 1, sub].astype(F32) + acc[part, PRV, sub, hi].astype(F32)
        ).astype(BF16)
        go(part, "hi1", u, r_far.at[part, 1, sub], r_high.at[part, 1, sub], first, -1)

    def reduce(part, u):
        sub = subs[u]
        for name in ("lo1", "hi0", "lo0", "hi1"):
            a[part, name, u].wait_recv()
        for h in (lo, hi):
            which = 0 if h is lo else 1
            red[part, sub, h] = (
                acc[part, OWN, sub, h].astype(F32)
                + r_low[part, which, sub].astype(F32)
                + r_high[part, which, sub].astype(F32)
            ).astype(BF16)

    both = (0, 1)
    for part in both:
        fill(part, FAR)
        send_far(part, 0)
    for part in both:
        fill(part, NXT)
        fill(part, PRV)
        send_near(part, 0)
    for part in both:
        send_far(part, 1)
        send_near(part, 1)
    for part in both:
        fill(part, OWN)
    for part in both:
        middle(part, 0)
    for part in both:
        send_far(part, 2)
        send_near(part, 2)
    for part in both:
        middle(part, 1)
    for part in both:
        reduce(part, 0)
        go(part, "tu", 0, red.at[part, FAR, lo], t_far.at[part, 0], second, 1)
        go(part, "td", 0, red.at[part, FAR, hi], t_far.at[part, 1], second, -1)
    for part in both:
        middle(part, 2)
    for part in both:
        reduce(part, 1)
        go(part, "tl1", 0, red.at[part, NXT, hi], t_low.at[part, 1], second, 1)
        go(part, "th0", 0, red.at[part, PRV, lo], t_high.at[part, 0], second, -1)
    for part in both:
        a[part, "tu", 0].wait_recv()
        t_far[part, 0] = (
            t_far[part, 0].astype(F32) + red[part, NXT, lo].astype(F32)
        ).astype(BF16)
        go(part, "tl0", 0, t_far.at[part, 0], t_low.at[part, 0], second, 1)
        a[part, "td", 0].wait_recv()
        t_far[part, 1] = (
            t_far[part, 1].astype(F32) + red[part, PRV, hi].astype(F32)
        ).astype(BF16)
        go(part, "th1", 0, t_far.at[part, 1], t_high.at[part, 1], second, -1)
    for part in both:
        reduce(part, 2)
    for part in both:
        for name in ("tl1", "th0", "tl0", "th1"):
            a[part, name, 0].wait_recv()
        for h in (0, 1):
            fin[part, pl.ds(3 * h, 3)] = (
                red[part, OWN, pl.ds(3 * h, 3)].astype(F32)
                + t_low[part, h].astype(F32)
                + t_high[part, h].astype(F32)
            )
    last = send(fin.at[1 - core], tot.at[core], sib)
    tot[core] = fin[core]
    last.wait_recv()

    start, n = starts[me], counts[me]
    factor = 1.0 / np.sqrt(np.float32(LEN * 32))
    for t in range(SLOTS):
        b = start + t
        parity = lax.rem(b, 2)
        v = tot[parity, b // 2 - (start + 1 - parity) // 2] * factor
        v = jnp.where(b < NQKV, v.T, v)
        out[t] = jnp.where(t < n, v, 0.0)
    for copy in sends:
        copy.wait_send()


def main(counts, cos, sin, sides, wo, curv, probs, qkv, normed):
    vmem = pl.BlockSpec(memory_space=pltpu.VMEM)
    hbm = pl.BlockSpec(memory_space=pl.ANY)
    smem = pl.BlockSpec(memory_space=pltpu.SMEM)
    block = (BLK, BLK)
    half = LEN // 2
    v = pltpu.VMEM
    return pl.pallas_call(
        main_kernel,
        out_shape=jax.ShapeDtypeStruct((SLOTS,) + block, F32),
        in_specs=[smem, vmem, vmem] + [hbm] * 6,
        out_specs=vmem,
        scratch_shapes=[
            pltpu.SMEM((32,), jnp.int32),
            v((2, LEN, OUT), BF16),
            v((4, 2, OUT, CHUNK), BF16),
            v((LEN, CHUNK), BF16),
            v((QH, LEN, LEN), BF16),
            v((LEN, QKV), BF16),
            v((LEN, D), BF16),
            v((4, 2, LEN, SUB), BF16),
            v((2, 2, half, SUB), BF16),
            v((2, 2, half, SUB), BF16),
            v((2, 2, half, SUB), BF16),
            v((4, 2, LEN, SUB), BF16),
            v((LEN, OUT), F32),
            v((QKV, LEN), BF16),
            v((2, NB // 2) + block, BF16),
            v((NB // 2,) + block, BF16),
            v((2, 4, 4, HALF) + block, BF16),
            v((2, 2, 4, 3) + block, BF16),
            v((2, 2, 4, 3) + block, BF16),
            v((2, 2, 4, 3) + block, BF16),
            v((2, 4, HALF) + block, BF16),
            v((2, 2, 3) + block, BF16),
            v((2, 2, 3) + block, BF16),
            v((2, 2, 3) + block, BF16),
            v((2, HALF) + block, F32),
            v((2, HALF) + block, F32),
            pltpu.SemaphoreType.DMA((82,)),
            pltpu.SemaphoreType.DMA((82,)),
            pltpu.SemaphoreType.DMA((9,)),
        ],
        compiler_params=pltpu.CompilerParams(
            collective_id=1, has_side_effects=True, vmem_limit_bytes=67_000_000
        ),
        name="main",
    )(counts, cos, sin, sides, wo, curv, probs, qkv, normed)


def local(tokens, norm_gain, curvature, weight_slots, probe_slots, block_counts):
    counts = block_counts[0]
    cos, sin = tables()
    normed, qkv, sides, probs, wo = forward(
        counts, weight_slots[0], probe_slots[0], norm_gain.reshape(1, D), tokens[0], cos, sin
    )
    out = main(counts, cos, sin, sides, wo, curvature[0], probs, qkv, normed)
    return out[None]


def solution(mesh):
    in_specs = (
        P("fsdp", None, None),
        P(),
        P("fsdp", None, None),
        P("seq", "fsdp", None, None),
        P("seq", "fsdp", None, None),
        P("seq", None),
    )
    out_specs = P("seq", "fsdp", None, None)
    return jax.shard_map(local, mesh=mesh, in_specs=in_specs, out_specs=out_specs, check_vma=False)
```

```python
import functools

import jax
import jax.numpy as jnp
import numpy as np
from jax import lax
from jax.experimental import pallas as pl
from jax.experimental.pallas import tpu as pltpu
from jax.sharding import PartitionSpec as P

D = 4096
HD = 128
BLK = 128
LEN = 512
QH = 4
QKV = 768
OUT = 512
NQKV = 192
NB = 320
SLOTS = 12
HALF = 6
CHUNK = 1024
SUB = 512
THETA = 500000.0
EPS = 1e-05
NEGATIVE = -1e30
VMEM_LIMIT = 66_000_000
MESH = pl.DeviceIdType.MESH
F32 = jnp.float32
BF16 = jnp.bfloat16


def tables():
    half = HD // 2
    frequency = np.exp(-np.log(THETA) * 2.0 * np.arange(half) / HD)
    angles = np.arange(LEN)[:, None] * frequency[None, :]
    c, s = np.cos(angles), np.sin(angles)
    return (
        np.concatenate([c, c], axis=1).astype(np.float32),
        np.concatenate([-s, s], axis=1).astype(np.float32),
    )


def place():
    me = lax.axis_index("fsdp")
    core = lax.rem(me, 2)
    y = lax.rem(me // 2, 4)
    z = me // 8
    return me, core, y, z


def index_of(z, y, core):
    return (z * 4 + y) * 2 + core


def wrap(a):
    return lax.rem(a + 4, 4)


def greet(targets):
    barrier = pltpu.get_barrier_semaphore()
    for t in targets:
        pl.semaphore_signal(barrier, inc=1, device_id=t, device_id_type=MESH)
    pl.semaphore_wait(barrier, len(targets))


def nt(a, b):
    return lax.dot_general(a, b, (((1,), (1,)), ((), ())), preferred_element_type=F32)


def nn(a, b):
    return jnp.dot(a, b, preferred_element_type=F32)


def causal_mask():
    row = lax.broadcasted_iota(jnp.int32, (LEN, LEN), 0)
    col = lax.broadcasted_iota(jnp.int32, (LEN, LEN), 1)
    return row >= col


def forward_kernel(
    counts, w_ref, p_ref, gain, tokens_in, cos_in, sin_in,
    normed_out, qkv_out, sides_out, probs_out, wo_out,
    table, slots_w, slots_p, normed, cos, sin, wqkv, pqkv, wout, proj, sides, probs, qkv,
    send_sem, recv_sem, local_sem,
):
    me, core, y, z = place()
    sib = {"fsdp": index_of(z, y, 1 - core)}

    def at(axis, step):
        if axis == "y":
            return {"fsdp": index_of(z, wrap(y + step), core)}
        return {"fsdp": index_of(wrap(z + step), y, core)}

    my_slots = pl.ds(me * SLOTS, SLOTS)
    local = [
        pltpu.make_async_copy(a, b, local_sem.at[i])
        for i, (a, b) in enumerate(
            (
                (tokens_in, normed),
                (cos_in, cos),
                (sin_in, sin),
                (w_ref, slots_w.at[my_slots]),
                (p_ref, slots_p.at[my_slots]),
            )
        )
    ]
    for copy in local:
        copy.start()
    greet([at("y", 1), at("y", -1), at("z", 1), at("z", -1), sib])

    first = ("y", "z", "y", "z")
    second = ("z", "y", "z", "y")
    mine = (w_ref, w_ref, p_ref, p_ref)
    landed = (slots_w, slots_w, slots_p, slots_p)
    counter = [0]
    sends = []
    arrivals = {}

    def send(key, src, dst, target):
        number = counter[0]
        counter[0] += 1
        copy = pltpu.make_async_remote_copy(
            src_ref=src,
            dst_ref=dst,
            send_sem=send_sem.at[number],
            recv_sem=recv_sem.at[number],
            device_id=target,
            device_id_type=MESH,
        )
        copy.start()
        sends.append(copy)
        arrivals[key] = copy

    def span(p, side):
        start = (p % 2) * HALF
        return (start, HALF) if side is None else (start + 3 * side, 3)

    def piece(p, origin, side=None):
        start, size = span(p, side)
        return landed[p].at[pl.ds(origin * SLOTS + start, size)]

    def origin_of(p, f, s):
        if p % 2 == 0:
            return index_of(wrap(z + s), wrap(y + f), core)
        return index_of(wrap(z + f), wrap(y + s), core)

    def go(p, role, f, s, axis, step, side=None):
        ref = piece(p, origin_of(p, f, s), side)
        src = ref
        if f == 0 and s == 0:
            src = mine[p].at[pl.ds(*span(p, side))]
        send((p,) + role, src, ref, at(axis[p], step))

    def to_sib(p, f, s):
        ref = piece(p, origin_of(p, f, s))
        src = ref
        if f == 0 and s == 0:
            src = mine[p].at[pl.ds(*span(p, None))]
        send((p, "sib", f, s), src, ref, sib)

    def got(*key):
        arrivals[key].wait_recv()

    def begin(parts):
        for p in parts:
            go(p, ("f+",), 0, 0, first, 1)
            go(p, ("f-",), 0, 0, first, -1)
        for p in parts:
            go(p, ("s+", 0), 0, 0, second, 1)
            go(p, ("s-", 0), 0, 0, second, -1)
        for p in parts:
            to_sib(p, 0, 0)

    def neighbours(p):
        got(p, "f+")
        go(p, ("fa",), -1, 0, first, 1, 0)
        go(p, ("s+", -1), -1, 0, second, 1)
        go(p, ("s-", -1), -1, 0, second, -1)
        got(p, "f-")
        go(p, ("fb",), 1, 0, first, -1, 1)
        go(p, ("s+", 1), 1, 0, second, 1)
        go(p, ("s-", 1), 1, 0, second, -1)
        to_sib(p, -1, 0)
        to_sib(p, 1, 0)

    def pass_on(p, f):
        got(p, "s+", f)
        go(p, ("sa", f), f, -1, second, 1, 0)
        to_sib(p, f, -1)
        got(p, "s-", f)
        go(p, ("sb", f), f, 1, second, -1, 1)
        to_sib(p, f, 1)

    def opposite(p):
        got(p, "fa")
        got(p, "fb")
        go(p, ("s+", 2), 2, 0, second, 1)
        go(p, ("s-", 2), 2, 0, second, -1)
        to_sib(p, 2, 0)

    def corner(p, f):
        got(p, "sa", f)
        got(p, "sb", f)
        to_sib(p, f, 2)

    def sibling_done(parts):
        for p in parts:
            for f in (0, -1, 1, 2):
                for s in (0, -1, 1, 2):
                    got(p, "sib", f, s)

    w, pr = (0, 1), (2, 3)
    begin(w)

    def locate(b, carry):
        d, t = carry
        table[b] = d * SLOTS + t
        more = t + 1 < counts[d]
        return jnp.where(more, d, jnp.minimum(d + 1, 31)), jnp.where(more, t + 1, 0)

    lax.fori_loop(0, NB, locate, (0, 0))
    local[0].wait()

    def norm(i, carry):
        rows = pl.ds(pl.multiple_of(i * 32, 32), 32)
        x = normed[rows, :].astype(F32)
        factor = lax.rsqrt(jnp.mean(x * x, axis=-1, keepdims=True) + EPS)
        normed[rows, :] = (x * factor * gain[...]).astype(BF16)
        return carry

    lax.fori_loop(0, LEN // 32, norm, 0)
    saves = [pltpu.make_async_copy(normed, normed_out, local_sem.at[5])]
    saves[-1].start()
    for i in (1, 2, 3, 4):
        local[i].wait()

    def cols_of(h):
        return pl.ds(h * HD if isinstance(h, int) else pl.multiple_of(h * HD, HD), HD)

    def assemble_qkv(src, dst, start, stop):
        def step(r, carry):
            rows = pl.ds(pl.multiple_of(r * BLK, BLK), BLK)
            for c in range(6):
                dst[rows, c * BLK : (c + 1) * BLK] = src[table[r * 6 + c]]
            return carry

        lax.fori_loop(start, stop, step, 0)

    def assemble_out(src, tensor):
        def step(i, carry):
            rows = pl.ds(pl.multiple_of(i * BLK, BLK), BLK)
            for j in range(32):
                wout[tensor, j // 8, rows, (j % 8) * BLK : (j % 8 + 1) * BLK] = src[
                    table[NQKV + i * 32 + j]
                ]
            return carry

        lax.fori_loop(0, 4, step, 0)
        saves.append(
            pltpu.make_async_copy(wout.at[tensor], wo_out.at[tensor], local_sem.at[6 + tensor])
        )
        saves[-1].start()

    def project(matrix, n):
        cols = slice(n * 256, (n + 1) * 256)
        proj[:, cols] = nn(normed[...], matrix[:, cols])

    def head(h, turn=True):
        x = proj[:, cols_of(h)]
        if turn:
            x = x * cos[...] + pltpu.roll(x, 64, 1) * sin[...]
        return x.astype(BF16)

    def heads():
        for h in range(QH + 2):
            qkv[:, cols_of(h)] = head(h, h < QH + 1)
        saves.append(pltpu.make_async_copy(qkv, qkv_out, local_sem.at[8]))
        saves[-1].start()

    scale = HD**-0.5

    def primal(h, carry):
        k = qkv[:, cols_of(QH)]
        v = qkv[:, cols_of(QH + 1)]
        s = jnp.where(causal_mask(), nt(qkv[:, cols_of(h)], k) * scale, NEGATIVE)
        m = jnp.max(s, axis=-1, keepdims=True)
        e = jnp.exp(s - m)
        p = (e * (1.0 / jnp.sum(e, axis=-1, keepdims=True))).astype(BF16)
        probs[h] = p
        sides[1, :, cols_of(h)] = nn(p, v).astype(BF16)
        return carry

    for p in w:
        neighbours(p)
    for p in w:
        pass_on(p, 0)
    for p in w:
        opposite(p)
    begin(pr)
    for f in (-1, 1):
        for p in w:
            pass_on(p, f)
    for p in w:
        corner(p, 0)
    for p in w:
        pass_on(p, 2)
    for p in pr:
        neighbours(p)
    for p in pr:
        pass_on(p, 0)
    for f in (-1, 1, 2):
        for p in w:
            corner(p, f)
    for p in pr:
        opposite(p)
    sibling_done(w)
    assemble_qkv(slots_w, wqkv, 0, 32)
    project(wqkv, 0)
    for p in pr:
        pass_on(p, -1)
    for p in pr:
        corner(p, 0)
    project(wqkv, 1)
    project(wqkv, 2)
    for p in pr:
        pass_on(p, 1)
    heads()
    lax.fori_loop(0, 2, primal, 0)
    for p in pr:
        pass_on(p, 2)
    lax.fori_loop(2, 4, primal, 0)
    saves.append(pltpu.make_async_copy(probs, probs_out, local_sem.at[9]))
    saves[-1].start()
    assemble_out(slots_w, 0)
    for f in (-1, 1, 2):
        for p in pr:
            corner(p, f)
    sibling_done(pr)

    assemble_qkv(slots_p, pqkv, 0, 32)
    for n in range(3):
        project(pqkv, n)
    assemble_out(slots_p, 1)
    k = qkv[:, cols_of(QH)]
    v = qkv[:, cols_of(QH + 1)]
    keys = jnp.concatenate([k, head(QH)], axis=1)
    values = head(QH + 1, False)

    def tangent(h, carry):
        pb = probs[h]
        p = pb.astype(F32)
        ts = nt(jnp.concatenate([head(h), qkv[:, cols_of(h)]], axis=1), keys) * scale
        pt = p * ts
        tp = pt - p * jnp.sum(pt, axis=-1, keepdims=True)
        sides[0, :, cols_of(h)] = (nn(tp.astype(BF16), v) + nn(pb, values)).astype(BF16)
        return carry

    lax.fori_loop(0, QH, tangent, 0)
    saves.append(pltpu.make_async_copy(sides, sides_out, local_sem.at[10]))
    saves[-1].start()
    for copy in saves:
        copy.wait()
    for copy in sends:
        copy.wait_send()


def forward(counts, w, p, gain, tokens, cos, sin):
    vmem = pl.BlockSpec(memory_space=pltpu.VMEM)
    hbm = pl.BlockSpec(memory_space=pl.ANY)
    smem = pl.BlockSpec(memory_space=pltpu.SMEM)
    shape = jax.ShapeDtypeStruct
    v = pltpu.VMEM
    return pl.pallas_call(
        forward_kernel,
        out_shape=[
            shape((LEN, D), BF16),
            shape((LEN, QKV), BF16),
            shape((2, LEN, OUT), BF16),
            shape((QH, LEN, LEN), BF16),
            shape((2, 4, OUT, CHUNK), BF16),
        ],
        in_specs=[smem, vmem, vmem, vmem, hbm, hbm, hbm],
        out_specs=[hbm] * 5,
        scratch_shapes=[
            pltpu.SMEM((NB,), jnp.int32),
            v((32 * SLOTS, BLK, BLK), BF16),
            v((32 * SLOTS, BLK, BLK), BF16),
            v((LEN, D), BF16),
            v((LEN, HD), F32),
            v((LEN, HD), F32),
            v((D, QKV), BF16),
            v((D, QKV), BF16),
            v((2, 4, OUT, CHUNK), BF16),
            v((LEN, QKV), F32),
            v((2, LEN, OUT), BF16),
            v((QH, LEN, LEN), BF16),
            v((LEN, QKV), BF16),
            pltpu.SemaphoreType.DMA((144,)),
            pltpu.SemaphoreType.DMA((144,)),
            pltpu.SemaphoreType.DMA((11,)),
        ],
        compiler_params=pltpu.CompilerParams(
            collective_id=0, has_side_effects=True, vmem_limit_bytes=67_000_000
        ),
        name="forward",
    )(counts, w, p, gain, tokens, cos, sin)


FAR, NXT, PRV, OWN = 0, 1, 2, 3


def main_kernel(
    counts, cos, sin, sides_in, wo_in, curv_in, probs_in, qkv_in, normed_in,
    out,
    starts, sides, wo, curv, probs, qkv, normed,
    tan, opp, low, high, wt, dmix, dprojt, gb, sb,
    acc, r_far, r_low, r_high, red, t_far, t_low, t_high, fin, tot,
    send_sem, recv_sem, local_sem,
):
    me, core, y, z = place()
    x = lax.axis_index("seq")
    sib = {"fsdp": index_of(z, y, 1 - core)}
    up, down = {"seq": wrap(x + 1)}, {"seq": wrap(x - 1)}

    def at(axis, step):
        if axis == "y":
            return {"fsdp": index_of(z, wrap(y + step), core)}
        return {"fsdp": index_of(wrap(z + step), y, core)}

    chunk = (wrap(x + 2), wrap(x + 1), wrap(x - 1), x)
    curv_cols = pl.ds(pl.multiple_of(x * CHUNK, CHUNK), CHUNK)
    loads = [
        pltpu.make_async_copy(a, b, local_sem.at[i])
        for i, (a, b) in enumerate(
            [(wo_in.at[:, chunk[rel]], wo.at[rel]) for rel in range(4)]
            + [
                (sides_in, sides),
                (curv_in.at[:, curv_cols], curv),
                (probs_in, probs),
                (qkv_in, qkv),
                (normed_in, normed),
            ]
        )
    ]
    for i in (4, 0, 1, 2, 3, 5, 6, 7, 8):
        loads[i].start()
    greet([up, down, at("y", 1), at("y", -1), at("z", 1), at("z", -1), sib])

    sends = []
    counter = [0]

    def send(src, dst, target):
        number = counter[0]
        counter[0] += 1
        copy = pltpu.make_async_remote_copy(
            src_ref=src,
            dst_ref=dst,
            send_sem=send_sem.at[number],
            recv_sem=recv_sem.at[number],
            device_id=target,
            device_id_type=MESH,
        )
        copy.start()
        sends.append(copy)
        return copy

    def prefix(d, s):
        starts[d] = s
        return s + counts[d]

    lax.fori_loop(0, 32, prefix, 0)

    half = LEN // 2
    rows = (pl.ds(0, half), pl.ds(half, half))

    def term(rel, part, s):
        r = rows[part]
        cols = slice(s * SUB, (s + 1) * SUB)
        tan[rel, s, r] = (
            nn(sides[0, r], wo[rel, 0, :, cols]) + nn(sides[1, r], wo[rel, 1, :, cols])
        ).astype(BF16)

    a0, a1, a2, b0, b1, b2 = {}, {}, {}, {}, {}, {}
    loads[4].wait()
    loads[FAR].wait()
    for s in (0, 1):
        term(FAR, 0, s)
        a0[s] = send(tan.at[FAR, s, rows[0]], opp.at[0, s], up)
        term(FAR, 1, s)
        b0[s] = send(tan.at[FAR, s, rows[1]], opp.at[1, s], down)
        if s == 0:
            loads[NXT].wait()
            term(NXT, 1, s)
            a1[s] = send(tan.at[NXT, s, rows[1]], low.at[1, s], up)
            loads[PRV].wait()
            term(PRV, 0, s)
            b1[s] = send(tan.at[PRV, s, rows[0]], high.at[0, s], down)
    term(NXT, 0, 0)
    term(PRV, 1, 0)
    term(NXT, 1, 1)
    term(PRV, 0, 1)
    term(NXT, 0, 1)
    term(PRV, 1, 1)
    loads[OWN].wait()
    for s in (0, 1):
        for part in (0, 1):
            term(OWN, part, s)
    for s in (0, 1):
        a0[s].wait_recv()
        opp[0, s] = (opp[0, s].astype(F32) + tan[NXT, s, rows[0]].astype(F32)).astype(BF16)
        a2[s] = send(opp.at[0, s], low.at[0, s], up)
        b0[s].wait_recv()
        opp[1, s] = (opp[1, s].astype(F32) + tan[PRV, s, rows[1]].astype(F32)).astype(BF16)
        b2[s] = send(opp.at[1, s], high.at[1, s], down)
        if s == 0:
            a1[1] = send(tan.at[NXT, 1, rows[1]], low.at[1, 1], up)
            b1[1] = send(tan.at[PRV, 1, rows[0]], high.at[0, 1], down)
    loads[5].wait()

    def weigh(part, s):
        r = rows[part]
        total = tan[OWN, s, r].astype(F32) + low[part, s].astype(F32) + high[part, s].astype(F32)
        c = curv[r, s * SUB : (s + 1) * SUB].astype(F32)
        wt[OWN, s, r] = (total * c).astype(BF16)

    def hand_on(src, dst, part, s, target):
        return send(wt.at[src, s, rows[part]], wt.at[dst, s, rows[part]], target)

    mixedt = sides[1].T

    def consume(rel, s):
        part = nt(wt[rel, s], wo[rel, 0, :, s * SUB : (s + 1) * SUB])
        if rel == OWN and s == 0:
            dmix[...] = part
        else:
            dmix[...] += part
        g = nn(mixedt, wt[rel, s]).astype(BF16)
        for i in range(4):
            for j in range(4):
                gb[j % 2, NQKV // 2 + 16 * i + 4 * chunk[rel] + 2 * s + j // 2] = g[
                    i * BLK : (i + 1) * BLK, j * BLK : (j + 1) * BLK
                ]

    c0, c1, d0, d1, e0, e1 = {}, {}, {}, {}, {}, {}
    for s in (0, 1):
        a1[s].wait_recv()
        b2[s].wait_recv()
        weigh(1, s)
        c1[s] = hand_on(OWN, PRV, 1, s, up)
        d1[s] = hand_on(OWN, NXT, 1, s, down)
        b1[s].wait_recv()
        a2[s].wait_recv()
        weigh(0, s)
        d0[s] = hand_on(OWN, NXT, 0, s, down)
        c0[s] = hand_on(OWN, PRV, 0, s, up)
        if s == 0:
            consume(OWN, 0)
    for s in (0, 1):
        c1[s].wait_recv()
        e1[s] = hand_on(PRV, FAR, 1, s, up)
        d0[s].wait_recv()
        e0[s] = hand_on(NXT, FAR, 0, s, down)
        if s == 0:
            consume(OWN, 1)
        d1[s].wait_recv()
        consume(NXT, s)
        c0[s].wait_recv()
        consume(PRV, s)
    for s in (0, 1):
        e1[s].wait_recv()
        e0[s].wait_recv()
        consume(FAR, s)
    n_out = NB // 2 - NQKV // 2
    out_part = pl.ds(NQKV // 2, n_out)
    swap_out = send(gb.at[1 - core, out_part], sb.at[out_part], sib)

    for i in (6, 7, 8):
        loads[i].wait()
    c2, s2 = cos[...], sin[...]

    def unrot(x):
        return x * c2 - pltpu.roll(x, 64, 1) * s2

    k = qkv[:, QH * HD : (QH + 1) * HD]
    v = qkv[:, (QH + 1) * HD :]
    scale = HD**-0.5
    dkt = jnp.zeros((HD, LEN), F32)
    dvt = jnp.zeros((HD, LEN), F32)
    for h in range(QH):
        dm = dmix[:, h * HD : (h + 1) * HD].astype(BF16)
        q = qkv[:, h * HD : (h + 1) * HD]
        pb = probs[h]
        dp = nt(dm, v).astype(BF16).astype(F32)
        dvt = dvt + nn(dm.T, pb)
        pf = pb.astype(F32)
        pd = pf * dp
        ds = ((pd - pf * jnp.sum(pd, axis=-1, keepdims=True)) * scale).astype(BF16)
        dkt = dkt + nn(q.T, ds)
        dq = unrot(nn(ds, k).astype(BF16).astype(F32)).astype(BF16)
        dprojt[h * HD : (h + 1) * HD, :] = dq.T
    dk = unrot(dkt.astype(BF16).astype(F32).T).astype(BF16)
    dprojt[QH * HD : (QH + 1) * HD, :] = dk.T
    dprojt[(QH + 1) * HD :, :] = dvt.astype(BF16)

    swaps = [swap_out]
    for n in range(8):
        cols = slice(n * 512, (n + 1) * 512)
        g = nn(dprojt[...], normed[:, cols]).astype(BF16)
        for r in range(4):
            for c in range(6):
                gb[c % 2, 3 * (4 * n + r) + c // 2] = g[
                    c * BLK : (c + 1) * BLK, r * BLK : (r + 1) * BLK
                ]
        piece = pl.ds(12 * n, 12)
        swaps.append(send(gb.at[1 - core, piece], sb.at[piece], sib))
    for copy in swaps:
        copy.wait_recv()

    first = ("z", "y")
    second = ("y", "z")
    here = {"y": y, "z": z}
    steps = (2, 1, -1, 0)

    def fill(part, rel):
        f = wrap(here[first[part]] + steps[rel])
        for srel in range(4):
            s = wrap(here[second[part]] + steps[srel])
            d = index_of(f, s, part) if part == 0 else index_of(s, f, part)
            base = (starts[d] + 1 - core) // 2
            for i in range(HALF):
                j = jnp.minimum(base + i, NB // 2 - 1)
                acc[part, rel, srel, i] = (
                    gb[core, j].astype(F32) + sb[j].astype(F32)
                ).astype(BF16)

    lo, hi = pl.ds(0, 3), pl.ds(3, 3)
    subs = (pl.ds(0, 1), pl.ds(1, 2), pl.ds(3, 1))
    a = {}

    def go(part, name, u, src, dst, axis, step):
        a[part, name, u] = send(src, dst, at(axis[part], step))

    def send_far(part, u):
        sub = subs[u]
        go(part, "fu", u, acc.at[part, FAR, sub, lo], r_far.at[part, 0, sub], first, 1)
        go(part, "fd", u, acc.at[part, FAR, sub, hi], r_far.at[part, 1, sub], first, -1)

    def send_near(part, u):
        sub = subs[u]
        go(part, "lo1", u, acc.at[part, NXT, sub, hi], r_low.at[part, 1, sub], first, 1)
        go(part, "hi0", u, acc.at[part, PRV, sub, lo], r_high.at[part, 0, sub], first, -1)

    def middle(part, u):
        sub = subs[u]
        a[part, "fu", u].wait_recv()
        r_far[part, 0, sub] = (
            r_far[part, 0, sub].astype(F32) + acc[part, NXT, sub, lo].astype(F32)
        ).astype(BF16)
        go(part, "lo0", u, r_far.at[part, 0, sub], r_low.at[part, 0, sub], first, 1)
        a[part, "fd", u].wait_recv()
        r_far[part, 1, sub] = (
            r_far[part, 1, sub].astype(F32) + acc[part, PRV, sub, hi].astype(F32)
        ).astype(BF16)
        go(part, "hi1", u, r_far.at[part, 1, sub], r_high.at[part, 1, sub], first, -1)

    def reduce(part, u):
        sub = subs[u]
        for name in ("lo1", "hi0", "lo0", "hi1"):
            a[part, name, u].wait_recv()
        for h in (lo, hi):
            which = 0 if h is lo else 1
            red[part, sub, h] = (
                acc[part, OWN, sub, h].astype(F32)
                + r_low[part, which, sub].astype(F32)
                + r_high[part, which, sub].astype(F32)
            ).astype(BF16)

    both = (0, 1)
    for part in both:
        fill(part, FAR)
        send_far(part, 0)
    for part in both:
        fill(part, NXT)
        fill(part, PRV)
        send_near(part, 0)
    for part in both:
        send_far(part, 1)
        send_near(part, 1)
    for part in both:
        fill(part, OWN)
    for part in both:
        middle(part, 0)
    for part in both:
        send_far(part, 2)
        send_near(part, 2)
    for part in both:
        middle(part, 1)
    for part in both:
        reduce(part, 0)
        go(part, "tu", 0, red.at[part, FAR, lo], t_far.at[part, 0], second, 1)
        go(part, "td", 0, red.at[part, FAR, hi], t_far.at[part, 1], second, -1)
    for part in both:
        middle(part, 2)
    for part in both:
        reduce(part, 1)
        go(part, "tl1", 0, red.at[part, NXT, hi], t_low.at[part, 1], second, 1)
        go(part, "th0", 0, red.at[part, PRV, lo], t_high.at[part, 0], second, -1)
    for part in both:
        a[part, "tu", 0].wait_recv()
        t_far[part, 0] = (
            t_far[part, 0].astype(F32) + red[part, NXT, lo].astype(F32)
        ).astype(BF16)
        go(part, "tl0", 0, t_far.at[part, 0], t_low.at[part, 0], second, 1)
        a[part, "td", 0].wait_recv()
        t_far[part, 1] = (
            t_far[part, 1].astype(F32) + red[part, PRV, hi].astype(F32)
        ).astype(BF16)
        go(part, "th1", 0, t_far.at[part, 1], t_high.at[part, 1], second, -1)
    for part in both:
        reduce(part, 2)
    for part in both:
        for name in ("tl1", "th0", "tl0", "th1"):
            a[part, name, 0].wait_recv()
        for h in (0, 1):
            fin[part, pl.ds(3 * h, 3)] = (
                red[part, OWN, pl.ds(3 * h, 3)].astype(F32)
                + t_low[part, h].astype(F32)
                + t_high[part, h].astype(F32)
            )
    last = send(fin.at[1 - core], tot.at[core], sib)
    tot[core] = fin[core]
    last.wait_recv()

    start, n = starts[me], counts[me]
    factor = 1.0 / np.sqrt(np.float32(LEN * 32))
    for t in range(SLOTS):
        b = start + t
        parity = lax.rem(b, 2)
        v = tot[parity, b // 2 - (start + 1 - parity) // 2] * factor
        v = jnp.where(b < NQKV, v.T, v)
        out[t] = jnp.where(t < n, v, 0.0)
    for copy in sends:
        copy.wait_send()


def main(counts, cos, sin, sides, wo, curv, probs, qkv, normed):
    vmem = pl.BlockSpec(memory_space=pltpu.VMEM)
    hbm = pl.BlockSpec(memory_space=pl.ANY)
    smem = pl.BlockSpec(memory_space=pltpu.SMEM)
    block = (BLK, BLK)
    half = LEN // 2
    v = pltpu.VMEM
    return pl.pallas_call(
        main_kernel,
        out_shape=jax.ShapeDtypeStruct((SLOTS,) + block, F32),
        in_specs=[smem, vmem, vmem] + [hbm] * 6,
        out_specs=vmem,
        scratch_shapes=[
            pltpu.SMEM((32,), jnp.int32),
            v((2, LEN, OUT), BF16),
            v((4, 2, OUT, CHUNK), BF16),
            v((LEN, CHUNK), BF16),
            v((QH, LEN, LEN), BF16),
            v((LEN, QKV), BF16),
            v((LEN, D), BF16),
            v((4, 2, LEN, SUB), BF16),
            v((2, 2, half, SUB), BF16),
            v((2, 2, half, SUB), BF16),
            v((2, 2, half, SUB), BF16),
            v((4, 2, LEN, SUB), BF16),
            v((LEN, OUT), F32),
            v((QKV, LEN), BF16),
            v((2, NB // 2) + block, BF16),
            v((NB // 2,) + block, BF16),
            v((2, 4, 4, HALF) + block, BF16),
            v((2, 2, 4, 3) + block, BF16),
            v((2, 2, 4, 3) + block, BF16),
            v((2, 2, 4, 3) + block, BF16),
            v((2, 4, HALF) + block, BF16),
            v((2, 2, 3) + block, BF16),
            v((2, 2, 3) + block, BF16),
            v((2, 2, 3) + block, BF16),
            v((2, HALF) + block, F32),
            v((2, HALF) + block, F32),
            pltpu.SemaphoreType.DMA((82,)),
            pltpu.SemaphoreType.DMA((82,)),
            pltpu.SemaphoreType.DMA((9,)),
        ],
        compiler_params=pltpu.CompilerParams(
            collective_id=1, has_side_effects=True, vmem_limit_bytes=67_000_000
        ),
        name="main",
    )(counts, cos, sin, sides, wo, curv, probs, qkv, normed)


def local(tokens, norm_gain, curvature, weight_slots, probe_slots, block_counts):
    counts = block_counts[0]
    cos, sin = tables()
    normed, qkv, sides, probs, wo = forward(
        counts, weight_slots[0], probe_slots[0], norm_gain.reshape(1, D), tokens[0], cos, sin
    )
    out = main(counts, cos, sin, sides, wo, curvature[0], probs, qkv, normed)
    return out[None]


def solution(mesh):
    in_specs = (
        P("fsdp", None, None),
        P(),
        P("fsdp", None, None),
        P("seq", "fsdp", None, None),
        P("seq", "fsdp", None, None),
        P("seq", None),
    )
    out_specs = P("seq", "fsdp", None, None)
    return jax.shard_map(local, mesh=mesh, in_specs=in_specs, out_specs=out_specs, check_vma=False)
```

```python
import functools

import jax
import jax.numpy as jnp
import numpy as np
from jax import lax
from jax.experimental import pallas as pl
from jax.experimental.pallas import tpu as pltpu
from jax.sharding import PartitionSpec as P

D = 4096
HD = 128
BLK = 128
LEN = 512
QH = 4
QKV = 768
OUT = 512
NQKV = 192
NB = 320
SLOTS = 12
HALF = 6
CHUNK = 1024
FAR, NXT, PRV, OWN = 0, 1, 2, 3
THETA = 500000.0
EPS = 1e-05
NEGATIVE = -1e30
VMEM_LIMIT = 66_000_000
MESH = pl.DeviceIdType.MESH
F32 = jnp.float32
BF16 = jnp.bfloat16


def tables():
    half = HD // 2
    frequency = np.exp(-np.log(THETA) * 2.0 * np.arange(half) / HD)
    angles = np.arange(LEN)[:, None] * frequency[None, :]
    c, s = np.cos(angles), np.sin(angles)
    return (
        np.concatenate([c, c], axis=1).astype(np.float32),
        np.concatenate([-s, s], axis=1).astype(np.float32),
    )


def place():
    me = lax.axis_index("fsdp")
    core = lax.rem(me, 2)
    y = lax.rem(me // 2, 4)
    z = me // 8
    return me, core, y, z


def index_of(z, y, core):
    return (z * 4 + y) * 2 + core


def wrap(a):
    return lax.rem(a + 4, 4)


def greet(targets):
    barrier = pltpu.get_barrier_semaphore()
    for t in targets:
        pl.semaphore_signal(barrier, inc=1, device_id=t, device_id_type=MESH)
    pl.semaphore_wait(barrier, len(targets))


def nt(a, b):
    return lax.dot_general(a, b, (((1,), (1,)), ((), ())), preferred_element_type=F32)


def nn(a, b):
    return jnp.dot(a, b, preferred_element_type=F32)


def causal_mask():
    row = lax.broadcasted_iota(jnp.int32, (LEN, LEN), 0)
    col = lax.broadcasted_iota(jnp.int32, (LEN, LEN), 1)
    return row >= col


def kernel(
    counts, w_in, p_in, gain, tokens_in, cos_in, sin_in, curv_in,
    out,
    table, starts, slots_w, slots_p, normed, cos, sin, wqkv, wout, proj, sides, probs, qkv,
    opp, low, high, wt, r_far, r_low, r_high, t_far, t_low, t_high, tot,
    send_sem, recv_sem, local_sem, ready,
):
    me, core, y, z = place()
    x = lax.axis_index("seq")
    sib = {"fsdp": index_of(z, y, 1 - core)}
    up, down = {"seq": wrap(x + 1)}, {"seq": wrap(x - 1)}

    def at(axis, step):
        if axis == "y":
            return {"fsdp": index_of(z, wrap(y + step), core)}
        return {"fsdp": index_of(wrap(z + step), y, core)}

    my_slots = pl.ds(me * SLOTS, SLOTS)
    local = [
        pltpu.make_async_copy(a, b, local_sem.at[i])
        for i, (a, b) in enumerate(
            (
                (w_in, slots_w.at[my_slots]),
                (p_in, slots_p.at[my_slots]),
                (tokens_in, normed),
                (cos_in, cos),
                (sin_in, sin),
            )
        )
    ]
    for copy in local:
        copy.start()
    greet([up, down, at("y", 1), at("y", -1), at("z", 1), at("z", -1), sib])

    first = ("y", "z", "y", "z")
    second = ("z", "y", "z", "y")
    landed = (slots_w, slots_w, slots_p, slots_p)
    counter = [0]
    sends = []
    arrivals = {}

    def send(key, src, dst, target):
        number = counter[0]
        counter[0] += 1
        copy = pltpu.make_async_remote_copy(
            src_ref=src,
            dst_ref=dst,
            send_sem=send_sem.at[number],
            recv_sem=recv_sem.at[number],
            device_id=target,
            device_id_type=MESH,
        )
        copy.start()
        sends.append(copy)
        arrivals[key] = copy
        return copy

    def span(p, side):
        start = (p % 2) * HALF
        return (start, HALF) if side is None else (start + 3 * side, 3)

    def piece(p, origin, side=None):
        start, size = span(p, side)
        return landed[p].at[pl.ds(origin * SLOTS + start, size)]

    def origin_of(p, f, s):
        if p % 2 == 0:
            return index_of(wrap(z + s), wrap(y + f), core)
        return index_of(wrap(z + f), wrap(y + s), core)

    def go(p, role, f, s, axis, step, side=None):
        ref = piece(p, origin_of(p, f, s), side)
        send((p,) + role, ref, ref, at(axis[p], step))

    def to_sib(p, f, s):
        ref = piece(p, origin_of(p, f, s))
        send((p, "sib", f, s), ref, ref, sib)

    def got(*key):
        arrivals[key].wait_recv()

    def begin(parts):
        for p in parts:
            go(p, ("f+",), 0, 0, first, 1)
            go(p, ("f-",), 0, 0, first, -1)
        for p in parts:
            go(p, ("s+", 0), 0, 0, second, 1)
            go(p, ("s-", 0), 0, 0, second, -1)
        for p in parts:
            to_sib(p, 0, 0)

    def neighbours(p):
        got(p, "f+")
        go(p, ("fa",), -1, 0, first, 1, 0)
        go(p, ("s+", -1), -1, 0, second, 1)
        go(p, ("s-", -1), -1, 0, second, -1)
        got(p, "f-")
        go(p, ("fb",), 1, 0, first, -1, 1)
        go(p, ("s+", 1), 1, 0, second, 1)
        go(p, ("s-", 1), 1, 0, second, -1)
        to_sib(p, -1, 0)
        to_sib(p, 1, 0)

    def pass_on(p, f):
        got(p, "s+", f)
        go(p, ("sa", f), f, -1, second, 1, 0)
        to_sib(p, f, -1)
        got(p, "s-", f)
        go(p, ("sb", f), f, 1, second, -1, 1)
        to_sib(p, f, 1)

    def opposite(p):
        got(p, "fa")
        got(p, "fb")
        go(p, ("s+", 2), 2, 0, second, 1)
        go(p, ("s-", 2), 2, 0, second, -1)
        to_sib(p, 2, 0)

    def corner(p, f):
        got(p, "sa", f)
        got(p, "sb", f)
        to_sib(p, f, 2)

    def sibling_done(parts):
        for p in parts:
            for f in (0, -1, 1, 2):
                for s in (0, -1, 1, 2):
                    got(p, "sib", f, s)

    w, pr = (0, 1), (2, 3)
    local[0].wait()
    local[1].wait()
    begin(w)

    def locate(b, carry):
        d, t = carry
        table[b] = d * SLOTS + t
        more = t + 1 < counts[d]
        return jnp.where(more, d, jnp.minimum(d + 1, 31)), jnp.where(more, t + 1, 0)

    lax.fori_loop(0, NB, locate, (0, 0))

    def prefix(d, s):
        starts[d] = s
        return s + counts[d]

    lax.fori_loop(0, 32, prefix, 0)
    local[2].wait()

    def norm(i, carry):
        rows = pl.ds(pl.multiple_of(i * 32, 32), 32)
        x = normed[rows, :].astype(F32)
        factor = lax.rsqrt(jnp.mean(x * x, axis=-1, keepdims=True) + EPS)
        normed[rows, :] = (x * factor * gain[...]).astype(BF16)
        return carry

    lax.fori_loop(0, LEN // 32, norm, 0)
    local[3].wait()
    local[4].wait()

    def cols_of(h):
        return pl.ds(h * HD if isinstance(h, int) else pl.multiple_of(h * HD, HD), HD)

    def assemble_qkv(src):
        def step(r, carry):
            rows = pl.ds(pl.multiple_of(r * BLK, BLK), BLK)
            for c in range(6):
                wqkv[rows, c * BLK : (c + 1) * BLK] = src[table[r * 6 + c]]
            return carry

        lax.fori_loop(0, 32, step, 0)

    def assemble_out(src, tensor):
        def step(i, carry):
            rows = pl.ds(pl.multiple_of(i * BLK, BLK), BLK)
            for j in range(32):
                wout[tensor, j // 8, rows, (j % 8) * BLK : (j % 8 + 1) * BLK] = src[
                    table[NQKV + i * 32 + j]
                ]
            return carry

        lax.fori_loop(0, 4, step, 0)

    all_rows = slice(0, LEN)
    half = LEN // 2
    halves = (slice(0, half), slice(half, LEN))

    def project(n, rows=all_rows):
        cols = slice(n * 256, (n + 1) * 256)
        proj[rows, cols] = nn(normed[rows, :], wqkv[:, cols])

    def head(h, turn=True, rows=all_rows):
        v = proj[rows, cols_of(h)]
        if turn:
            v = v * cos[rows, :] + pltpu.roll(v, 64, 1) * sin[rows, :]
        return v.astype(BF16)

    def heads():
        for h in range(QH + 2):
            qkv[:, cols_of(h)] = head(h, h < QH + 1)

    scale = HD**-0.5

    def primal(h, carry):
        k = qkv[:, cols_of(QH)]
        v = qkv[:, cols_of(QH + 1)]
        s = jnp.where(causal_mask(), nt(qkv[:, cols_of(h)], k) * scale, NEGATIVE)
        m = jnp.max(s, axis=-1, keepdims=True)
        e = jnp.exp(s - m)
        p = (e * (1.0 / jnp.sum(e, axis=-1, keepdims=True))).astype(BF16)
        probs[h] = p
        sides[1, :, cols_of(h)] = nn(p, v).astype(BF16)
        return carry

    for p in w:
        neighbours(p)
    for p in w:
        pass_on(p, 0)
    for p in w:
        opposite(p)
    begin(pr)
    for f in (-1, 1):
        for p in w:
            pass_on(p, f)
    for p in w:
        corner(p, 0)
    for p in w:
        pass_on(p, 2)
    for p in pr:
        neighbours(p)
    for p in pr:
        pass_on(p, 0)
    for f in (-1, 1, 2):
        for p in w:
            corner(p, f)
    for p in pr:
        opposite(p)
    sibling_done(w)
    assemble_qkv(slots_w)
    project(0)
    for p in pr:
        pass_on(p, -1)
    for p in pr:
        corner(p, 0)
    project(1)
    project(2)
    for p in pr:
        pass_on(p, 1)
    heads()
    lax.fori_loop(0, 2, primal, 0)
    for p in pr:
        pass_on(p, 2)
    lax.fori_loop(2, 4, primal, 0)
    assemble_out(slots_w, 0)
    for f in (-1, 1, 2):
        for p in pr:
            corner(p, f)
    sibling_done(pr)

    chunk = (wrap(x + 2), wrap(x + 1), wrap(x - 1), x)
    key_tangent, value_tangent = cols_of(0), cols_of(1)

    def tangent(s):
        rows, seen = halves[s], slice(0, half * (s + 1))
        for n in range(3):
            project(n, rows)
        wt[OWN, rows, key_tangent] = head(QH, True, rows)
        wt[OWN, rows, value_tangent] = head(QH + 1, False, rows)
        keys = jnp.concatenate([qkv[seen, cols_of(QH)], wt[OWN, seen, key_tangent]], axis=1)

        def one(h, carry):
            pb = probs[h, rows, seen]
            pf = pb.astype(F32)
            side = jnp.concatenate([head(h, True, rows), qkv[rows, cols_of(h)]], axis=1)
            pt = pf * (nt(side, keys) * scale)
            tp = (pt - pf * jnp.sum(pt, axis=-1, keepdims=True)).astype(BF16)
            sides[0, rows, cols_of(h)] = (
                nn(tp, qkv[seen, cols_of(QH + 1)]) + nn(pb, wt[OWN, seen, value_tangent])
            ).astype(BF16)
            return carry

        lax.fori_loop(0, QH, one, 0)

    def term_at(rel, s, part):
        return ((rel * 2 + s) * 2 + part) * 8

    def term(rel, s):
        rows = halves[s]
        for n in range(2):
            cols = slice(n * 512, (n + 1) * 512)
            v = (
                nn(sides[0, rows, :], wout[0, chunk[rel], :, cols])
                + nn(sides[1, rows, :], wout[1, chunk[rel], :, cols])
            ).astype(BF16)
            for part in (0, 1):
                for j in range(4):
                    slots_p[term_at(rel, s, part) + 4 * n + j] = v[
                        part * BLK : (part + 1) * BLK, j * BLK : (j + 1) * BLK
                    ]

    def terms(rel, s, part):
        return slots_p.at[pl.ds(term_at(rel, s, part), 8)]

    def cast(name, src, dst, target):
        return send(name, src, dst, target)

    assemble_qkv(slots_p)
    assemble_out(slots_p, 1)
    tangent(0)
    for copy in sends:
        copy.wait_send()
    sends.clear()
    pl.semaphore_signal(ready, inc=1, device_id=sib, device_id_type=MESH)
    for s in (0, 1):
        if s == 1:
            tangent(1)
        term(FAR, s)
        cast(("a0", s), terms(FAR, s, 0), opp.at[0, s], up)
        cast(("b0", s), terms(FAR, s, 1), opp.at[1, s], down)
        term(NXT, s)
        term(PRV, s)
        if s == 0:
            cast(("a1", s), terms(NXT, s, 1), low.at[1, s], up)
            cast(("b1", s), terms(PRV, s, 0), high.at[0, s], down)
    curv_loads = []
    for n in range(2):
        curv_loads.append(
            pltpu.make_async_copy(
                curv_in.at[:, pl.ds(pl.multiple_of(x * CHUNK + n * 512, 512), 512)],
                wqkv.at[n * LEN : (n + 1) * LEN, 0:512],
                local_sem.at[5 + n],
            )
        )
        curv_loads[-1].start()
    for s in (0, 1):
        got("a0", s)
        mine = slots_p[pl.ds(term_at(NXT, s, 0), 8)].astype(F32)
        opp[0, s] = (opp[0, s].astype(F32) + mine).astype(BF16)
        cast(("a2", s), opp.at[0, s], low.at[0, s], up)
        got("b0", s)
        mine = slots_p[pl.ds(term_at(PRV, s, 1), 8)].astype(F32)
        opp[1, s] = (opp[1, s].astype(F32) + mine).astype(BF16)
        cast(("b2", s), opp.at[1, s], high.at[1, s], down)
        if s == 0:
            cast(("a1", 1), terms(NXT, 1, 1), low.at[1, 1], up)
            cast(("b1", 1), terms(PRV, 1, 0), high.at[0, 1], down)
            term(OWN, 0)
            term(OWN, 1)
            turned = slice(2 * LEN, 3 * LEN)
            wqkv[turned, 0:512] = sides[1].T
            for copy in curv_loads:
                copy.wait()

    def part_rows(s, part):
        return pl.ds(s * half + part * BLK, BLK)

    def weigh(part, s):
        rows = s * half + part * BLK
        for j in range(8):
            total = (
                slots_p[term_at(OWN, s, part) + j].astype(F32)
                + low[part, s, j].astype(F32)
                + high[part, s, j].astype(F32)
            )
            at_row = (j // 4) * LEN + rows
            c = wqkv[at_row : at_row + BLK, (j % 4) * BLK : (j % 4 + 1) * BLK].astype(F32)
            wt[OWN, rows : rows + BLK, j * BLK : (j + 1) * BLK] = (total * c).astype(BF16)

    def hand_on(name, src, dst, part, s, target):
        r = part_rows(s, part)
        cast((name, s), wt.at[src, r], wt.at[dst, r], target)

    def mixed_cotangent(rel, s):
        rows = halves[s]
        v = nt(wt[rel, rows, :], wout[0, chunk[rel]])
        if rel == OWN:
            proj[rows, 0:OUT] = v
        else:
            proj[rows, 0:OUT] += v

    per = NB // 2
    n_in = NQKV // 2

    def out_gradient(rel):
        for n in range(2):
            g = nn(wqkv[turned, 0:512], wt[rel, :, n * 512 : (n + 1) * 512]).astype(BF16)
            for i in range(4):
                for j in range(4):
                    slots_w[(j % 2) * per + n_in + 16 * i + 4 * chunk[rel] + 2 * n + j // 2] = g[
                        i * BLK : (i + 1) * BLK, j * BLK : (j + 1) * BLK
                    ]

    for s in (0, 1):
        got("a1", s)
        got("b2", s)
        weigh(1, s)
        hand_on("c1", OWN, PRV, 1, s, up)
        hand_on("d1", OWN, NXT, 1, s, down)
        got("b1", s)
        got("a2", s)
        weigh(0, s)
        hand_on("d0", OWN, NXT, 0, s, down)
        hand_on("c0", OWN, PRV, 0, s, up)
        mixed_cotangent(OWN, s)
    for s in (0, 1):
        got("c1", s)
        hand_on("e1", PRV, FAR, 1, s, up)
        got("d0", s)
        hand_on("e0", NXT, FAR, 0, s, down)
        if s == 0:
            out_gradient(OWN)
        got("d1", s)
        mixed_cotangent(NXT, s)
        got("c0", s)
        mixed_cotangent(PRV, s)
    got("e1", 0)
    got("e0", 0)
    mixed_cotangent(FAR, 0)

    def unrot(v, rows):
        return v * cos[rows, :] - pltpu.roll(v, 64, 1) * sin[rows, :]

    tail = slice(OUT, QKV)
    proj[:, tail] = jnp.zeros((LEN, QKV - OUT), F32)

    def attention_back(s):
        rows, seen = halves[s], slice(0, half * (s + 1))

        def one(h, carry):
            dm = proj[rows, cols_of(h)].astype(BF16)
            q = qkv[rows, cols_of(h)]
            pb = probs[h, rows, seen]
            dp = nt(dm, qkv[seen, cols_of(QH + 1)]).astype(BF16).astype(F32)
            pf = pb.astype(F32)
            pd = pf * dp
            ds = ((pd - pf * jnp.sum(pd, axis=-1, keepdims=True)) * scale).astype(BF16)
            dk = nn(q.T, ds)
            dv = nn(dm.T, pb)
            for u in range(s + 1):
                proj[u * BLK : (u + 1) * BLK, tail] += dk[:, u * half : (u + 1) * half]
                proj[half + u * BLK : half + (u + 1) * BLK, tail] += dv[
                    :, u * half : (u + 1) * half
                ]
            dq = unrot(nn(ds, qkv[seen, cols_of(QH)]).astype(BF16).astype(F32), rows).astype(BF16)
            sides[0, cols_of(h), rows] = dq.T
            return carry

        lax.fori_loop(0, QH, one, 0)

    attention_back(0)
    out_gradient(NXT)
    out_gradient(PRV)
    got("e1", 1)
    got("e0", 1)
    out_gradient(FAR)
    pl.semaphore_wait(ready, 1)
    sb = 192
    out_part = pl.ds((1 - core) * per + n_in, per - n_in)
    cast(("swap", 8), slots_w.at[out_part], slots_p.at[pl.ds(sb + n_in, per - n_in)], sib)
    mixed_cotangent(FAR, 1)
    attention_back(1)
    for u in range(2):
        dk = proj[u * BLK : (u + 1) * BLK, tail].astype(BF16).astype(F32).T
        sides[1, 0:BLK, halves[u]] = unrot(dk, halves[u]).astype(BF16).T
        sides[1, BLK : 2 * BLK, halves[u]] = proj[
            half + u * BLK : half + (u + 1) * BLK, tail
        ].astype(BF16)
    for n in range(8):
        cols = slice(n * 512, (n + 1) * 512)
        for c0, lhs in ((0, sides[0]), (4, sides[1, 0 : 2 * BLK, :])):
            g = nn(lhs, normed[:, cols]).astype(BF16)
            for r in range(4):
                for c in range(lhs.shape[0] // BLK):
                    slots_w[((c0 + c) % 2) * per + 3 * (4 * n + r) + (c0 + c) // 2] = g[
                        c * BLK : (c + 1) * BLK, r * BLK : (r + 1) * BLK
                    ]
        cast(
            ("swap", n),
            slots_w.at[pl.ds((1 - core) * per + 12 * n, 12)],
            slots_p.at[pl.ds(sb + 12 * n, 12)],
            sib,
        )
    for n in (8, 0, 1, 2, 3, 4, 5, 6, 7):
        got("swap", n)
    for copy in sends:
        copy.wait_send()
    sends.clear()

    chain = (("z", "y"), ("y", "z"))
    here = {"y": y, "z": z}
    steps = (2, 1, -1, 0)

    def acc_at(part, rel, h):
        return ((part * 4 + rel) * 2 + h) * 12

    def red_at(part, h, srel):
        return 2 * per + (part * 2 + h) * 12 + 3 * srel

    def fill(part, rel):
        f = wrap(here[chain[part][0]] + steps[rel])
        for srel in range(4):
            s = wrap(here[chain[part][1]] + steps[srel])
            d = index_of(f, s, part) if part == 0 else index_of(s, f, part)
            base = (starts[d] + 1 - core) // 2
            for i in range(HALF):
                j = jnp.minimum(base + i, per - 1)
                slots_p[acc_at(part, rel, i // 3) + 3 * srel + i % 3] = (
                    slots_w[core * per + j].astype(F32) + slots_p[sb + j].astype(F32)
                ).astype(BF16)

    subs = ((0, 3), (3, 6), (9, 3))

    def acc(part, rel, h, u):
        return pl.ds(acc_at(part, rel, h) + subs[u][0], subs[u][1])

    def ring(part, name, u, src, dst, leg, step):
        send((part, name, u), src, dst, at(chain[part][leg], step))

    def send_far(part, u):
        sub = pl.ds(*subs[u])
        ring(part, "fu", u, slots_p.at[acc(part, FAR, 0, u)], r_far.at[part, 0, sub], 0, 1)
        ring(part, "fd", u, slots_p.at[acc(part, FAR, 1, u)], r_far.at[part, 1, sub], 0, -1)

    def send_near(part, u):
        sub = pl.ds(*subs[u])
        ring(part, "lo1", u, slots_p.at[acc(part, NXT, 1, u)], r_low.at[part, 1, sub], 0, 1)
        ring(part, "hi0", u, slots_p.at[acc(part, PRV, 0, u)], r_high.at[part, 0, sub], 0, -1)

    def middle(part, u):
        sub = pl.ds(*subs[u])
        got(part, "fu", u)
        r_far[part, 0, sub] = (
            r_far[part, 0, sub].astype(F32) + slots_p[acc(part, NXT, 0, u)].astype(F32)
        ).astype(BF16)
        ring(part, "lo0", u, r_far.at[part, 0, sub], r_low.at[part, 0, sub], 0, 1)
        got(part, "fd", u)
        r_far[part, 1, sub] = (
            r_far[part, 1, sub].astype(F32) + slots_p[acc(part, PRV, 1, u)].astype(F32)
        ).astype(BF16)
        ring(part, "hi1", u, r_far.at[part, 1, sub], r_high.at[part, 1, sub], 0, -1)

    def reduce(part, u):
        sub = pl.ds(*subs[u])
        for name in ("lo1", "hi0", "lo0", "hi1"):
            got(part, name, u)
        for h in (0, 1):
            slots_w[pl.ds(red_at(part, h, 0) + subs[u][0], subs[u][1])] = (
                slots_p[acc(part, OWN, h, u)].astype(F32)
                + r_low[part, h, sub].astype(F32)
                + r_high[part, h, sub].astype(F32)
            ).astype(BF16)

    def red(part, h, srel):
        return pl.ds(red_at(part, h, srel), 3)

    both = (0, 1)
    for part in both:
        fill(part, FAR)
        send_far(part, 0)
    for part in both:
        fill(part, NXT)
        fill(part, PRV)
        send_near(part, 0)
    for part in both:
        send_far(part, 1)
        send_near(part, 1)
    for part in both:
        fill(part, OWN)
    for part in both:
        middle(part, 0)
    for part in both:
        send_far(part, 2)
        send_near(part, 2)
    for part in both:
        middle(part, 1)
    for part in both:
        reduce(part, 0)
        ring(part, "tu", 0, slots_w.at[red(part, 0, FAR)], t_far.at[part, 0], 1, 1)
        ring(part, "td", 0, slots_w.at[red(part, 1, FAR)], t_far.at[part, 1], 1, -1)
    for part in both:
        middle(part, 2)
    for part in both:
        reduce(part, 1)
        ring(part, "tl1", 0, slots_w.at[red(part, 1, NXT)], t_low.at[part, 1], 1, 1)
        ring(part, "th0", 0, slots_w.at[red(part, 0, PRV)], t_high.at[part, 0], 1, -1)
    for part in both:
        got(part, "tu", 0)
        t_far[part, 0] = (
            t_far[part, 0].astype(F32) + slots_w[red(part, 0, NXT)].astype(F32)
        ).astype(BF16)
        ring(part, "tl0", 0, t_far.at[part, 0], t_low.at[part, 0], 1, 1)
        got(part, "td", 0)
        t_far[part, 1] = (
            t_far[part, 1].astype(F32) + slots_w[red(part, 1, PRV)].astype(F32)
        ).astype(BF16)
        ring(part, "th1", 0, t_far.at[part, 1], t_high.at[part, 1], 1, -1)
    for part in both:
        reduce(part, 2)
    for part in both:
        for name in ("tl1", "th0", "tl0", "th1"):
            got(part, name, 0)

    def whole(part, h):
        return (
            slots_w[pl.ds(2 * per + (part * 2 + h) * 12 + 3 * OWN, 3)].astype(F32)
            + t_low[part, h].astype(F32)
            + t_high[part, h].astype(F32)
        )

    for h in (0, 1):
        out[pl.ds(3 * h, 3)] = whole(1 - core, h)
    last = cast(("last",), out.at[pl.ds(0, HALF)], tot.at[core], sib)
    for h in (0, 1):
        tot[core, pl.ds(3 * h, 3)] = whole(core, h)
    last.wait_recv()
    for copy in sends:
        copy.wait_send()

    start, n = starts[me], counts[me]
    factor = 1.0 / np.sqrt(np.float32(LEN * 32))
    for t in range(SLOTS):
        b = start + t
        parity = lax.rem(b, 2)
        v = tot[parity, b // 2 - (start + 1 - parity) // 2] * factor
        v = jnp.where(b < NQKV, v.T, v)
        out[t] = jnp.where(t < n, v, 0.0)


def product(counts, w, p, gain, tokens, cos, sin, curv):
    vmem = pl.BlockSpec(memory_space=pltpu.VMEM)
    hbm = pl.BlockSpec(memory_space=pl.ANY)
    smem = pl.BlockSpec(memory_space=pltpu.SMEM)
    v = pltpu.VMEM
    block = (BLK, BLK)
    return pl.pallas_call(
        kernel,
        out_shape=jax.ShapeDtypeStruct((SLOTS,) + block, F32),
        in_specs=[smem, hbm, hbm, vmem, hbm, hbm, hbm, hbm],
        out_specs=vmem,
        scratch_shapes=[
            pltpu.SMEM((NB,), jnp.int32),
            pltpu.SMEM((32,), jnp.int32),
            v((32 * SLOTS,) + block, BF16),
            v((32 * SLOTS,) + block, BF16),
            v((LEN, D), BF16),
            v((LEN, HD), F32),
            v((LEN, HD), F32),
            v((D, QKV), BF16),
            v((2, 4, OUT, CHUNK), BF16),
            v((LEN, QKV), F32),
            v((2, LEN, OUT), BF16),
            v((QH, LEN, LEN), BF16),
            v((LEN, QKV), BF16),
            v((2, 2, 8) + block, BF16),
            v((2, 2, 8) + block, BF16),
            v((2, 2, 8) + block, BF16),
            v((4, LEN, CHUNK), BF16),
            v((2, 2, 12) + block, BF16),
            v((2, 2, 12) + block, BF16),
            v((2, 2, 12) + block, BF16),
            v((2, 2, 3) + block, BF16),
            v((2, 2, 3) + block, BF16),
            v((2, 2, 3) + block, BF16),
            v((2, HALF) + block, F32),
            pltpu.SemaphoreType.DMA((226,)),
            pltpu.SemaphoreType.DMA((226,)),
            pltpu.SemaphoreType.DMA((7,)),
            pltpu.SemaphoreType.REGULAR,
        ],
        compiler_params=pltpu.CompilerParams(
            collective_id=0, has_side_effects=True, vmem_limit_bytes=67_000_000
        ),
        name="product",
    )(counts, w, p, gain, tokens, cos, sin, curv)


def local(tokens, norm_gain, curvature, weight_slots, probe_slots, block_counts):
    counts = block_counts[0]
    cos, sin = tables()
    out = product(
        counts,
        weight_slots[0],
        probe_slots[0],
        norm_gain.reshape(1, D),
        tokens[0],
        cos,
        sin,
        curvature[0],
    )
    return out[None]


def solution(mesh):
    in_specs = (
        P("fsdp", None, None),
        P(),
        P("fsdp", None, None),
        P("seq", "fsdp", None, None),
        P("seq", "fsdp", None, None),
        P("seq", None),
    )
    out_specs = P("seq", "fsdp", None, None)
    return jax.shard_map(local, mesh=mesh, in_specs=in_specs, out_specs=out_specs, check_vma=False)
```

```python
import functools

import jax
import jax.numpy as jnp
import numpy as np
from jax import lax
from jax.experimental import pallas as pl
from jax.experimental.pallas import tpu as pltpu
from jax.sharding import PartitionSpec as P

D = 4096
HD = 128
BLK = 128
LEN = 512
QH = 4
QKV = 768
OUT = 512
NQKV = 192
NB = 320
SLOTS = 12
HALF = 6
CHUNK = 1024
FAR, NXT, PRV, OWN = 0, 1, 2, 3
THETA = 500000.0
EPS = 1e-05
NEGATIVE = -1e30
VMEM_LIMIT = 66_000_000
MESH = pl.DeviceIdType.MESH
F32 = jnp.float32
BF16 = jnp.bfloat16


def tables():
    half = HD // 2
    frequency = np.exp(-np.log(THETA) * 2.0 * np.arange(half) / HD)
    angles = np.arange(LEN)[:, None] * frequency[None, :]
    c, s = np.cos(angles), np.sin(angles)
    return (
        np.concatenate([c, c], axis=1).astype(np.float32),
        np.concatenate([-s, s], axis=1).astype(np.float32),
    )


def place():
    me = lax.axis_index("fsdp")
    core = lax.rem(me, 2)
    y = lax.rem(me // 2, 4)
    z = me // 8
    return me, core, y, z


def index_of(z, y, core):
    return (z * 4 + y) * 2 + core


def wrap(a):
    return lax.rem(a + 4, 4)


def greet(targets):
    barrier = pltpu.get_barrier_semaphore()
    for t in targets:
        pl.semaphore_signal(barrier, inc=1, device_id=t, device_id_type=MESH)
    pl.semaphore_wait(barrier, len(targets))


def nt(a, b):
    return lax.dot_general(a, b, (((1,), (1,)), ((), ())), preferred_element_type=F32)


def nn(a, b):
    return jnp.dot(a, b, preferred_element_type=F32)


def causal_mask():
    row = lax.broadcasted_iota(jnp.int32, (LEN, LEN), 0)
    col = lax.broadcasted_iota(jnp.int32, (LEN, LEN), 1)
    return row >= col


def kernel(
    counts, w_in, p_in, gain, tokens_in, cos_in, sin_in, curv_in,
    out,
    table, starts, slots_w, slots_p, normed, cos, sin, wqkv, wout, proj, sides, probs, qkv,
    opp, low, high, wt, r_far, r_low, r_high, t_far, t_low, t_high, tot,
    send_sem, recv_sem, local_sem, ready,
):
    me, core, y, z = place()
    x = lax.axis_index("seq")
    sib = {"fsdp": index_of(z, y, 1 - core)}
    up, down = {"seq": wrap(x + 1)}, {"seq": wrap(x - 1)}

    def at(axis, step):
        if axis == "y":
            return {"fsdp": index_of(z, wrap(y + step), core)}
        return {"fsdp": index_of(wrap(z + step), y, core)}

    my_slots = pl.ds(me * SLOTS, SLOTS)
    local = [
        pltpu.make_async_copy(a, b, local_sem.at[i])
        for i, (a, b) in enumerate(
            (
                (w_in, slots_w.at[my_slots]),
                (p_in, slots_p.at[my_slots]),
                (tokens_in, normed),
                (cos_in, cos),
                (sin_in, sin),
            )
        )
    ]
    for copy in local:
        copy.start()
    greet([up, down, at("y", 1), at("y", -1), at("z", 1), at("z", -1), sib])

    first = ("y", "z", "y", "z")
    second = ("z", "y", "z", "y")
    landed = (slots_w, slots_w, slots_p, slots_p)
    counter = [0]
    sends = []
    arrivals = {}

    def send(key, src, dst, target):
        number = counter[0]
        counter[0] += 1
        copy = pltpu.make_async_remote_copy(
            src_ref=src,
            dst_ref=dst,
            send_sem=send_sem.at[number],
            recv_sem=recv_sem.at[number],
            device_id=target,
            device_id_type=MESH,
        )
        copy.start()
        sends.append(copy)
        arrivals[key] = copy
        return copy

    def span(p, side):
        start = (p % 2) * HALF
        return (start, HALF) if side is None else (start + 3 * side, 3)

    def piece(p, origin, side=None):
        start, size = span(p, side)
        return landed[p].at[pl.ds(origin * SLOTS + start, size)]

    def origin_of(p, f, s):
        if p % 2 == 0:
            return index_of(wrap(z + s), wrap(y + f), core)
        return index_of(wrap(z + f), wrap(y + s), core)

    def go(p, role, f, s, axis, step, side=None):
        ref = piece(p, origin_of(p, f, s), side)
        send((p,) + role, ref, ref, at(axis[p], step))

    def to_sib(p, f, s):
        ref = piece(p, origin_of(p, f, s))
        send((p, "sib", f, s), ref, ref, sib)

    def got(*key):
        arrivals[key].wait_recv()

    def begin(parts):
        for p in parts:
            go(p, ("f+",), 0, 0, first, 1)
            go(p, ("f-",), 0, 0, first, -1)
        for p in parts:
            go(p, ("s+", 0), 0, 0, second, 1)
            go(p, ("s-", 0), 0, 0, second, -1)
        for p in parts:
            to_sib(p, 0, 0)

    def neighbours(p):
        got(p, "f+")
        go(p, ("fa",), -1, 0, first, 1, 0)
        go(p, ("s+", -1), -1, 0, second, 1)
        go(p, ("s-", -1), -1, 0, second, -1)
        got(p, "f-")
        go(p, ("fb",), 1, 0, first, -1, 1)
        go(p, ("s+", 1), 1, 0, second, 1)
        go(p, ("s-", 1), 1, 0, second, -1)
        to_sib(p, -1, 0)
        to_sib(p, 1, 0)

    def pass_on(p, f):
        got(p, "s+", f)
        go(p, ("sa", f), f, -1, second, 1, 0)
        to_sib(p, f, -1)
        got(p, "s-", f)
        go(p, ("sb", f), f, 1, second, -1, 1)
        to_sib(p, f, 1)

    def opposite(p):
        got(p, "fa")
        got(p, "fb")
        go(p, ("s+", 2), 2, 0, second, 1)
        go(p, ("s-", 2), 2, 0, second, -1)
        to_sib(p, 2, 0)

    def corner(p, f):
        got(p, "sa", f)
        got(p, "sb", f)
        to_sib(p, f, 2)

    def sibling_done(parts):
        for p in parts:
            for f in (0, -1, 1, 2):
                for s in (0, -1, 1, 2):
                    got(p, "sib", f, s)

    w, pr = (0, 1), (2, 3)
    local[0].wait()
    local[1].wait()
    begin(w)

    def locate(b, carry):
        d, t = carry
        table[b] = d * SLOTS + t
        more = t + 1 < counts[d]
        return jnp.where(more, d, jnp.minimum(d + 1, 31)), jnp.where(more, t + 1, 0)

    lax.fori_loop(0, NB, locate, (0, 0))

    def prefix(d, s):
        starts[d] = s
        return s + counts[d]

    lax.fori_loop(0, 32, prefix, 0)
    local[2].wait()

    def norm(i, carry):
        rows = pl.ds(pl.multiple_of(i * 32, 32), 32)
        x = normed[rows, :].astype(F32)
        factor = lax.rsqrt(jnp.mean(x * x, axis=-1, keepdims=True) + EPS)
        normed[rows, :] = (x * factor * gain[...]).astype(BF16)
        return carry

    lax.fori_loop(0, LEN // 32, norm, 0)
    local[3].wait()
    local[4].wait()

    def cols_of(h):
        return pl.ds(h * HD if isinstance(h, int) else pl.multiple_of(h * HD, HD), HD)

    def assemble_qkv(src):
        def step(r, carry):
            rows = pl.ds(pl.multiple_of(r * BLK, BLK), BLK)
            for c in range(6):
                wqkv[rows, c * BLK : (c + 1) * BLK] = src[table[r * 6 + c]]
            return carry

        lax.fori_loop(0, 32, step, 0, unroll=2)

    def assemble_out_chunk(src, tensor, q):
        for i in range(4):
            for j in range(8):
                wout[tensor, q, i * BLK : (i + 1) * BLK, j * BLK : (j + 1) * BLK] = src[
                    table[NQKV + i * 32 + q * 8 + j]
                ]

    def assemble_out(src, tensor):
        def step(i, carry):
            rows = pl.ds(pl.multiple_of(i * BLK, BLK), BLK)
            for j in range(32):
                wout[tensor, j // 8, rows, (j % 8) * BLK : (j % 8 + 1) * BLK] = src[
                    table[NQKV + i * 32 + j]
                ]
            return carry

        lax.fori_loop(0, 4, step, 0)

    all_rows = slice(0, LEN)
    half = LEN // 2
    halves = (slice(0, half), slice(half, LEN))

    def project(n, rows=all_rows):
        cols = slice(n * 256, (n + 1) * 256)
        proj[rows, cols] = nn(normed[rows, :], wqkv[:, cols])

    def head(h, turn=True, rows=all_rows):
        v = proj[rows, cols_of(h)]
        if turn:
            v = v * cos[rows, :] + pltpu.roll(v, 64, 1) * sin[rows, :]
        return v.astype(BF16)

    def heads():
        for h in range(QH + 2):
            qkv[:, cols_of(h)] = head(h, h < QH + 1)

    scale = HD**-0.5

    def primal(h, carry):
        k = qkv[:, cols_of(QH)]
        v = qkv[:, cols_of(QH + 1)]
        s = jnp.where(causal_mask(), nt(qkv[:, cols_of(h)], k) * scale, NEGATIVE)
        m = jnp.max(s, axis=-1, keepdims=True)
        e = jnp.exp(s - m)
        p = (e * (1.0 / jnp.sum(e, axis=-1, keepdims=True))).astype(BF16)
        probs[h] = p
        sides[1, :, cols_of(h)] = nn(p, v).astype(BF16)
        return carry

    for p in w:
        neighbours(p)
    for p in w:
        pass_on(p, 0)
    for p in w:
        opposite(p)
    begin(pr)
    for f in (-1, 1):
        for p in w:
            pass_on(p, f)
    for p in w:
        corner(p, 0)
    for p in w:
        pass_on(p, 2)
    for p in pr:
        neighbours(p)
    for p in pr:
        pass_on(p, 0)
    for f in (-1, 1, 2):
        for p in w:
            corner(p, f)
    for p in pr:
        opposite(p)
    sibling_done(w)
    assemble_qkv(slots_w)
    project(0)
    for p in pr:
        pass_on(p, -1)
    for p in pr:
        corner(p, 0)
    project(1)
    project(2)
    for p in pr:
        pass_on(p, 1)
    heads()
    lax.fori_loop(0, 2, primal, 0)
    for p in pr:
        pass_on(p, 2)
    lax.fori_loop(2, 4, primal, 0)
    assemble_out(slots_w, 0)
    for f in (-1, 1, 2):
        for p in pr:
            corner(p, f)
    sibling_done(pr)

    chunk = (wrap(x + 2), wrap(x + 1), wrap(x - 1), x)
    key_tangent, value_tangent = cols_of(0), cols_of(1)

    def tangent(s):
        rows, seen = halves[s], slice(0, half * (s + 1))
        for n in range(3):
            project(n, rows)
        wt[OWN, rows, key_tangent] = head(QH, True, rows)
        wt[OWN, rows, value_tangent] = head(QH + 1, False, rows)
        keys = jnp.concatenate([qkv[seen, cols_of(QH)], wt[OWN, seen, key_tangent]], axis=1)

        def one(h, carry):
            pb = probs[h, rows, seen]
            pf = pb.astype(F32)
            side = jnp.concatenate([head(h, True, rows), qkv[rows, cols_of(h)]], axis=1)
            pt = pf * (nt(side, keys) * scale)
            tp = (pt - pf * jnp.sum(pt, axis=-1, keepdims=True)).astype(BF16)
            sides[0, rows, cols_of(h)] = (
                nn(tp, qkv[seen, cols_of(QH + 1)]) + nn(pb, wt[OWN, seen, value_tangent])
            ).astype(BF16)
            return carry

        lax.fori_loop(0, QH, one, 0)

    def term_at(rel, s, part):
        return (0, 32, 64, 160)[rel] + (s * 2 + part) * 8

    def term(rel, s):
        rows = halves[s]
        for n in range(2):
            cols = slice(n * 512, (n + 1) * 512)
            v = (
                nn(sides[0, rows, :], wout[0, chunk[rel], :, cols])
                + nn(sides[1, rows, :], wout[1, chunk[rel], :, cols])
            ).astype(BF16)
            for part in (0, 1):
                for j in range(4):
                    slots_w[term_at(rel, s, part) + 4 * n + j] = v[
                        part * BLK : (part + 1) * BLK, j * BLK : (j + 1) * BLK
                    ]

    def terms(rel, s, part):
        return slots_w.at[pl.ds(term_at(rel, s, part), 8)]

    def cast(name, src, dst, target):
        return send(name, src, dst, target)

    assemble_qkv(slots_p)
    tangent(0)
    for copy in sends:
        copy.wait_send()
    sends.clear()
    for s in (0, 1):
        if s == 1:
            tangent(1)
        for rel in (FAR, NXT, PRV):
            if s == 0:
                assemble_out_chunk(slots_p, 1, chunk[rel])
            term(rel, s)
            if rel == FAR:
                cast(("a0", s), terms(FAR, s, 0), opp.at[0, s], up)
                cast(("b0", s), terms(FAR, s, 1), opp.at[1, s], down)
            if rel == NXT and s == 0:
                cast(("a1", s), terms(NXT, s, 1), low.at[1, s], up)
            if rel == PRV and s == 0:
                cast(("b1", s), terms(PRV, s, 0), high.at[0, s], down)
        if s == 0:
            assemble_out_chunk(slots_p, 1, chunk[OWN])
            pl.semaphore_signal(ready, inc=1, device_id=sib, device_id_type=MESH)
    curv_loads = []
    for n in range(2):
        curv_loads.append(
            pltpu.make_async_copy(
                curv_in.at[:, pl.ds(pl.multiple_of(x * CHUNK + n * 512, 512), 512)],
                wqkv.at[n * LEN : (n + 1) * LEN, 0:512],
                local_sem.at[5 + n],
            )
        )
        curv_loads[-1].start()
    for s in (0, 1):
        got("a0", s)
        mine = slots_w[pl.ds(term_at(NXT, s, 0), 8)].astype(F32)
        opp[0, s] = (opp[0, s].astype(F32) + mine).astype(BF16)
        cast(("a2", s), opp.at[0, s], low.at[0, s], up)
        got("b0", s)
        mine = slots_w[pl.ds(term_at(PRV, s, 1), 8)].astype(F32)
        opp[1, s] = (opp[1, s].astype(F32) + mine).astype(BF16)
        cast(("b2", s), opp.at[1, s], high.at[1, s], down)
        if s == 0:
            cast(("a1", 1), terms(NXT, 1, 1), low.at[1, 1], up)
            cast(("b1", 1), terms(PRV, 1, 0), high.at[0, 1], down)
            term(OWN, 0)
            term(OWN, 1)
            turned = slice(2 * LEN, 3 * LEN)
            wqkv[turned, 0:512] = sides[1].T
            for copy in curv_loads:
                copy.wait()

    def part_rows(s, part):
        return pl.ds(s * half + part * BLK, BLK)

    def weigh(part, s):
        rows = s * half + part * BLK
        for j in range(8):
            total = (
                slots_w[term_at(OWN, s, part) + j].astype(F32)
                + low[part, s, j].astype(F32)
                + high[part, s, j].astype(F32)
            )
            at_row = (j // 4) * LEN + rows
            c = wqkv[at_row : at_row + BLK, (j % 4) * BLK : (j % 4 + 1) * BLK].astype(F32)
            wt[OWN, rows : rows + BLK, j * BLK : (j + 1) * BLK] = (total * c).astype(BF16)

    def hand_on(name, src, dst, part, s, target):
        r = part_rows(s, part)
        cast((name, s), wt.at[src, r], wt.at[dst, r], target)

    def mixed_cotangent(rel, s):
        rows = halves[s]
        v = nt(wt[rel, rows, :], wout[0, chunk[rel]])
        if rel == OWN:
            proj[rows, 0:OUT] = v
        else:
            proj[rows, 0:OUT] += v

    per = NB // 2
    n_in = NQKV // 2
    sb = 192

    def out_gradient(rel):
        for n in range(2):
            g = nn(wqkv[turned, 0:512], wt[rel, :, n * 512 : (n + 1) * 512]).astype(BF16)
            for i in range(4):
                for j in range(4):
                    slots_w[(j % 2) * per + n_in + 16 * i + 4 * chunk[rel] + 2 * n + j // 2] = g[
                        i * BLK : (i + 1) * BLK, j * BLK : (j + 1) * BLK
                    ]
        if rel == OWN:
            pl.semaphore_wait(ready, 1)
        for i in range(4):
            b = n_in + 16 * i + 4 * chunk[rel]
            cast(
                ("swap", rel, i),
                slots_w.at[pl.ds((1 - core) * per + b, 4)],
                slots_p.at[pl.ds(sb + b, 4)],
                sib,
            )

    for s in (0, 1):
        got("a1", s)
        got("b2", s)
        weigh(1, s)
        hand_on("c1", OWN, PRV, 1, s, up)
        hand_on("d1", OWN, NXT, 1, s, down)
        got("b1", s)
        got("a2", s)
        weigh(0, s)
        hand_on("d0", OWN, NXT, 0, s, down)
        hand_on("c0", OWN, PRV, 0, s, up)
        mixed_cotangent(OWN, s)
    for s in (0, 1):
        got("c1", s)
        hand_on("e1", PRV, FAR, 1, s, up)
        got("d0", s)
        hand_on("e0", NXT, FAR, 0, s, down)
        if s == 0:
            out_gradient(OWN)
        got("d1", s)
        mixed_cotangent(NXT, s)
        got("c0", s)
        mixed_cotangent(PRV, s)
    got("e1", 0)
    got("e0", 0)
    mixed_cotangent(FAR, 0)

    def unrot(v, rows):
        return v * cos[rows, :] - pltpu.roll(v, 64, 1) * sin[rows, :]

    tail = slice(OUT, QKV)
    proj[:, tail] = jnp.zeros((LEN, QKV - OUT), F32)

    def attention_back(s):
        rows, seen = halves[s], slice(0, half * (s + 1))

        def one(h, carry):
            dm = proj[rows, cols_of(h)].astype(BF16)
            q = qkv[rows, cols_of(h)]
            pb = probs[h, rows, seen]
            dp = nt(dm, qkv[seen, cols_of(QH + 1)]).astype(BF16).astype(F32)
            pf = pb.astype(F32)
            pd = pf * dp
            ds = ((pd - pf * jnp.sum(pd, axis=-1, keepdims=True)) * scale).astype(BF16)
            dk = nn(q.T, ds)
            dv = nn(dm.T, pb)
            for u in range(s + 1):
                proj[u * BLK : (u + 1) * BLK, tail] += dk[:, u * half : (u + 1) * half]
                proj[half + u * BLK : half + (u + 1) * BLK, tail] += dv[
                    :, u * half : (u + 1) * half
                ]
            dq = unrot(nn(ds, qkv[seen, cols_of(QH)]).astype(BF16).astype(F32), rows).astype(BF16)
            sides[0, cols_of(h), rows] = dq.T
            return carry

        lax.fori_loop(0, QH, one, 0)

    attention_back(0)
    out_gradient(NXT)
    out_gradient(PRV)
    got("e1", 1)
    got("e0", 1)
    out_gradient(FAR)
    mixed_cotangent(FAR, 1)
    attention_back(1)
    for u in range(2):
        dk = proj[u * BLK : (u + 1) * BLK, tail].astype(BF16).astype(F32).T
        sides[1, 0:BLK, halves[u]] = unrot(dk, halves[u]).astype(BF16).T
        sides[1, BLK : 2 * BLK, halves[u]] = proj[
            half + u * BLK : half + (u + 1) * BLK, tail
        ].astype(BF16)
    for s in (0, 1):
        for name in ("a0", "b0", "a1", "b1"):
            done = arrivals[name, s]
            done.wait_send()
            sends[:] = [copy for copy in sends if copy is not done]
    for n in range(8):
        cols = slice(n * 512, (n + 1) * 512)
        for c0, lhs in ((0, sides[0]), (4, sides[1, 0 : 2 * BLK, :])):
            g = nn(lhs, normed[:, cols]).astype(BF16)
            for r in range(4):
                for c in range(lhs.shape[0] // BLK):
                    slots_w[((c0 + c) % 2) * per + 3 * (4 * n + r) + (c0 + c) // 2] = g[
                        c * BLK : (c + 1) * BLK, r * BLK : (r + 1) * BLK
                    ]
        cast(
            ("swap", n),
            slots_w.at[pl.ds((1 - core) * per + 12 * n, 12)],
            slots_p.at[pl.ds(sb + 12 * n, 12)],
            sib,
        )
    for rel in (OWN, NXT, PRV, FAR):
        for i in range(4):
            got("swap", rel, i)
    for n in range(8):
        got("swap", n)
    for copy in sends:
        copy.wait_send()
    sends.clear()

    chain = (("z", "y"), ("y", "z"))
    here = {"y": y, "z": z}
    steps = (2, 1, -1, 0)

    def acc_at(part, rel, h):
        return ((part * 4 + rel) * 2 + h) * 12

    def red_at(part, h, srel):
        return 2 * per + (part * 2 + h) * 12 + 3 * srel

    def fill(part, rel):
        f = wrap(here[chain[part][0]] + steps[rel])
        for srel in range(4):
            s = wrap(here[chain[part][1]] + steps[srel])
            d = index_of(f, s, part) if part == 0 else index_of(s, f, part)
            base = (starts[d] + 1 - core) // 2
            for i in range(HALF):
                j = jnp.minimum(base + i, per - 1)
                slots_p[acc_at(part, rel, i // 3) + 3 * srel + i % 3] = (
                    slots_w[core * per + j].astype(F32) + slots_p[sb + j].astype(F32)
                ).astype(BF16)

    subs = ((0, 3), (3, 6), (9, 3))

    def acc(part, rel, h, u):
        return pl.ds(acc_at(part, rel, h) + subs[u][0], subs[u][1])

    def ring(part, name, u, src, dst, leg, step):
        send((part, name, u), src, dst, at(chain[part][leg], step))

    def send_far(part, u):
        sub = pl.ds(*subs[u])
        ring(part, "fu", u, slots_p.at[acc(part, FAR, 0, u)], r_far.at[part, 0, sub], 0, 1)
        ring(part, "fd", u, slots_p.at[acc(part, FAR, 1, u)], r_far.at[part, 1, sub], 0, -1)

    def send_near(part, u):
        sub = pl.ds(*subs[u])
        ring(part, "lo1", u, slots_p.at[acc(part, NXT, 1, u)], r_low.at[part, 1, sub], 0, 1)
        ring(part, "hi0", u, slots_p.at[acc(part, PRV, 0, u)], r_high.at[part, 0, sub], 0, -1)

    def middle(part, u):
        sub = pl.ds(*subs[u])
        got(part, "fu", u)
        r_far[part, 0, sub] = (
            r_far[part, 0, sub].astype(F32) + slots_p[acc(part, NXT, 0, u)].astype(F32)
        ).astype(BF16)
        ring(part, "lo0", u, r_far.at[part, 0, sub], r_low.at[part, 0, sub], 0, 1)
        got(part, "fd", u)
        r_far[part, 1, sub] = (
            r_far[part, 1, sub].astype(F32) + slots_p[acc(part, PRV, 1, u)].astype(F32)
        ).astype(BF16)
        ring(part, "hi1", u, r_far.at[part, 1, sub], r_high.at[part, 1, sub], 0, -1)

    def reduce(part, u):
        sub = pl.ds(*subs[u])
        for name in ("lo1", "hi0", "lo0", "hi1"):
            got(part, name, u)
        for h in (0, 1):
            slots_w[pl.ds(red_at(part, h, 0) + subs[u][0], subs[u][1])] = (
                slots_p[acc(part, OWN, h, u)].astype(F32)
                + r_low[part, h, sub].astype(F32)
                + r_high[part, h, sub].astype(F32)
            ).astype(BF16)

    def red(part, h, srel):
        return pl.ds(red_at(part, h, srel), 3)

    both = (0, 1)
    for part in both:
        fill(part, FAR)
        send_far(part, 0)
    for part in both:
        fill(part, NXT)
        fill(part, PRV)
        send_near(part, 0)
    for part in both:
        send_far(part, 1)
        send_near(part, 1)
    for part in both:
        fill(part, OWN)
    for part in both:
        middle(part, 0)
    for part in both:
        send_far(part, 2)
        send_near(part, 2)
    for part in both:
        middle(part, 1)
    for part in both:
        reduce(part, 0)
        ring(part, "tu", 0, slots_w.at[red(part, 0, FAR)], t_far.at[part, 0], 1, 1)
        ring(part, "td", 0, slots_w.at[red(part, 1, FAR)], t_far.at[part, 1], 1, -1)
    for part in both:
        middle(part, 2)
    for part in both:
        reduce(part, 1)
        ring(part, "tl1", 0, slots_w.at[red(part, 1, NXT)], t_low.at[part, 1], 1, 1)
        ring(part, "th0", 0, slots_w.at[red(part, 0, PRV)], t_high.at[part, 0], 1, -1)
    for part in both:
        got(part, "tu", 0)
        t_far[part, 0] = (
            t_far[part, 0].astype(F32) + slots_w[red(part, 0, NXT)].astype(F32)
        ).astype(BF16)
        ring(part, "tl0", 0, t_far.at[part, 0], t_low.at[part, 0], 1, 1)
        got(part, "td", 0)
        t_far[part, 1] = (
            t_far[part, 1].astype(F32) + slots_w[red(part, 1, PRV)].astype(F32)
        ).astype(BF16)
        ring(part, "th1", 0, t_far.at[part, 1], t_high.at[part, 1], 1, -1)
    for part in both:
        reduce(part, 2)
    for part in both:
        for name in ("tl1", "th0", "tl0", "th1"):
            got(part, name, 0)

    def whole(part, h):
        return (
            slots_w[pl.ds(2 * per + (part * 2 + h) * 12 + 3 * OWN, 3)].astype(F32)
            + t_low[part, h].astype(F32)
            + t_high[part, h].astype(F32)
        )

    for h in (0, 1):
        out[pl.ds(3 * h, 3)] = whole(1 - core, h)
    last = cast(("last",), out.at[pl.ds(0, HALF)], tot.at[core], sib)
    for h in (0, 1):
        tot[core, pl.ds(3 * h, 3)] = whole(core, h)
    last.wait_recv()
    for copy in sends:
        copy.wait_send()

    start, n = starts[me], counts[me]
    for t in range(SLOTS):
        b = start + t
        parity = lax.rem(b, 2)
        v = tot[parity, b // 2 - (start + 1 - parity) // 2]
        v = jnp.where(b < NQKV, v.T, v)
        out[t] = jnp.where(t < n, v, 0.0)


def product(counts, w, p, gain, tokens, cos, sin, curv):
    vmem = pl.BlockSpec(memory_space=pltpu.VMEM)
    hbm = pl.BlockSpec(memory_space=pl.ANY)
    smem = pl.BlockSpec(memory_space=pltpu.SMEM)
    v = pltpu.VMEM
    block = (BLK, BLK)
    return pl.pallas_call(
        kernel,
        out_shape=jax.ShapeDtypeStruct((SLOTS,) + block, F32),
        in_specs=[smem, hbm, hbm, vmem, hbm, hbm, hbm, hbm],
        out_specs=vmem,
        scratch_shapes=[
            pltpu.SMEM((NB,), jnp.int32),
            pltpu.SMEM((32,), jnp.int32),
            v((32 * SLOTS,) + block, BF16),
            v((32 * SLOTS,) + block, BF16),
            v((LEN, D), BF16),
            v((LEN, HD), F32),
            v((LEN, HD), F32),
            v((D, QKV), BF16),
            v((2, 4, OUT, CHUNK), BF16),
            v((LEN, QKV), F32),
            v((2, LEN, OUT), BF16),
            v((QH, LEN, LEN), BF16),
            v((LEN, QKV), BF16),
            v((2, 2, 8) + block, BF16),
            v((2, 2, 8) + block, BF16),
            v((2, 2, 8) + block, BF16),
            v((4, LEN, CHUNK), BF16),
            v((2, 2, 12) + block, BF16),
            v((2, 2, 12) + block, BF16),
            v((2, 2, 12) + block, BF16),
            v((2, 2, 3) + block, BF16),
            v((2, 2, 3) + block, BF16),
            v((2, 2, 3) + block, BF16),
            v((2, HALF) + block, F32),
            pltpu.SemaphoreType.DMA((241,)),
            pltpu.SemaphoreType.DMA((241,)),
            pltpu.SemaphoreType.DMA((7,)),
            pltpu.SemaphoreType.REGULAR,
        ],
        compiler_params=pltpu.CompilerParams(
            collective_id=0, has_side_effects=True, vmem_limit_bytes=67_000_000
        ),
        name="product",
    )(counts, w, p, gain, tokens, cos, sin, curv)


def local(tokens, norm_gain, curvature, weight_slots, probe_slots, block_counts):
    counts = block_counts[0]
    cos, sin = tables()
    out = product(
        counts,
        weight_slots[0],
        probe_slots[0],
        norm_gain.reshape(1, D),
        tokens[0],
        cos,
        sin,
        curvature[0],
    )
    return (out * (1.0 / np.sqrt(np.float32(LEN * 32))))[None]


def solution(mesh):
    in_specs = (
        P("fsdp", None, None),
        P(),
        P("fsdp", None, None),
        P("seq", "fsdp", None, None),
        P("seq", "fsdp", None, None),
        P("seq", None),
    )
    out_specs = P("seq", "fsdp", None, None)
    return jax.shard_map(local, mesh=mesh, in_specs=in_specs, out_specs=out_specs, check_vma=False)
```

```python
import functools

import jax
import jax.numpy as jnp
import numpy as np
from jax import lax
from jax.experimental import pallas as pl
from jax.experimental.pallas import tpu as pltpu
from jax.sharding import PartitionSpec as P

D = 4096
HD = 128
BLK = 128
LEN = 512
QH = 4
QKV = 768
OUT = 512
NQKV = 192
NB = 320
SLOTS = 12
HALF = 6
CHUNK = 1024
FAR, NXT, PRV, OWN = 0, 1, 2, 3
THETA = 500000.0
EPS = 1e-05
NEGATIVE = -1e30
VMEM_LIMIT = 66_000_000
MESH = pl.DeviceIdType.MESH
F32 = jnp.float32
BF16 = jnp.bfloat16


def tables():
    half = HD // 2
    frequency = np.exp(-np.log(THETA) * 2.0 * np.arange(half) / HD)
    angles = np.arange(LEN)[:, None] * frequency[None, :]
    c, s = np.cos(angles), np.sin(angles)
    return (
        np.concatenate([c, c], axis=1).astype(np.float32),
        np.concatenate([-s, s], axis=1).astype(np.float32),
    )


def place():
    me = lax.axis_index("fsdp")
    core = lax.rem(me, 2)
    y = lax.rem(me // 2, 4)
    z = me // 8
    return me, core, y, z


def index_of(z, y, core):
    return (z * 4 + y) * 2 + core


def wrap(a):
    return lax.rem(a + 4, 4)


def greet(targets):
    barrier = pltpu.get_barrier_semaphore()
    for t in targets:
        pl.semaphore_signal(barrier, inc=1, device_id=t, device_id_type=MESH)
    pl.semaphore_wait(barrier, len(targets))


def nt(a, b):
    return lax.dot_general(a, b, (((1,), (1,)), ((), ())), preferred_element_type=F32)


def nn(a, b):
    return jnp.dot(a, b, preferred_element_type=F32)


def causal_mask():
    row = lax.broadcasted_iota(jnp.int32, (LEN, LEN), 0)
    col = lax.broadcasted_iota(jnp.int32, (LEN, LEN), 1)
    return row >= col


def kernel(
    counts, w_in, p_in, gain, tokens_in, cos_in, sin_in, curv_in,
    out,
    table, starts, slots_w, slots_p, normed, cos, sin, wqkv, wout, proj, sides, probs, qkv,
    opp, low, high, wt, r_far, r_low, r_high, t_far, t_low, t_high, tot,
    send_sem, recv_sem, local_sem, ready,
):
    me, core, y, z = place()
    x = lax.axis_index("seq")
    sib = {"fsdp": index_of(z, y, 1 - core)}
    up, down = {"seq": wrap(x + 1)}, {"seq": wrap(x - 1)}

    def at(axis, step):
        if axis == "y":
            return {"fsdp": index_of(z, wrap(y + step), core)}
        return {"fsdp": index_of(wrap(z + step), y, core)}

    my_slots = pl.ds(me * SLOTS, SLOTS)
    local = [
        pltpu.make_async_copy(a, b, local_sem.at[i])
        for i, (a, b) in enumerate(
            (
                (w_in, slots_w.at[my_slots]),
                (p_in, slots_p.at[my_slots]),
                (tokens_in, normed),
                (cos_in, cos),
                (sin_in, sin),
            )
        )
    ]
    for copy in local:
        copy.start()
    greet([up, down, at("y", 1), at("y", -1), at("z", 1), at("z", -1), sib])

    first = ("y", "z", "y", "z")
    second = ("z", "y", "z", "y")
    landed = (slots_w, slots_w, slots_p, slots_p)
    counter = [0]
    sends = []
    arrivals = {}

    def send(key, src, dst, target):
        number = counter[0]
        counter[0] += 1
        copy = pltpu.make_async_remote_copy(
            src_ref=src,
            dst_ref=dst,
            send_sem=send_sem.at[number],
            recv_sem=recv_sem.at[number],
            device_id=target,
            device_id_type=MESH,
        )
        copy.start()
        sends.append(copy)
        arrivals[key] = copy
        return copy

    def span(p, side):
        start = (p % 2) * HALF
        return (start, HALF) if side is None else (start + 3 * side, 3)

    def piece(p, origin, side=None):
        start, size = span(p, side)
        return landed[p].at[pl.ds(origin * SLOTS + start, size)]

    def origin_of(p, f, s):
        if p % 2 == 0:
            return index_of(wrap(z + s), wrap(y + f), core)
        return index_of(wrap(z + f), wrap(y + s), core)

    def go(p, role, f, s, axis, step, side=None):
        ref = piece(p, origin_of(p, f, s), side)
        send((p,) + role, ref, ref, at(axis[p], step))

    def to_sib(p, f, s):
        ref = piece(p, origin_of(p, f, s))
        send((p, "sib", f, s), ref, ref, sib)

    def got(*key):
        arrivals[key].wait_recv()

    def begin(parts):
        for p in parts:
            go(p, ("f+",), 0, 0, first, 1)
            go(p, ("f-",), 0, 0, first, -1)
        for p in parts:
            go(p, ("s+", 0), 0, 0, second, 1)
            go(p, ("s-", 0), 0, 0, second, -1)
        for p in parts:
            to_sib(p, 0, 0)

    def neighbours(p):
        got(p, "f+")
        go(p, ("fa",), -1, 0, first, 1, 0)
        go(p, ("s+", -1), -1, 0, second, 1)
        go(p, ("s-", -1), -1, 0, second, -1)
        got(p, "f-")
        go(p, ("fb",), 1, 0, first, -1, 1)
        go(p, ("s+", 1), 1, 0, second, 1)
        go(p, ("s-", 1), 1, 0, second, -1)
        to_sib(p, -1, 0)
        to_sib(p, 1, 0)

    def pass_on(p, f):
        got(p, "s+", f)
        go(p, ("sa", f), f, -1, second, 1, 0)
        to_sib(p, f, -1)
        got(p, "s-", f)
        go(p, ("sb", f), f, 1, second, -1, 1)
        to_sib(p, f, 1)

    def opposite(p):
        got(p, "fa")
        got(p, "fb")
        go(p, ("s+", 2), 2, 0, second, 1)
        go(p, ("s-", 2), 2, 0, second, -1)
        to_sib(p, 2, 0)

    def corner(p, f):
        got(p, "sa", f)
        got(p, "sb", f)
        to_sib(p, f, 2)

    def sibling_done(parts):
        for p in parts:
            for f in (0, -1, 1, 2):
                for s in (0, -1, 1, 2):
                    got(p, "sib", f, s)

    w, pr = (0, 1), (2, 3)
    local[0].wait()
    local[1].wait()
    begin(w)

    def locate(b, carry):
        d, t = carry
        table[b] = d * SLOTS + t
        more = t + 1 < counts[d]
        return jnp.where(more, d, jnp.minimum(d + 1, 31)), jnp.where(more, t + 1, 0)

    lax.fori_loop(0, NB, locate, (0, 0))

    def prefix(d, s):
        starts[d] = s
        return s + counts[d]

    lax.fori_loop(0, 32, prefix, 0)
    local[2].wait()

    def norm(i, carry):
        rows = pl.ds(pl.multiple_of(i * 32, 32), 32)
        x = normed[rows, :].astype(F32)
        factor = lax.rsqrt(jnp.mean(x * x, axis=-1, keepdims=True) + EPS)
        normed[rows, :] = (x * factor * gain[...]).astype(BF16)
        return carry

    lax.fori_loop(0, LEN // 32, norm, 0)
    local[3].wait()
    local[4].wait()

    def cols_of(h):
        return pl.ds(h * HD if isinstance(h, int) else pl.multiple_of(h * HD, HD), HD)

    def assemble_qkv(src):
        def step(r, carry):
            rows = pl.ds(pl.multiple_of(r * BLK, BLK), BLK)
            for c in range(6):
                wqkv[rows, c * BLK : (c + 1) * BLK] = src[table[r * 6 + c]]
            return carry

        lax.fori_loop(0, 32, step, 0, unroll=2)

    def assemble_out_chunk(src, tensor, q):
        for i in range(4):
            for j in range(8):
                wout[tensor, q, i * BLK : (i + 1) * BLK, j * BLK : (j + 1) * BLK] = src[
                    table[NQKV + i * 32 + q * 8 + j]
                ]

    def assemble_out(src, tensor):
        def step(i, carry):
            rows = pl.ds(pl.multiple_of(i * BLK, BLK), BLK)
            for j in range(32):
                wout[tensor, j // 8, rows, (j % 8) * BLK : (j % 8 + 1) * BLK] = src[
                    table[NQKV + i * 32 + j]
                ]
            return carry

        lax.fori_loop(0, 4, step, 0)

    all_rows = slice(0, LEN)
    half = LEN // 2
    halves = (slice(0, half), slice(half, LEN))

    def project(n, rows=all_rows):
        cols = slice(n * 256, (n + 1) * 256)
        proj[rows, cols] = nn(normed[rows, :], wqkv[:, cols])

    def head(h, turn=True, rows=all_rows):
        v = proj[rows, cols_of(h)]
        if turn:
            v = v * cos[rows, :] + pltpu.roll(v, 64, 1) * sin[rows, :]
        return v.astype(BF16)

    def heads():
        for h in range(QH + 2):
            qkv[:, cols_of(h)] = head(h, h < QH + 1)

    scale = HD**-0.5

    def primal(h, carry):
        k = qkv[:, cols_of(QH)]
        v = qkv[:, cols_of(QH + 1)]
        s = jnp.where(causal_mask(), nt(qkv[:, cols_of(h)], k) * scale, NEGATIVE)
        m = jnp.max(s, axis=-1, keepdims=True)
        e = jnp.exp(s - m)
        p = (e * (1.0 / jnp.sum(e, axis=-1, keepdims=True))).astype(BF16)
        probs[h] = p
        sides[1, :, cols_of(h)] = nn(p, v).astype(BF16)
        return carry

    for p in w:
        neighbours(p)
    for p in w:
        pass_on(p, 0)
    for p in w:
        opposite(p)
    begin(pr)
    for f in (-1, 1):
        for p in w:
            pass_on(p, f)
    for p in w:
        corner(p, 0)
    for p in w:
        pass_on(p, 2)
    for p in pr:
        neighbours(p)
    for p in pr:
        pass_on(p, 0)
    for f in (-1, 1, 2):
        for p in w:
            corner(p, f)
    for p in pr:
        opposite(p)
    sibling_done(w)
    assemble_qkv(slots_w)
    project(0)
    for p in pr:
        pass_on(p, -1)
    for p in pr:
        corner(p, 0)
    project(1)
    project(2)
    for p in pr:
        pass_on(p, 1)
    heads()
    lax.fori_loop(0, 2, primal, 0)
    for p in pr:
        pass_on(p, 2)
    lax.fori_loop(2, 4, primal, 0)
    assemble_out(slots_w, 0)
    for f in (-1, 1, 2):
        for p in pr:
            corner(p, f)
    sibling_done(pr)

    chunk = (wrap(x + 2), wrap(x + 1), wrap(x - 1), x)
    key_tangent, value_tangent = cols_of(0), cols_of(1)

    def tangent(s):
        rows, seen = halves[s], slice(0, half * (s + 1))
        for n in range(3):
            project(n, rows)
        wt[OWN, rows, key_tangent] = head(QH, True, rows)
        wt[OWN, rows, value_tangent] = head(QH + 1, False, rows)
        keys = jnp.concatenate([qkv[seen, cols_of(QH)], wt[OWN, seen, key_tangent]], axis=1)

        def one(h, carry):
            pb = probs[h, rows, seen]
            pf = pb.astype(F32)
            side = jnp.concatenate([head(h, True, rows), qkv[rows, cols_of(h)]], axis=1)
            pt = pf * (nt(side, keys) * scale)
            tp = (pt - pf * jnp.sum(pt, axis=-1, keepdims=True)).astype(BF16)
            sides[0, rows, cols_of(h)] = (
                nn(tp, qkv[seen, cols_of(QH + 1)]) + nn(pb, wt[OWN, seen, value_tangent])
            ).astype(BF16)
            return carry

        lax.fori_loop(0, QH, one, 0)

    def term_at(rel, s, part):
        return (0, 32, 64, 160)[rel] + (s * 2 + part) * 8

    def term(rel, s):
        rows = halves[s]
        for n in range(2):
            cols = slice(n * 512, (n + 1) * 512)
            v = (
                nn(sides[0, rows, :], wout[0, chunk[rel], :, cols])
                + nn(sides[1, rows, :], wout[1, chunk[rel], :, cols])
            ).astype(BF16)
            for part in (0, 1):
                for j in range(4):
                    slots_w[term_at(rel, s, part) + 4 * n + j] = v[
                        part * BLK : (part + 1) * BLK, j * BLK : (j + 1) * BLK
                    ]

    def terms(rel, s, part):
        return slots_w.at[pl.ds(term_at(rel, s, part), 8)]

    def cast(name, src, dst, target):
        return send(name, src, dst, target)

    assemble_qkv(slots_p)
    tangent(0)
    for copy in sends:
        copy.wait_send()
    sends.clear()
    for s in (0, 1):
        if s == 1:
            tangent(1)
        for rel in (FAR, NXT, PRV):
            if s == 0:
                assemble_out_chunk(slots_p, 1, chunk[rel])
            term(rel, s)
            if rel == FAR:
                cast(("a0", s), terms(FAR, s, 0), opp.at[0, s], up)
                cast(("b0", s), terms(FAR, s, 1), opp.at[1, s], down)
            if rel == NXT and s == 0:
                cast(("a1", s), terms(NXT, s, 1), low.at[1, s], up)
            if rel == PRV and s == 0:
                cast(("b1", s), terms(PRV, s, 0), high.at[0, s], down)
        if s == 0:
            assemble_out_chunk(slots_p, 1, chunk[OWN])
            pl.semaphore_signal(ready, inc=1, device_id=sib, device_id_type=MESH)
    curv_loads = []
    for n in range(2):
        curv_loads.append(
            pltpu.make_async_copy(
                curv_in.at[:, pl.ds(pl.multiple_of(x * CHUNK + n * 512, 512), 512)],
                wqkv.at[n * LEN : (n + 1) * LEN, 0:512],
                local_sem.at[5 + n],
            )
        )
        curv_loads[-1].start()
    for s in (0, 1):
        got("a0", s)
        mine = slots_w[pl.ds(term_at(NXT, s, 0), 8)].astype(F32)
        opp[0, s] = (opp[0, s].astype(F32) + mine).astype(BF16)
        cast(("a2", s), opp.at[0, s], low.at[0, s], up)
        got("b0", s)
        mine = slots_w[pl.ds(term_at(PRV, s, 1), 8)].astype(F32)
        opp[1, s] = (opp[1, s].astype(F32) + mine).astype(BF16)
        cast(("b2", s), opp.at[1, s], high.at[1, s], down)
        if s == 0:
            cast(("a1", 1), terms(NXT, 1, 1), low.at[1, 1], up)
            cast(("b1", 1), terms(PRV, 1, 0), high.at[0, 1], down)
            term(OWN, 0)
            term(OWN, 1)
            turned = slice(2 * LEN, 3 * LEN)
            wqkv[turned, 0:512] = sides[1].T
            for copy in curv_loads:
                copy.wait()

    def part_rows(s, part):
        return pl.ds(s * half + part * BLK, BLK)

    def weigh(part, s):
        rows = s * half + part * BLK
        for j in range(8):
            total = (
                slots_w[term_at(OWN, s, part) + j].astype(F32)
                + low[part, s, j].astype(F32)
                + high[part, s, j].astype(F32)
            )
            at_row = (j // 4) * LEN + rows
            c = wqkv[at_row : at_row + BLK, (j % 4) * BLK : (j % 4 + 1) * BLK].astype(F32)
            wt[OWN, rows : rows + BLK, j * BLK : (j + 1) * BLK] = (total * c).astype(BF16)

    def hand_on(name, src, dst, part, s, target):
        r = part_rows(s, part)
        cast((name, s), wt.at[src, r], wt.at[dst, r], target)

    def mixed_cotangent(rel, s):
        rows = halves[s]
        v = nt(wt[rel, rows, :], wout[0, chunk[rel]])
        if rel == OWN:
            proj[rows, 0:OUT] = v
        else:
            proj[rows, 0:OUT] += v

    per = NB // 2
    n_in = NQKV // 2
    sb = 192

    def out_gradient(rel):
        for n in range(2):
            g = nn(wqkv[turned, 0:512], wt[rel, :, n * 512 : (n + 1) * 512]).astype(BF16)
            for i in range(4):
                for j in range(4):
                    slots_w[(j % 2) * per + n_in + 16 * i + 4 * chunk[rel] + 2 * n + j // 2] = g[
                        i * BLK : (i + 1) * BLK, j * BLK : (j + 1) * BLK
                    ]
        if rel == OWN:
            pl.semaphore_wait(ready, 1)
        for i in range(4):
            b = n_in + 16 * i + 4 * chunk[rel]
            cast(
                ("swap", rel, i),
                slots_w.at[pl.ds((1 - core) * per + b, 4)],
                slots_p.at[pl.ds(sb + b, 4)],
                sib,
            )

    for s in (0, 1):
        got("a1", s)
        got("b2", s)
        weigh(1, s)
        hand_on("c1", OWN, PRV, 1, s, up)
        hand_on("d1", OWN, NXT, 1, s, down)
        got("b1", s)
        got("a2", s)
        weigh(0, s)
        hand_on("d0", OWN, NXT, 0, s, down)
        hand_on("c0", OWN, PRV, 0, s, up)
        mixed_cotangent(OWN, s)
    for s in (0, 1):
        got("c1", s)
        hand_on("e1", PRV, FAR, 1, s, up)
        got("d0", s)
        hand_on("e0", NXT, FAR, 0, s, down)
        if s == 0:
            out_gradient(OWN)
        got("d1", s)
        mixed_cotangent(NXT, s)
        got("c0", s)
        mixed_cotangent(PRV, s)
    got("e1", 0)
    got("e0", 0)
    mixed_cotangent(FAR, 0)

    def unrot(v, rows):
        return v * cos[rows, :] - pltpu.roll(v, 64, 1) * sin[rows, :]

    tail = slice(OUT, QKV)
    proj[:, tail] = jnp.zeros((LEN, QKV - OUT), F32)

    def attention_back(s, begin, end, unroll):
        rows, seen = halves[s], slice(0, half * (s + 1))

        def one(h, carry):
            dm = proj[rows, cols_of(h)].astype(BF16)
            q = qkv[rows, cols_of(h)]
            pb = probs[h, rows, seen]
            dp = nt(dm, qkv[seen, cols_of(QH + 1)]).astype(BF16).astype(F32)
            pf = pb.astype(F32)
            pd = pf * dp
            ds = ((pd - pf * jnp.sum(pd, axis=-1, keepdims=True)) * scale).astype(BF16)
            dk = nn(q.T, ds)
            dv = nn(dm.T, pb)
            for u in range(s + 1):
                proj[u * BLK : (u + 1) * BLK, tail] += dk[:, u * half : (u + 1) * half]
                proj[half + u * BLK : half + (u + 1) * BLK, tail] += dv[
                    :, u * half : (u + 1) * half
                ]
            dq = unrot(nn(ds, qkv[seen, cols_of(QH)]).astype(BF16).astype(F32), rows).astype(BF16)
            sides[0, cols_of(h), rows] = dq.T
            return carry

        lax.fori_loop(begin, end, one, 0, unroll=unroll)

    attention_back(0, 0, QH, 1)
    out_gradient(NXT)
    out_gradient(PRV)
    got("e1", 1)
    got("e0", 1)
    out_gradient(FAR)
    mixed_cotangent(FAR, 1)
    for s in (0, 1):
        for name in ("a0", "b0", "a1", "b1"):
            done = arrivals[name, s]
            done.wait_send()
            sends[:] = [copy for copy in sends if copy is not done]

    def in_gradient(pair, lhs):
        for n in range(8):
            g = nn(lhs, normed[:, n * 512 : (n + 1) * 512]).astype(BF16)
            for r in range(4):
                for c in range(2):
                    slots_w[c * per + 32 * pair + 4 * n + r] = g[
                        c * BLK : (c + 1) * BLK, r * BLK : (r + 1) * BLK
                    ]
            if n % 2 == 1:
                b = 32 * pair + 8 * (n // 2)
                cast(
                    ("swap", pair, n // 2, 0),
                    slots_w.at[pl.ds((1 - core) * per + b, 8)],
                    slots_p.at[pl.ds(sb + b, 8)],
                    sib,
                )

    for pair in (0, 1):
        attention_back(1, 2 * pair, 2 * pair + 2, 2)
        in_gradient(pair, sides[0, 2 * pair * BLK : 2 * (pair + 1) * BLK, :])
    for u in range(2):
        dk = proj[u * BLK : (u + 1) * BLK, tail].astype(BF16).astype(F32).T
        sides[1, 0:BLK, halves[u]] = unrot(dk, halves[u]).astype(BF16).T
        sides[1, BLK : 2 * BLK, halves[u]] = proj[
            half + u * BLK : half + (u + 1) * BLK, tail
        ].astype(BF16)
    in_gradient(2, sides[1, 0 : 2 * BLK, :])
    for rel in (OWN, NXT, PRV, FAR):
        for i in range(4):
            got("swap", rel, i)
    for pair in range(3):
        for n in range(4):
            got("swap", pair, n, 0)
    for copy in sends:
        copy.wait_send()
    sends.clear()

    chain = (("z", "y"), ("y", "z"))
    here = {"y": y, "z": z}
    steps = (2, 1, -1, 0)

    def acc_at(part, rel, h):
        return ((part * 4 + rel) * 2 + h) * 12

    def red_at(part, h, srel):
        return 2 * per + (part * 2 + h) * 12 + 3 * srel

    def fill(part, rel):
        f = wrap(here[chain[part][0]] + steps[rel])
        for srel in range(4):
            s = wrap(here[chain[part][1]] + steps[srel])
            d = index_of(f, s, part) if part == 0 else index_of(s, f, part)
            base = (starts[d] + 1 - core) // 2
            for i in range(HALF):
                j = jnp.minimum(base + i, per - 1)
                j = jnp.where(j < n_in, 32 * lax.rem(j, 3) + lax.div(j, 3), j)
                slots_p[acc_at(part, rel, i // 3) + 3 * srel + i % 3] = (
                    slots_w[core * per + j].astype(F32) + slots_p[sb + j].astype(F32)
                ).astype(BF16)

    subs = ((0, 3), (3, 6), (9, 3))

    def acc(part, rel, h, u):
        return pl.ds(acc_at(part, rel, h) + subs[u][0], subs[u][1])

    def ring(part, name, u, src, dst, leg, step):
        send((part, name, u), src, dst, at(chain[part][leg], step))

    def send_far(part, u):
        sub = pl.ds(*subs[u])
        ring(part, "fu", u, slots_p.at[acc(part, FAR, 0, u)], r_far.at[part, 0, sub], 0, 1)
        ring(part, "fd", u, slots_p.at[acc(part, FAR, 1, u)], r_far.at[part, 1, sub], 0, -1)

    def send_near(part, u):
        sub = pl.ds(*subs[u])
        ring(part, "lo1", u, slots_p.at[acc(part, NXT, 1, u)], r_low.at[part, 1, sub], 0, 1)
        ring(part, "hi0", u, slots_p.at[acc(part, PRV, 0, u)], r_high.at[part, 0, sub], 0, -1)

    def middle(part, u):
        sub = pl.ds(*subs[u])
        got(part, "fu", u)
        r_far[part, 0, sub] = (
            r_far[part, 0, sub].astype(F32) + slots_p[acc(part, NXT, 0, u)].astype(F32)
        ).astype(BF16)
        ring(part, "lo0", u, r_far.at[part, 0, sub], r_low.at[part, 0, sub], 0, 1)
        got(part, "fd", u)
        r_far[part, 1, sub] = (
            r_far[part, 1, sub].astype(F32) + slots_p[acc(part, PRV, 1, u)].astype(F32)
        ).astype(BF16)
        ring(part, "hi1", u, r_far.at[part, 1, sub], r_high.at[part, 1, sub], 0, -1)

    def reduce(part, u):
        sub = pl.ds(*subs[u])
        for name in ("lo1", "hi0", "lo0", "hi1"):
            got(part, name, u)
        for h in (0, 1):
            slots_w[pl.ds(red_at(part, h, 0) + subs[u][0], subs[u][1])] = (
                slots_p[acc(part, OWN, h, u)].astype(F32)
                + r_low[part, h, sub].astype(F32)
                + r_high[part, h, sub].astype(F32)
            ).astype(BF16)

    def red(part, h, srel):
        return pl.ds(red_at(part, h, srel), 3)

    both = (0, 1)
    for part in both:
        fill(part, FAR)
        send_far(part, 0)
    for part in both:
        fill(part, NXT)
        fill(part, PRV)
        send_near(part, 0)
    for part in both:
        send_far(part, 1)
        send_near(part, 1)
    for part in both:
        fill(part, OWN)
    for part in both:
        middle(part, 0)
    for part in both:
        send_far(part, 2)
        send_near(part, 2)
    for part in both:
        middle(part, 1)
    for part in both:
        reduce(part, 0)
        ring(part, "tu", 0, slots_w.at[red(part, 0, FAR)], t_far.at[part, 0], 1, 1)
        ring(part, "td", 0, slots_w.at[red(part, 1, FAR)], t_far.at[part, 1], 1, -1)
    for part in both:
        middle(part, 2)
    for part in both:
        reduce(part, 1)
        ring(part, "tl1", 0, slots_w.at[red(part, 1, NXT)], t_low.at[part, 1], 1, 1)
        ring(part, "th0", 0, slots_w.at[red(part, 0, PRV)], t_high.at[part, 0], 1, -1)
    for part in both:
        got(part, "tu", 0)
        t_far[part, 0] = (
            t_far[part, 0].astype(F32) + slots_w[red(part, 0, NXT)].astype(F32)
        ).astype(BF16)
        ring(part, "tl0", 0, t_far.at[part, 0], t_low.at[part, 0], 1, 1)
        got(part, "td", 0)
        t_far[part, 1] = (
            t_far[part, 1].astype(F32) + slots_w[red(part, 1, PRV)].astype(F32)
        ).astype(BF16)
        ring(part, "th1", 0, t_far.at[part, 1], t_high.at[part, 1], 1, -1)
    for part in both:
        reduce(part, 2)
    for part in both:
        for name in ("tl1", "th0", "tl0", "th1"):
            got(part, name, 0)

    def whole(part, h):
        return (
            slots_w[pl.ds(2 * per + (part * 2 + h) * 12 + 3 * OWN, 3)].astype(F32)
            + t_low[part, h].astype(F32)
            + t_high[part, h].astype(F32)
        )

    for h in (0, 1):
        out[pl.ds(3 * h, 3)] = whole(1 - core, h)
    last = cast(("last",), out.at[pl.ds(0, HALF)], tot.at[core], sib)
    for h in (0, 1):
        tot[core, pl.ds(3 * h, 3)] = whole(core, h)
    last.wait_recv()
    for copy in sends:
        copy.wait_send()

    start, n = starts[me], counts[me]
    for t in range(SLOTS):
        b = start + t
        parity = lax.rem(b, 2)
        v = tot[parity, b // 2 - (start + 1 - parity) // 2]
        v = jnp.where(b < NQKV, v.T, v)
        out[t] = jnp.where(t < n, v, 0.0)


def product(counts, w, p, gain, tokens, cos, sin, curv):
    vmem = pl.BlockSpec(memory_space=pltpu.VMEM)
    hbm = pl.BlockSpec(memory_space=pl.ANY)
    smem = pl.BlockSpec(memory_space=pltpu.SMEM)
    v = pltpu.VMEM
    block = (BLK, BLK)
    return pl.pallas_call(
        kernel,
        out_shape=jax.ShapeDtypeStruct((SLOTS,) + block, F32),
        in_specs=[smem, hbm, hbm, vmem, hbm, hbm, hbm, hbm],
        out_specs=vmem,
        scratch_shapes=[
            pltpu.SMEM((NB,), jnp.int32),
            pltpu.SMEM((32,), jnp.int32),
            v((32 * SLOTS,) + block, BF16),
            v((32 * SLOTS,) + block, BF16),
            v((LEN, D), BF16),
            v((LEN, HD), F32),
            v((LEN, HD), F32),
            v((D, QKV), BF16),
            v((2, 4, OUT, CHUNK), BF16),
            v((LEN, QKV), F32),
            v((2, LEN, OUT), BF16),
            v((QH, LEN, LEN), BF16),
            v((LEN, QKV), BF16),
            v((2, 2, 8) + block, BF16),
            v((2, 2, 8) + block, BF16),
            v((2, 2, 8) + block, BF16),
            v((4, LEN, CHUNK), BF16),
            v((2, 2, 12) + block, BF16),
            v((2, 2, 12) + block, BF16),
            v((2, 2, 12) + block, BF16),
            v((2, 2, 3) + block, BF16),
            v((2, 2, 3) + block, BF16),
            v((2, 2, 3) + block, BF16),
            v((2, HALF) + block, F32),
            pltpu.SemaphoreType.DMA((245,)),
            pltpu.SemaphoreType.DMA((245,)),
            pltpu.SemaphoreType.DMA((7,)),
            pltpu.SemaphoreType.REGULAR,
        ],
        compiler_params=pltpu.CompilerParams(
            collective_id=0, has_side_effects=True, vmem_limit_bytes=67_000_000
        ),
        name="product",
    )(counts, w, p, gain, tokens, cos, sin, curv)


def local(tokens, norm_gain, curvature, weight_slots, probe_slots, block_counts):
    counts = block_counts[0]
    cos, sin = tables()
    out = product(
        counts,
        weight_slots[0],
        probe_slots[0],
        norm_gain.reshape(1, D),
        tokens[0],
        cos,
        sin,
        curvature[0],
    )
    return (out * (1.0 / np.sqrt(np.float32(LEN * 32))))[None]


def solution(mesh):
    in_specs = (
        P("fsdp", None, None),
        P(),
        P("fsdp", None, None),
        P("seq", "fsdp", None, None),
        P("seq", "fsdp", None, None),
        P("seq", None),
    )
    out_specs = P("seq", "fsdp", None, None)
    return jax.shard_map(local, mesh=mesh, in_specs=in_specs, out_specs=out_specs, check_vma=False)
```

```python
import functools

import jax
import jax.numpy as jnp
import numpy as np
from jax import lax
from jax.experimental import pallas as pl
from jax.experimental.pallas import tpu as pltpu
from jax.sharding import PartitionSpec as P

D = 4096
HD = 128
BLK = 128
LEN = 512
QH = 4
QKV = 768
OUT = 512
NQKV = 192
NB = 320
SLOTS = 12
HALF = 6
CHUNK = 1024
FAR, NXT, PRV, OWN = 0, 1, 2, 3
THETA = 500000.0
EPS = 1e-05
NEGATIVE = -1e30
VMEM_LIMIT = 66_000_000
MESH = pl.DeviceIdType.MESH
F32 = jnp.float32
BF16 = jnp.bfloat16


def tables():
    half = HD // 2
    frequency = np.exp(-np.log(THETA) * 2.0 * np.arange(half) / HD)
    angles = np.arange(LEN)[:, None] * frequency[None, :]
    c, s = np.cos(angles), np.sin(angles)
    return (
        np.concatenate([c, c], axis=1).astype(np.float32),
        np.concatenate([-s, s], axis=1).astype(np.float32),
    )


def place():
    me = lax.axis_index("fsdp")
    core = lax.rem(me, 2)
    y = lax.rem(me // 2, 4)
    z = me // 8
    return me, core, y, z


def index_of(z, y, core):
    return (z * 4 + y) * 2 + core


def wrap(a):
    return lax.rem(a + 4, 4)


def greet(targets):
    barrier = pltpu.get_barrier_semaphore()
    for t in targets:
        pl.semaphore_signal(barrier, inc=1, device_id=t, device_id_type=MESH)
    pl.semaphore_wait(barrier, len(targets))


def nt(a, b):
    return lax.dot_general(a, b, (((1,), (1,)), ((), ())), preferred_element_type=F32)


def nn(a, b):
    return jnp.dot(a, b, preferred_element_type=F32)


def causal_mask():
    row = lax.broadcasted_iota(jnp.int32, (LEN, LEN), 0)
    col = lax.broadcasted_iota(jnp.int32, (LEN, LEN), 1)
    return row >= col


def kernel(
    counts, w_in, p_in, gain, tokens_in, cos_in, sin_in, curv_in,
    out,
    table, starts, slots_w, slots_p, normed, cos, sin, wqkv, wout, proj, sides, probs, qkv,
    opp, low, high, wt, r_far, r_low, r_high, t_far, t_low, t_high, tot,
    send_sem, recv_sem, local_sem, ready,
):
    me, core, y, z = place()
    x = lax.axis_index("seq")
    sib = {"fsdp": index_of(z, y, 1 - core)}
    up, down = {"seq": wrap(x + 1)}, {"seq": wrap(x - 1)}

    def at(axis, step):
        if axis == "y":
            return {"fsdp": index_of(z, wrap(y + step), core)}
        return {"fsdp": index_of(wrap(z + step), y, core)}

    my_slots = pl.ds(me * SLOTS, SLOTS)
    local = [
        pltpu.make_async_copy(a, b, local_sem.at[i])
        for i, (a, b) in enumerate(
            (
                (w_in, slots_w.at[my_slots]),
                (p_in, slots_p.at[my_slots]),
                (tokens_in, normed),
                (cos_in, cos),
                (sin_in, sin),
            )
        )
    ]
    for copy in local:
        copy.start()
    greet([up, down, at("y", 1), at("y", -1), at("z", 1), at("z", -1), sib])

    first = ("y", "z", "y", "z")
    second = ("z", "y", "z", "y")
    landed = (slots_w, slots_w, slots_p, slots_p)
    counter = [0]
    sends = []
    arrivals = {}

    def send(key, src, dst, target):
        number = counter[0]
        counter[0] += 1
        copy = pltpu.make_async_remote_copy(
            src_ref=src,
            dst_ref=dst,
            send_sem=send_sem.at[number],
            recv_sem=recv_sem.at[number],
            device_id=target,
            device_id_type=MESH,
        )
        copy.start()
        sends.append(copy)
        arrivals[key] = copy
        return copy

    def span(p, side):
        start = (p % 2) * HALF
        return (start, HALF) if side is None else (start + 3 * side, 3)

    def piece(p, origin, side=None):
        start, size = span(p, side)
        return landed[p].at[pl.ds(origin * SLOTS + start, size)]

    def origin_of(p, f, s):
        if p % 2 == 0:
            return index_of(wrap(z + s), wrap(y + f), core)
        return index_of(wrap(z + f), wrap(y + s), core)

    def go(p, role, f, s, axis, step, side=None):
        ref = piece(p, origin_of(p, f, s), side)
        send((p,) + role, ref, ref, at(axis[p], step))

    def to_sib(p, f, s):
        ref = piece(p, origin_of(p, f, s))
        send((p, "sib", f, s), ref, ref, sib)

    def got(*key):
        arrivals[key].wait_recv()

    def begin(parts):
        for p in parts:
            go(p, ("f+",), 0, 0, first, 1)
            go(p, ("f-",), 0, 0, first, -1)
        for p in parts:
            go(p, ("s+", 0), 0, 0, second, 1)
            go(p, ("s-", 0), 0, 0, second, -1)
        for p in parts:
            to_sib(p, 0, 0)

    def neighbours(p):
        got(p, "f+")
        go(p, ("fa",), -1, 0, first, 1, 0)
        go(p, ("s+", -1), -1, 0, second, 1)
        go(p, ("s-", -1), -1, 0, second, -1)
        got(p, "f-")
        go(p, ("fb",), 1, 0, first, -1, 1)
        go(p, ("s+", 1), 1, 0, second, 1)
        go(p, ("s-", 1), 1, 0, second, -1)
        to_sib(p, -1, 0)
        to_sib(p, 1, 0)

    def pass_on(p, f):
        got(p, "s+", f)
        go(p, ("sa", f), f, -1, second, 1, 0)
        to_sib(p, f, -1)
        got(p, "s-", f)
        go(p, ("sb", f), f, 1, second, -1, 1)
        to_sib(p, f, 1)

    def opposite(p):
        got(p, "fa")
        got(p, "fb")
        go(p, ("s+", 2), 2, 0, second, 1)
        go(p, ("s-", 2), 2, 0, second, -1)
        to_sib(p, 2, 0)

    def corner(p, f):
        got(p, "sa", f)
        got(p, "sb", f)
        to_sib(p, f, 2)

    def sibling_done(parts):
        for p in parts:
            for f in (0, -1, 1, 2):
                for s in (0, -1, 1, 2):
                    got(p, "sib", f, s)

    w, pr = (0, 1), (2, 3)
    local[0].wait()
    local[1].wait()
    begin(w)

    def locate(b, carry):
        d, t = carry
        table[b] = d * SLOTS + t
        more = t + 1 < counts[d]
        return jnp.where(more, d, jnp.minimum(d + 1, 31)), jnp.where(more, t + 1, 0)

    lax.fori_loop(0, NB, locate, (0, 0))

    def prefix(d, s):
        starts[d] = s
        return s + counts[d]

    lax.fori_loop(0, 32, prefix, 0)
    local[2].wait()

    def norm(i, carry):
        rows = pl.ds(pl.multiple_of(i * 32, 32), 32)
        x = normed[rows, :].astype(F32)
        factor = lax.rsqrt(jnp.mean(x * x, axis=-1, keepdims=True) + EPS)
        normed[rows, :] = (x * factor * gain[...]).astype(BF16)
        return carry

    lax.fori_loop(0, LEN // 32, norm, 0)
    local[3].wait()
    local[4].wait()

    def cols_of(h):
        return pl.ds(h * HD if isinstance(h, int) else pl.multiple_of(h * HD, HD), HD)

    def assemble_qkv(src):
        def step(r, carry):
            rows = pl.ds(pl.multiple_of(r * BLK, BLK), BLK)
            for c in range(6):
                wqkv[rows, c * BLK : (c + 1) * BLK] = src[table[r * 6 + c]]
            return carry

        lax.fori_loop(0, 32, step, 0, unroll=2)

    def assemble_out_chunk(src, tensor, q):
        for i in range(4):
            for j in range(8):
                wout[tensor, q, i * BLK : (i + 1) * BLK, j * BLK : (j + 1) * BLK] = src[
                    table[NQKV + i * 32 + q * 8 + j]
                ]

    def assemble_out(src, tensor):
        def step(i, carry):
            rows = pl.ds(pl.multiple_of(i * BLK, BLK), BLK)
            for j in range(32):
                wout[tensor, j // 8, rows, (j % 8) * BLK : (j % 8 + 1) * BLK] = src[
                    table[NQKV + i * 32 + j]
                ]
            return carry

        lax.fori_loop(0, 4, step, 0)

    all_rows = slice(0, LEN)
    half = LEN // 2
    halves = (slice(0, half), slice(half, LEN))

    def project(n, rows=all_rows):
        cols = slice(n * 256, (n + 1) * 256)
        proj[rows, cols] = nn(normed[rows, :], wqkv[:, cols])

    def head(h, turn=True, rows=all_rows):
        v = proj[rows, cols_of(h)]
        if turn:
            v = v * cos[rows, :] + pltpu.roll(v, 64, 1) * sin[rows, :]
        return v.astype(BF16)

    def heads():
        for h in range(QH + 2):
            qkv[:, cols_of(h)] = head(h, h < QH + 1)

    scale = HD**-0.5

    def primal(h, carry):
        k = qkv[:, cols_of(QH)]
        v = qkv[:, cols_of(QH + 1)]
        s = jnp.where(causal_mask(), nt(qkv[:, cols_of(h)], k) * scale, NEGATIVE)
        m = jnp.max(s, axis=-1, keepdims=True)
        e = jnp.exp(s - m)
        p = (e * (1.0 / jnp.sum(e, axis=-1, keepdims=True))).astype(BF16)
        probs[h] = p
        sides[1, :, cols_of(h)] = nn(p, v).astype(BF16)
        return carry

    for p in w:
        neighbours(p)
    for p in w:
        pass_on(p, 0)
    for p in w:
        opposite(p)
    begin(pr)
    for f in (-1, 1):
        for p in w:
            pass_on(p, f)
    for p in w:
        corner(p, 0)
    for p in w:
        pass_on(p, 2)
    for p in pr:
        neighbours(p)
    for p in pr:
        pass_on(p, 0)
    for f in (-1, 1, 2):
        for p in w:
            corner(p, f)
    for p in pr:
        opposite(p)
    sibling_done(w)
    assemble_qkv(slots_w)
    project(0)
    for p in pr:
        pass_on(p, -1)
    for p in pr:
        corner(p, 0)
    project(1)
    project(2)
    for p in pr:
        pass_on(p, 1)
    heads()
    lax.fori_loop(0, 2, primal, 0)
    for p in pr:
        pass_on(p, 2)
    lax.fori_loop(2, 4, primal, 0)
    assemble_out(slots_w, 0)
    for f in (-1, 1, 2):
        for p in pr:
            corner(p, f)
    sibling_done(pr)

    chunk = (wrap(x + 2), wrap(x + 1), wrap(x - 1), x)
    key_tangent, value_tangent = cols_of(0), cols_of(1)

    def tangent(s):
        rows, seen = halves[s], slice(0, half * (s + 1))
        for n in range(3):
            project(n, rows)
        wt[OWN, rows, key_tangent] = head(QH, True, rows)
        wt[OWN, rows, value_tangent] = head(QH + 1, False, rows)
        keys = jnp.concatenate([qkv[seen, cols_of(QH)], wt[OWN, seen, key_tangent]], axis=1)

        def one(h, carry):
            pb = probs[h, rows, seen]
            pf = pb.astype(F32)
            side = jnp.concatenate([head(h, True, rows), qkv[rows, cols_of(h)]], axis=1)
            pt = pf * (nt(side, keys) * scale)
            tp = (pt - pf * jnp.sum(pt, axis=-1, keepdims=True)).astype(BF16)
            sides[0, rows, cols_of(h)] = (
                nn(tp, qkv[seen, cols_of(QH + 1)]) + nn(pb, wt[OWN, seen, value_tangent])
            ).astype(BF16)
            return carry

        lax.fori_loop(0, QH, one, 0, unroll=2 - s)

    def term_at(rel, s, part):
        return (0, 32, 64, 160)[rel] + (s * 2 + part) * 8

    def term(rel, s):
        rows = halves[s]
        for n in range(2):
            cols = slice(n * 512, (n + 1) * 512)
            v = (
                nn(sides[0, rows, :], wout[0, chunk[rel], :, cols])
                + nn(sides[1, rows, :], wout[1, chunk[rel], :, cols])
            ).astype(BF16)
            for part in (0, 1):
                for j in range(4):
                    slots_w[term_at(rel, s, part) + 4 * n + j] = v[
                        part * BLK : (part + 1) * BLK, j * BLK : (j + 1) * BLK
                    ]

    def terms(rel, s, part):
        return slots_w.at[pl.ds(term_at(rel, s, part), 8)]

    def cast(name, src, dst, target):
        return send(name, src, dst, target)

    assemble_qkv(slots_p)
    tangent(0)
    for copy in sends:
        copy.wait_send()
    sends.clear()
    for s in (0, 1):
        if s == 1:
            tangent(1)
        for rel in (FAR, NXT, PRV):
            if s == 0:
                assemble_out_chunk(slots_p, 1, chunk[rel])
            term(rel, s)
            if rel == FAR:
                cast(("a0", s), terms(FAR, s, 0), opp.at[0, s], up)
                cast(("b0", s), terms(FAR, s, 1), opp.at[1, s], down)
            if rel == NXT and s == 0:
                cast(("a1", s), terms(NXT, s, 1), low.at[1, s], up)
            if rel == PRV and s == 0:
                cast(("b1", s), terms(PRV, s, 0), high.at[0, s], down)
        if s == 0:
            assemble_out_chunk(slots_p, 1, chunk[OWN])
            pl.semaphore_signal(ready, inc=1, device_id=sib, device_id_type=MESH)
    curv_loads = []
    for n in range(2):
        curv_loads.append(
            pltpu.make_async_copy(
                curv_in.at[:, pl.ds(pl.multiple_of(x * CHUNK + n * 512, 512), 512)],
                wqkv.at[n * LEN : (n + 1) * LEN, 0:512],
                local_sem.at[5 + n],
            )
        )
        curv_loads[-1].start()
    for s in (0, 1):
        got("a0", s)
        mine = slots_w[pl.ds(term_at(NXT, s, 0), 8)].astype(F32)
        opp[0, s] = (opp[0, s].astype(F32) + mine).astype(BF16)
        cast(("a2", s), opp.at[0, s], low.at[0, s], up)
        got("b0", s)
        mine = slots_w[pl.ds(term_at(PRV, s, 1), 8)].astype(F32)
        opp[1, s] = (opp[1, s].astype(F32) + mine).astype(BF16)
        cast(("b2", s), opp.at[1, s], high.at[1, s], down)
        if s == 0:
            cast(("a1", 1), terms(NXT, 1, 1), low.at[1, 1], up)
            cast(("b1", 1), terms(PRV, 1, 0), high.at[0, 1], down)
            term(OWN, 0)
            term(OWN, 1)
            turned = slice(2 * LEN, 3 * LEN)
            wqkv[turned, 0:512] = sides[1].T
            for copy in curv_loads:
                copy.wait()

    def part_rows(s, part):
        return pl.ds(s * half + part * BLK, BLK)

    def weigh(part, s):
        rows = s * half + part * BLK
        for j in range(8):
            total = (
                slots_w[term_at(OWN, s, part) + j].astype(F32)
                + low[part, s, j].astype(F32)
                + high[part, s, j].astype(F32)
            )
            at_row = (j // 4) * LEN + rows
            c = wqkv[at_row : at_row + BLK, (j % 4) * BLK : (j % 4 + 1) * BLK].astype(F32)
            wt[OWN, rows : rows + BLK, j * BLK : (j + 1) * BLK] = (total * c).astype(BF16)

    def hand_on(name, src, dst, part, s, target):
        r = part_rows(s, part)
        cast((name, s), wt.at[src, r], wt.at[dst, r], target)

    def mixed_cotangent(rel, s):
        rows = halves[s]
        v = nt(wt[rel, rows, :], wout[0, chunk[rel]])
        if rel == OWN:
            proj[rows, 0:OUT] = v
        else:
            proj[rows, 0:OUT] += v

    per = NB // 2
    n_in = NQKV // 2
    sb = 192

    def out_gradient(rel):
        for n in range(2):
            g = nn(wqkv[turned, 0:512], wt[rel, :, n * 512 : (n + 1) * 512]).astype(BF16)
            for i in range(4):
                for j in range(4):
                    slots_w[(j % 2) * per + n_in + 16 * i + 4 * chunk[rel] + 2 * n + j // 2] = g[
                        i * BLK : (i + 1) * BLK, j * BLK : (j + 1) * BLK
                    ]
        if rel == OWN:
            pl.semaphore_wait(ready, 1)
        for i in range(4):
            b = n_in + 16 * i + 4 * chunk[rel]
            cast(
                ("swap", rel, i),
                slots_w.at[pl.ds((1 - core) * per + b, 4)],
                slots_p.at[pl.ds(sb + b, 4)],
                sib,
            )

    for s in (0, 1):
        got("a1", s)
        got("b2", s)
        weigh(1, s)
        hand_on("c1", OWN, PRV, 1, s, up)
        hand_on("d1", OWN, NXT, 1, s, down)
        got("b1", s)
        got("a2", s)
        weigh(0, s)
        hand_on("d0", OWN, NXT, 0, s, down)
        hand_on("c0", OWN, PRV, 0, s, up)
        mixed_cotangent(OWN, s)
    for s in (0, 1):
        got("c1", s)
        hand_on("e1", PRV, FAR, 1, s, up)
        got("d0", s)
        hand_on("e0", NXT, FAR, 0, s, down)
        if s == 0:
            out_gradient(OWN)
        got("d1", s)
        mixed_cotangent(NXT, s)
        got("c0", s)
        mixed_cotangent(PRV, s)
    got("e1", 0)
    got("e0", 0)
    mixed_cotangent(FAR, 0)

    def unrot(v, rows):
        return v * cos[rows, :] - pltpu.roll(v, 64, 1) * sin[rows, :]

    tail = slice(OUT, QKV)
    proj[:, tail] = jnp.zeros((LEN, QKV - OUT), F32)

    def attention_back(s, begin, end, unroll):
        rows, seen = halves[s], slice(0, half * (s + 1))

        def one(h, carry):
            dm = proj[rows, cols_of(h)].astype(BF16)
            q = qkv[rows, cols_of(h)]
            pb = probs[h, rows, seen]
            dp = nt(dm, qkv[seen, cols_of(QH + 1)]).astype(BF16).astype(F32)
            pf = pb.astype(F32)
            pd = pf * dp
            ds = ((pd - pf * jnp.sum(pd, axis=-1, keepdims=True)) * scale).astype(BF16)
            dk = nn(q.T, ds)
            dv = nn(dm.T, pb)
            for u in range(s + 1):
                proj[u * BLK : (u + 1) * BLK, tail] += dk[:, u * half : (u + 1) * half]
                proj[half + u * BLK : half + (u + 1) * BLK, tail] += dv[
                    :, u * half : (u + 1) * half
                ]
            dq = unrot(nn(ds, qkv[seen, cols_of(QH)]).astype(BF16).astype(F32), rows).astype(BF16)
            sides[0, cols_of(h), rows] = dq.T
            return carry

        lax.fori_loop(begin, end, one, 0, unroll=unroll)

    attention_back(0, 0, QH, 1)
    out_gradient(NXT)
    out_gradient(PRV)
    got("e1", 1)
    got("e0", 1)
    out_gradient(FAR)
    mixed_cotangent(FAR, 1)
    for s in (0, 1):
        for name in ("a0", "b0", "a1", "b1"):
            done = arrivals[name, s]
            done.wait_send()
            sends[:] = [copy for copy in sends if copy is not done]

    def in_gradient(pair, lhs):
        for n in range(8):
            g = nn(lhs, normed[:, n * 512 : (n + 1) * 512]).astype(BF16)
            for r in range(4):
                for c in range(2):
                    slots_w[c * per + 32 * pair + 4 * n + r] = g[
                        c * BLK : (c + 1) * BLK, r * BLK : (r + 1) * BLK
                    ]
            if n % 2 == 1:
                b = 32 * pair + 8 * (n // 2)
                cast(
                    ("swap", pair, n // 2, 0),
                    slots_w.at[pl.ds((1 - core) * per + b, 8)],
                    slots_p.at[pl.ds(sb + b, 8)],
                    sib,
                )

    for pair in (0, 1):
        attention_back(1, 2 * pair, 2 * pair + 2, 2)
        in_gradient(pair, sides[0, 2 * pair * BLK : 2 * (pair + 1) * BLK, :])
    for u in range(2):
        dk = proj[u * BLK : (u + 1) * BLK, tail].astype(BF16).astype(F32).T
        sides[1, 0:BLK, halves[u]] = unrot(dk, halves[u]).astype(BF16).T
        sides[1, BLK : 2 * BLK, halves[u]] = proj[
            half + u * BLK : half + (u + 1) * BLK, tail
        ].astype(BF16)
    in_gradient(2, sides[1, 0 : 2 * BLK, :])
    for rel in (OWN, NXT, PRV, FAR):
        for i in range(4):
            got("swap", rel, i)
    for pair in range(3):
        for n in range(4):
            got("swap", pair, n, 0)
    for copy in sends:
        copy.wait_send()
    sends.clear()

    chain = (("z", "y"), ("y", "z"))
    here = {"y": y, "z": z}
    steps = (2, 1, -1, 0)

    def acc_at(part, rel, h):
        return ((part * 4 + rel) * 2 + h) * 12

    def red_at(part, h, srel):
        return 2 * per + (part * 2 + h) * 12 + 3 * srel

    def fill(part, rel):
        f = wrap(here[chain[part][0]] + steps[rel])
        for srel in range(4):
            s = wrap(here[chain[part][1]] + steps[srel])
            d = index_of(f, s, part) if part == 0 else index_of(s, f, part)
            base = (starts[d] + 1 - core) // 2
            for i in range(HALF):
                j = jnp.minimum(base + i, per - 1)
                j = jnp.where(j < n_in, 32 * lax.rem(j, 3) + lax.div(j, 3), j)
                slots_p[acc_at(part, rel, i // 3) + 3 * srel + i % 3] = (
                    slots_w[core * per + j].astype(F32) + slots_p[sb + j].astype(F32)
                ).astype(BF16)

    subs = ((0, 3), (3, 6), (9, 3))

    def acc(part, rel, h, u):
        return pl.ds(acc_at(part, rel, h) + subs[u][0], subs[u][1])

    def ring(part, name, u, src, dst, leg, step):
        send((part, name, u), src, dst, at(chain[part][leg], step))

    def send_far(part, u):
        sub = pl.ds(*subs[u])
        ring(part, "fu", u, slots_p.at[acc(part, FAR, 0, u)], r_far.at[part, 0, sub], 0, 1)
        ring(part, "fd", u, slots_p.at[acc(part, FAR, 1, u)], r_far.at[part, 1, sub], 0, -1)

    def send_near(part, u):
        sub = pl.ds(*subs[u])
        ring(part, "lo1", u, slots_p.at[acc(part, NXT, 1, u)], r_low.at[part, 1, sub], 0, 1)
        ring(part, "hi0", u, slots_p.at[acc(part, PRV, 0, u)], r_high.at[part, 0, sub], 0, -1)

    def middle(part, u):
        sub = pl.ds(*subs[u])
        got(part, "fu", u)
        r_far[part, 0, sub] = (
            r_far[part, 0, sub].astype(F32) + slots_p[acc(part, NXT, 0, u)].astype(F32)
        ).astype(BF16)
        ring(part, "lo0", u, r_far.at[part, 0, sub], r_low.at[part, 0, sub], 0, 1)
        got(part, "fd", u)
        r_far[part, 1, sub] = (
            r_far[part, 1, sub].astype(F32) + slots_p[acc(part, PRV, 1, u)].astype(F32)
        ).astype(BF16)
        ring(part, "hi1", u, r_far.at[part, 1, sub], r_high.at[part, 1, sub], 0, -1)

    def reduce(part, u):
        sub = pl.ds(*subs[u])
        for name in ("lo1", "hi0", "lo0", "hi1"):
            got(part, name, u)
        for h in (0, 1):
            slots_w[pl.ds(red_at(part, h, 0) + subs[u][0], subs[u][1])] = (
                slots_p[acc(part, OWN, h, u)].astype(F32)
                + r_low[part, h, sub].astype(F32)
                + r_high[part, h, sub].astype(F32)
            ).astype(BF16)

    def red(part, h, srel):
        return pl.ds(red_at(part, h, srel), 3)

    both = (0, 1)
    for part in both:
        fill(part, FAR)
        send_far(part, 0)
    for part in both:
        fill(part, NXT)
        fill(part, PRV)
        send_near(part, 0)
    for part in both:
        send_far(part, 1)
        send_near(part, 1)
    for part in both:
        fill(part, OWN)
    for part in both:
        middle(part, 0)
    for part in both:
        send_far(part, 2)
        send_near(part, 2)
    for part in both:
        middle(part, 1)
    for part in both:
        reduce(part, 0)
        ring(part, "tu", 0, slots_w.at[red(part, 0, FAR)], t_far.at[part, 0], 1, 1)
        ring(part, "td", 0, slots_w.at[red(part, 1, FAR)], t_far.at[part, 1], 1, -1)
    for part in both:
        middle(part, 2)
    for part in both:
        reduce(part, 1)
        ring(part, "tl1", 0, slots_w.at[red(part, 1, NXT)], t_low.at[part, 1], 1, 1)
        ring(part, "th0", 0, slots_w.at[red(part, 0, PRV)], t_high.at[part, 0], 1, -1)
    for part in both:
        got(part, "tu", 0)
        t_far[part, 0] = (
            t_far[part, 0].astype(F32) + slots_w[red(part, 0, NXT)].astype(F32)
        ).astype(BF16)
        ring(part, "tl0", 0, t_far.at[part, 0], t_low.at[part, 0], 1, 1)
        got(part, "td", 0)
        t_far[part, 1] = (
            t_far[part, 1].astype(F32) + slots_w[red(part, 1, PRV)].astype(F32)
        ).astype(BF16)
        ring(part, "th1", 0, t_far.at[part, 1], t_high.at[part, 1], 1, -1)
    for part in both:
        reduce(part, 2)
    for part in both:
        for name in ("tl1", "th0", "tl0", "th1"):
            got(part, name, 0)

    def whole(part, h):
        return (
            slots_w[pl.ds(2 * per + (part * 2 + h) * 12 + 3 * OWN, 3)].astype(F32)
            + t_low[part, h].astype(F32)
            + t_high[part, h].astype(F32)
        )

    for h in (0, 1):
        out[pl.ds(3 * h, 3)] = whole(1 - core, h)
    last = cast(("last",), out.at[pl.ds(0, HALF)], tot.at[core], sib)
    for h in (0, 1):
        tot[core, pl.ds(3 * h, 3)] = whole(core, h)
    last.wait_recv()
    for copy in sends:
        copy.wait_send()

    start, n = starts[me], counts[me]
    for t in range(SLOTS):
        b = start + t
        parity = lax.rem(b, 2)
        v = tot[parity, b // 2 - (start + 1 - parity) // 2]
        v = jnp.where(b < NQKV, v.T, v)
        out[t] = jnp.where(t < n, v, 0.0)


def product(counts, w, p, gain, tokens, cos, sin, curv):
    vmem = pl.BlockSpec(memory_space=pltpu.VMEM)
    hbm = pl.BlockSpec(memory_space=pl.ANY)
    smem = pl.BlockSpec(memory_space=pltpu.SMEM)
    v = pltpu.VMEM
    block = (BLK, BLK)
    return pl.pallas_call(
        kernel,
        out_shape=jax.ShapeDtypeStruct((SLOTS,) + block, F32),
        in_specs=[smem, hbm, hbm, vmem, hbm, hbm, hbm, hbm],
        out_specs=vmem,
        scratch_shapes=[
            pltpu.SMEM((NB,), jnp.int32),
            pltpu.SMEM((32,), jnp.int32),
            v((32 * SLOTS,) + block, BF16),
            v((32 * SLOTS,) + block, BF16),
            v((LEN, D), BF16),
            v((LEN, HD), F32),
            v((LEN, HD), F32),
            v((D, QKV), BF16),
            v((2, 4, OUT, CHUNK), BF16),
            v((LEN, QKV), F32),
            v((2, LEN, OUT), BF16),
            v((QH, LEN, LEN), BF16),
            v((LEN, QKV), BF16),
            v((2, 2, 8) + block, BF16),
            v((2, 2, 8) + block, BF16),
            v((2, 2, 8) + block, BF16),
            v((4, LEN, CHUNK), BF16),
            v((2, 2, 12) + block, BF16),
            v((2, 2, 12) + block, BF16),
            v((2, 2, 12) + block, BF16),
            v((2, 2, 3) + block, BF16),
            v((2, 2, 3) + block, BF16),
            v((2, 2, 3) + block, BF16),
            v((2, HALF) + block, F32),
            pltpu.SemaphoreType.DMA((245,)),
            pltpu.SemaphoreType.DMA((245,)),
            pltpu.SemaphoreType.DMA((7,)),
            pltpu.SemaphoreType.REGULAR,
        ],
        compiler_params=pltpu.CompilerParams(
            collective_id=0, has_side_effects=True, vmem_limit_bytes=67_000_000
        ),
        name="product",
    )(counts, w, p, gain, tokens, cos, sin, curv)


def local(tokens, norm_gain, curvature, weight_slots, probe_slots, block_counts):
    counts = block_counts[0]
    cos, sin = tables()
    out = product(
        counts,
        weight_slots[0],
        probe_slots[0],
        norm_gain.reshape(1, D),
        tokens[0],
        cos,
        sin,
        curvature[0],
    )
    return (out * (1.0 / np.sqrt(np.float32(LEN * 32))))[None]


def solution(mesh):
    in_specs = (
        P("fsdp", None, None),
        P(),
        P("fsdp", None, None),
        P("seq", "fsdp", None, None),
        P("seq", "fsdp", None, None),
        P("seq", None),
    )
    out_specs = P("seq", "fsdp", None, None)
    return jax.shard_map(local, mesh=mesh, in_specs=in_specs, out_specs=out_specs, check_vma=False)
```
